512 devices in a mesh: row: 32 (over z_hi, y), col: 16 (over x, z_lo, core).
Axes of the slice: x: 4, y: 8, z: 8 (z_hi: 4, z_lo: 2; z = z_hi * 2 + z_lo), core: 2. Of those that a mesh axis runs over, the one named last changes fastest.
Arguments:
- sequence: bfloat16 [512, 1024], P('row'), may hold values from -6 to 6
- pair_state: bfloat16 [512, 512, 128], P('row', 'col'), may hold values from -6 to 6
- residue_mask: int32 [512], replicated, may hold values 0 or 1
- chain_index: int32 [512], replicated, may hold values from 0 to 3, never falling along the last dimension, each value on 1 to 256 neighbouring positions
- attention_in: bfloat16 [1024, 4, 1024], P(None, None, 'col'), may hold values from -0.1875 to 0.1875
- attention_out: bfloat16 [1024, 1024], P('col'), may hold values from -0.1875 to 0.1875
- bias_weight: bfloat16 [128, 32], replicated, may hold values from -40 to 40
- chain_bias: float32 [32], replicated, may hold values from -2 to 2
- outer_in: bfloat16 [1024, 128], replicated, may hold values from -0.1875 to 0.1875
- outer_out: bfloat16 [128, 128], replicated, may hold values from -0.5 to 0.5
- triangle_in: bfloat16 [128, 5, 128], replicated, may hold values from -0.5 to 0.5
- triangle_out: bfloat16 [128, 128], replicated, may hold values from -0.5 to 0.5
- transition_up: bfloat16 [128, 512], replicated, may hold values from -0.5 to 0.5
- transition_down: bfloat16 [512, 128], replicated, may hold values from -0.25 to 0.25
Outputs:
- sequence_out: bfloat16 [512, 1024], P('row')
- pair_out: bfloat16 [512, 512, 128], P('row', 'col')
The draws below stay inside these ranges and needn't reach their ends.
Inputs may be any that keep to these rules, and one draw needn't show every extreme that they name: chain_index never falls along the residues; each chain holds at most 256 residues.
All inputs are finite; a program needn't handle non-finite values.
Results may differ from the reference program's by a relative error of at most 0.0095.
The reference program's roundings to bfloat16 on the way count: a program that leaves them out, or rounds other values in their place, can miss the bound.
Values may be sent and summed in bfloat16 or wider, within the bound.
No kernel may reach another device: no remote copies, remote signals or barrier semaphores. Data moves between devices by JAX's collectives and lax.ppermute only.
A program may use at most 64 MiB of HBM per device.

```python
import math
import jax
import jax.numpy as jnp
import numpy as np
from jax import lax

D = 1024
HEADS = 32
HEADDIM = 32
C = 128
P_SIZE = 64
F = 512
L = 512


def draw_bias_weight(key, part):
    base = jax.random.normal(jax.random.fold_in(key, 11), (C, HEADS), jnp.float32)
    values = base * (1.5 / math.sqrt(C))
    return jnp.clip(values, -40.0, 40.0).astype(jnp.bfloat16)


def plant(entries, stream_key, smallest, top_value):
    longest = entries.shape.index(max(entries.shape))
    spots = []
    for shift in (0, 1):
        where = [jax.random.randint(jax.random.fold_in(stream_key, axis), (), 0, length) for axis, length in enumerate(entries.shape)]
        where[longest] = (where[longest] + shift) % entries.shape[longest]
        spots.append(tuple(where))
    return entries.at[spots[0]].set(smallest).at[spots[1]].set(top_value)


def block_levels(own_key, shape, split, smallest, top_value):
    loudness = 1.0
    for dim, shards_of in split:
        draws = jax.random.uniform(jax.random.fold_in(jax.random.fold_in(own_key, 6), dim), (shards_of,), jnp.float32, smallest / len(split), top_value / len(split))
        loudness = loudness * jnp.repeat(jnp.exp(draws), shape[dim] // shards_of).reshape((-1,) + (1,) * (len(shape) - 1 - dim))
    return loudness


def length_profile(number_of, total, limit, skew):
    weights = [(1 << 20) // math.isqrt(standing ** skew) + 1 for standing in range(2, number_of + 1)]
    surplus, holding = total - limit - (number_of - 1), [1] * (number_of - 1)
    while surplus > 0:
        free = [i for i in range(number_of - 1) if holding[i] < limit]
        mass, left = sum([weights[i] for i in free]), surplus
        for i in free:
            more = min(limit - holding[i], max(1, left * weights[i] // mass), surplus)
            holding[i] = holding[i] + more
            surplus = surplus - more
    return np.array([limit] + holding)


def uneven_parts(key, count, total, limit, lean):
    if count == 2:
        one = jax.random.randint(key, (), max(1, total - limit), min(limit, total - 1) + 1)
        return jnp.stack([one, total - one])
    lengths = jnp.asarray(length_profile(count, total, limit, lean), jnp.int32)
    pairs = (count - 1) // 2
    source_of, taker = lengths[1:1 + 2 * pairs:2], lengths[2:2 + 2 * pairs:2]
    room = jnp.minimum(source_of - 1, limit - taker)
    passed = jax.random.randint(jax.random.fold_in(key, 1), (pairs,), 0, 1 << 20) % (room + 1)
    lengths = lengths.at[1:1 + 2 * pairs:2].set(source_of - passed).at[2:2 + 2 * pairs:2].set(taker + passed)
    return lengths[jax.random.permutation(jax.random.fold_in(key, 2), count)]


def gaussian(own_key, shape, width, reach, shards=(), held_as=jnp.bfloat16):
    factor_of = block_levels(own_key, shape, shards, -0.22, 0.18) if shards else 1.0
    drawn = jax.random.normal(own_key, shape, jnp.float32) * width * factor_of
    return jnp.minimum(jnp.maximum(drawn, -reach), reach).astype(held_as)


def setup_inputs(seed: int = 0) -> dict:
    seeds = jax.random.split(jax.random.key(seed), 15)
    sequence = gaussian(seeds[0], (L, D), 1.0, 6.0, ((0, 32),))
    pair_state = gaussian(seeds[1], (L, L, C), 1.0, 6.0, ((0, 32), (1, 16)))
    residue_mask = plant((jax.random.randint(seeds[2], (L,), 0, 8) < 7).astype(jnp.int32), jax.random.fold_in(seeds[2], 1), 0, 1)
    chain_index = jnp.searchsorted(jnp.cumsum(uneven_parts(seeds[3], 4, L, L // 2, 0)), jnp.arange(L), side="right").astype(jnp.int32)
    attention_in = gaussian(seeds[4], (D, 4, D), D ** -0.5, 0.1875, ((2, 16),))
    attention_out = gaussian(seeds[5], (D, D), D ** -0.5, 0.1875, ((0, 16),))
    bias_weight = draw_bias_weight(jax.random.fold_in(seeds[14], 71), 0)
    chain_bias = jnp.clip(jax.random.uniform(seeds[7], (HEADS,), jnp.float32, -2.0, 2.0), -2.0, 2.0)
    outer_in = gaussian(seeds[8], (D, 2 * P_SIZE), D ** -0.5, 0.1875)
    outer_out = gaussian(seeds[9], (2 * P_SIZE, C), (2 * P_SIZE) ** -0.5, 0.5)
    triangle_in = gaussian(seeds[10], (C, 5, C), C ** -0.5, 0.5)
    triangle_out = gaussian(seeds[11], (C, C), C ** -0.5, 0.5)
    transition_up = gaussian(seeds[12], (C, F), C ** -0.5, 0.5)
    transition_down = gaussian(seeds[13], (F, C), F ** -0.5, 0.25)
    return dict(sequence=sequence, pair_state=pair_state, residue_mask=residue_mask, chain_index=chain_index, attention_in=attention_in, attention_out=attention_out, bias_weight=bias_weight, chain_bias=chain_bias, outer_in=outer_in, outer_out=outer_out, triangle_in=triangle_in, triangle_out=triangle_out, transition_up=transition_up, transition_down=transition_down)


def layer_norm(values):
    center = values - lax.optimization_barrier(jnp.mean(values, axis=-1, keepdims=True))
    spread = lax.optimization_barrier(jnp.mean(center * center, axis=-1, keepdims=True))
    return center * lax.rsqrt(spread + 1e-05)

def reference(sequence, pair_state, residue_mask, chain_index, attention_in, attention_out, bias_weight, chain_bias, outer_in, outer_out, triangle_in, triangle_out, transition_up, transition_down):
    pair_wide = pair_state.astype(jnp.float32)
    normed_pair = layer_norm(pair_wide).astype(jnp.bfloat16)
    pair_bias = jnp.einsum('ijc,ch->hij', normed_pair.astype(jnp.float32), bias_weight.astype(jnp.float32))
    normed_seq = layer_norm(sequence.astype(jnp.float32)).astype(jnp.bfloat16)
    projected = jnp.einsum('id,dpe->ipe', normed_seq.astype(jnp.float32), attention_in.astype(jnp.float32))
    query = projected[:, 0].astype(jnp.bfloat16).reshape(L, HEADS, HEADDIM)
    keys = projected[:, 1].astype(jnp.bfloat16).reshape(L, HEADS, HEADDIM)
    values = projected[:, 2].astype(jnp.bfloat16).reshape(L, HEADS, HEADDIM)
    gate = jax.nn.sigmoid(projected[:, 3])
    scale = 1.0 / math.sqrt(HEADDIM)
    scores = jnp.einsum('ihd,jhd->hij', query.astype(jnp.float32), keys.astype(jnp.float32)) * scale
    same_chain = (chain_index[:, None] == chain_index[None, :]).astype(jnp.float32)
    scores = scores + pair_bias + chain_bias[:, None, None] * same_chain[None]
    positions = jnp.arange(L, dtype=jnp.int32)
    allowed = (residue_mask[None, :] == 1) | (positions[:, None] == positions[None, :])
    allowed = allowed[None]
    highest = lax.optimization_barrier(jnp.max(jnp.where(allowed, scores, -jnp.inf), axis=-1, keepdims=True))
    raised = jnp.where(allowed, jnp.exp(scores - highest), 0.0)
    weights = (raised / lax.optimization_barrier(jnp.sum(raised, axis=-1, keepdims=True))).astype(jnp.bfloat16)
    gathered = jnp.einsum('hij,jhd->ihd', weights.astype(jnp.float32), values.astype(jnp.float32)).reshape(L, D)
    mixed = (gate * gathered).astype(jnp.bfloat16)
    update = jnp.dot(mixed, attention_out, preferred_element_type=jnp.float32)
    sequence_out = (sequence.astype(jnp.float32) + update).astype(jnp.bfloat16)
    normed_out = layer_norm(sequence_out.astype(jnp.float32)).astype(jnp.bfloat16)
    outer_rows = jnp.dot(normed_out, outer_in, preferred_element_type=jnp.float32).astype(jnp.bfloat16)
    left_side = outer_rows[:, :P_SIZE].astype(jnp.float32)
    right_side = outer_rows[:, P_SIZE:].astype(jnp.float32)
    outer_feat = jnp.concatenate([left_side[:, None, :] * right_side[None, :, :], left_side[:, None, :] - right_side[None, :, :]], axis=-1).astype(jnp.bfloat16)
    pair_mid = pair_wide + jnp.einsum('ijc,ce->ije', outer_feat.astype(jnp.float32), outer_out.astype(jnp.float32))
    normed_mid = layer_norm(pair_mid).astype(jnp.bfloat16)
    live = residue_mask.astype(jnp.float32)
    flat_in = triangle_in.reshape(C, 5 * C)

    def triangle_row(packed):
        row_normed, row_live = packed
        tri = jnp.dot(row_normed, flat_in, preferred_element_type=jnp.float32).reshape(L, 5, C)
        pair_live = (row_live * live)[:, None]
        left_row = (jax.nn.sigmoid(tri[:, 0]) * tri[:, 1] * pair_live).astype(jnp.bfloat16)
        right_row = (jax.nn.sigmoid(tri[:, 2]) * tri[:, 3] * pair_live).astype(jnp.bfloat16)
        return (left_row, right_row, jax.nn.sigmoid(tri[:, 4]))
    left_op, right_op, out_gate = lax.map(triangle_row, (normed_mid, live))
    product = jnp.einsum('ikc,jkc->ijc', left_op.astype(jnp.float32), right_op.astype(jnp.float32))
    normed_product = layer_norm(product).astype(jnp.bfloat16)
    pair_late = pair_mid + out_gate * jnp.einsum('ijc,ce->ije', normed_product.astype(jnp.float32), triangle_out.astype(jnp.float32))
    normed_late = layer_norm(pair_late).astype(jnp.bfloat16)

    def transition_row(row_normed):
        hidden = jax.nn.relu(jnp.dot(row_normed, transition_up, preferred_element_type=jnp.float32)).astype(jnp.bfloat16)
        return jnp.dot(hidden, transition_down, preferred_element_type=jnp.float32)
    pair_out = (pair_late + lax.map(transition_row, normed_late)).astype(jnp.bfloat16)
    return (sequence_out, pair_out)
```

```python
import math

import jax
import jax.numpy as jnp
from jax import lax
from jax.sharding import Mesh
from jax.sharding import PartitionSpec as P

ROW = ("row_0", "row_1")
BF16 = jnp.bfloat16
F32 = jnp.float32


def exchange(blocks, axis):
    return lax.all_to_all(blocks, axis, split_axis=0, concat_axis=0, tiled=True)


def from_everyone(value, axis):
    copies = jnp.broadcast_to(value, (lax.axis_size(axis), *value.shape))
    return exchange(copies, axis)


def layer_norm(values, axis=-1):
    center = values - jnp.mean(values, axis=axis, keepdims=True)
    spread = jnp.mean(center * center, axis=axis, keepdims=True)
    return center * lax.rsqrt(spread + 1e-05)


def per_device(
    sequence,
    pair_state,
    residue_mask,
    chain_index,
    attention_in,
    attention_out,
    bias_weight,
    chain_bias,
    outer_in,
    outer_out,
    triangle_in,
    triangle_out,
    transition_up,
    transition_down,
):
    rows_here, cols_here, channels = pair_state.shape
    length_all = residue_mask.shape[0]
    pairs_here = rows_here * cols_here
    row_index = lax.axis_index(ROW)
    col_index = lax.axis_index("col")
    outer_rows_count = lax.axis_size("row_0")
    inner_rows_count = lax.axis_size("row_1")
    row_count = outer_rows_count * inner_rows_count
    col_count = lax.axis_size("col")
    row_start = row_index * rows_here
    col_start = col_index * cols_here

    normed_seq = layer_norm(sequence.astype(F32)).astype(BF16)
    projected = jnp.einsum("id,dpe->ipe", normed_seq, attention_in, preferred_element_type=F32)
    query = projected[:, 0].astype(BF16)
    key_values = projected[:, 1:3].astype(BF16).reshape(rows_here, -1)
    gate = jax.nn.sigmoid(projected[:, 3])
    key_values, pair_state = lax.optimization_barrier((key_values, pair_state))
    key_values_all = from_everyone(key_values, ROW).reshape(length_all, -1)

    pair_wide = pair_state.astype(F32)
    normed_pair = layer_norm(pair_wide).astype(BF16)
    bias_tile = jnp.einsum("ijc,ch->hij", normed_pair, bias_weight, preferred_element_type=F32)
    pair_bias = lax.all_to_all(bias_tile, "col", split_axis=0, concat_axis=2, tiled=True)
    heads_here = pair_bias.shape[0]

    width = query.shape[1]
    head_width = width // heads_here
    query_heads = query.reshape(rows_here, heads_here, head_width)
    key_heads = key_values_all[:, :width].reshape(length_all, heads_here, head_width)
    value_heads = key_values_all[:, width:].reshape(length_all, heads_here, head_width)
    scale = 1.0 / math.sqrt(head_width)
    scores = (
        jnp.einsum("ihd,jhd->hij", query_heads, key_heads, preferred_element_type=F32) * scale
    )
    chain_rows = lax.dynamic_slice_in_dim(chain_index, row_start, rows_here, 0)
    same_chain = (chain_rows[:, None] == chain_index[None, :]).astype(F32)
    head_offset = lax.dynamic_slice_in_dim(chain_bias, col_index * heads_here, heads_here, 0)
    scores = scores + pair_bias + head_offset[:, None, None] * same_chain[None]
    positions = jnp.arange(length_all, dtype=jnp.int32)
    query_ids = row_start + jnp.arange(rows_here, dtype=jnp.int32)
    allowed = (residue_mask[None, :] == 1) | (query_ids[:, None] == positions[None, :])
    allowed = allowed[None]
    highest = jnp.max(jnp.where(allowed, scores, -jnp.inf), axis=-1, keepdims=True)
    raised = jnp.where(allowed, jnp.exp(scores - highest), 0.0)
    weights = (raised / jnp.sum(raised, axis=-1, keepdims=True)).astype(BF16)
    gathered = jnp.einsum(
        "hij,jhd->ihd", weights, value_heads, preferred_element_type=F32
    ).reshape(rows_here, -1)
    mixed = (gate * gathered).astype(BF16)
    head_terms = jnp.dot(mixed, attention_out, preferred_element_type=F32).astype(BF16)
    update = jnp.sum(from_everyone(head_terms, "col").astype(F32), axis=0)
    sequence_out = (sequence.astype(F32) + update).astype(BF16)

    normed_out = layer_norm(sequence_out.astype(F32)).astype(BF16)
    outer_rows = jnp.dot(normed_out, outer_in, preferred_element_type=F32).astype(BF16)
    half_width = outer_rows.shape[1] // 2
    outer_all = from_everyone(outer_rows, ROW).reshape(length_all, -1)
    right_side = lax.dynamic_slice_in_dim(outer_all, col_start, cols_here, 0)
    right_side = right_side[:, half_width:].astype(F32)
    left_side = outer_rows[:, :half_width].astype(F32)
    outer_feat = jnp.concatenate(
        [
            left_side[:, None, :] * right_side[None, :, :],
            left_side[:, None, :] - right_side[None, :, :],
        ],
        axis=-1,
    ).astype(BF16)
    pair_mid = pair_wide.reshape(pairs_here, channels) + jnp.dot(
        outer_feat.reshape(pairs_here, 2 * half_width), outer_out, preferred_element_type=F32
    )
    normed_mid = layer_norm(pair_mid).astype(BF16)

    operand_in = triangle_in[:, :4].reshape(channels, 4 * channels)
    tri = lax.dot_general(
        operand_in, normed_mid, (((0,), (1,)), ((), ())), preferred_element_type=F32
    ).reshape(4, channels, pairs_here)
    live = residue_mask.astype(F32)
    row_live = lax.dynamic_slice_in_dim(live, row_start, rows_here, 0)
    col_live = lax.dynamic_slice_in_dim(live, col_start, cols_here, 0)
    pair_live = (row_live[:, None] * col_live[None, :]).reshape(1, pairs_here)
    left_op = (jax.nn.sigmoid(tri[0]) * tri[1] * pair_live).astype(BF16)
    right_op = (jax.nn.sigmoid(tri[2]) * tri[3] * pair_live).astype(BF16)
    out_gate = jax.nn.sigmoid(
        jnp.dot(normed_mid, triangle_in[:, 4], preferred_element_type=F32)
    )

    group = channels // col_count
    tiles = jnp.concatenate(
        [
            left_op.reshape(col_count, group, pairs_here),
            right_op.reshape(col_count, group, pairs_here),
        ],
        axis=1,
    )
    tiles = exchange(tiles, "col").reshape(col_count, 2, group, rows_here, cols_here)
    panels = jnp.transpose(tiles, (2, 1, 3, 0, 4)).reshape(group, 2 * rows_here, length_all)
    panels = exchange(panels, "row_1")
    lefts = panels[:, :rows_here].reshape(-1, length_all)
    rights = panels[:, rows_here:].reshape(-1, length_all)
    here = lax.axis_index("row_0")
    rights_all = jnp.zeros((outer_rows_count, *rights.shape), rights.dtype)
    for step in range(outer_rows_count):
        turn = [(p, (p + step) % outer_rows_count) for p in range(outer_rows_count)]
        arrived = lax.ppermute(rights, "row_0", turn) if step else rights
        origin = lax.rem(here - step + outer_rows_count, outer_rows_count)
        rights_all = lax.dynamic_update_slice_in_dim(rights_all, arrived[None], origin, 0)
    product = lax.dot_general(
        lefts,
        rights_all.reshape(-1, length_all),
        (((1,), (1,)), ((), ())),
        preferred_element_type=F32,
    ).astype(BF16)
    product = exchange(product.reshape(inner_rows_count, rows_here, length_all), "row_1")
    product = jnp.transpose(
        product.reshape(group, rows_here, col_count, cols_here), (2, 0, 1, 3)
    ).reshape(col_count, group, pairs_here)
    product = exchange(product, "col").reshape(channels, pairs_here)

    normed_product = layer_norm(product.astype(F32), axis=0).astype(BF16)
    projected_product = lax.dot_general(
        normed_product, triangle_out, (((0,), (0,)), ((), ())), preferred_element_type=F32
    )
    pair_late = pair_mid + out_gate * projected_product
    normed_late = layer_norm(pair_late).astype(BF16)
    hidden = jax.nn.relu(
        jnp.dot(normed_late, transition_up, preferred_element_type=F32)
    ).astype(BF16)
    lowered = jnp.dot(hidden, transition_down, preferred_element_type=F32)
    pair_out = (pair_late + lowered).astype(BF16).reshape(rows_here, cols_here, channels)
    return (sequence_out, pair_out)


def solution(mesh):
    finer = Mesh(mesh.devices.reshape(4, 8, mesh.shape["col"]), ("row_0", "row_1", "col"))
    placed = (
        P(ROW, None),
        P(ROW, "col", None),
        P(),
        P(),
        P(None, None, "col"),
        P("col", None),
        P(),
        P(),
        P(),
        P(),
        P(),
        P(),
        P(),
        P(),
    )
    return jax.shard_map(
        per_device,
        mesh=finer,
        in_specs=placed,
        out_specs=(P(ROW, None), P(ROW, "col", None)),
        check_vma=False,
    )
```

```python
import math

import jax
import jax.numpy as jnp
from jax import lax
from jax.sharding import Mesh
from jax.sharding import PartitionSpec as P

ROW = ("row_0", "row_1")
BF16 = jnp.bfloat16
F32 = jnp.float32
K_PARTS = 2
I_PARTS = 2


def exchange(blocks, axis):
    return lax.all_to_all(blocks, axis, split_axis=0, concat_axis=0, tiled=True)


def from_everyone(value, axis):
    copies = jnp.broadcast_to(value, (lax.axis_size(axis), *value.shape))
    return exchange(copies, axis)


def layer_norm(values, axis=-1):
    center = values - jnp.mean(values, axis=axis, keepdims=True)
    spread = jnp.mean(center * center, axis=axis, keepdims=True)
    return center * lax.rsqrt(spread + 1e-05)


def per_device(
    sequence,
    pair_state,
    residue_mask,
    chain_index,
    attention_in,
    attention_out,
    bias_weight,
    chain_bias,
    outer_in,
    outer_out,
    triangle_in,
    triangle_out,
    transition_up,
    transition_down,
):
    rows_here, cols_here, channels = pair_state.shape
    length_all = residue_mask.shape[0]
    pairs_here = rows_here * cols_here
    row_index = lax.axis_index(ROW)
    col_index = lax.axis_index("col")
    row_count = lax.axis_size(ROW)
    col_count = lax.axis_size("col")
    row_start = row_index * rows_here
    col_start = col_index * cols_here

    normed_seq = layer_norm(sequence.astype(F32)).astype(BF16)
    projected = jnp.einsum("id,dpe->ipe", normed_seq, attention_in, preferred_element_type=F32)
    query = projected[:, 0].astype(BF16)
    key_values = projected[:, 1:3].astype(BF16).reshape(rows_here, -1)
    gate = jax.nn.sigmoid(projected[:, 3])
    key_values, pair_state = lax.optimization_barrier((key_values, pair_state))
    key_values_all = from_everyone(key_values, ROW).reshape(length_all, -1)

    pair_wide = pair_state.astype(F32)
    normed_pair = layer_norm(pair_wide).astype(BF16)
    bias_tile = jnp.einsum("ijc,ch->hij", normed_pair, bias_weight, preferred_element_type=F32)
    pair_bias = lax.all_to_all(bias_tile, "col", split_axis=0, concat_axis=2, tiled=True)
    heads_here = pair_bias.shape[0]

    width = query.shape[1]
    head_width = width // heads_here
    query_heads = query.reshape(rows_here, heads_here, head_width)
    key_heads = key_values_all[:, :width].reshape(length_all, heads_here, head_width)
    value_heads = key_values_all[:, width:].reshape(length_all, heads_here, head_width)
    scale = 1.0 / math.sqrt(head_width)
    scores = (
        jnp.einsum("ihd,jhd->hij", query_heads, key_heads, preferred_element_type=F32) * scale
    )
    chain_rows = lax.dynamic_slice_in_dim(chain_index, row_start, rows_here, 0)
    same_chain = (chain_rows[:, None] == chain_index[None, :]).astype(F32)
    head_offset = lax.dynamic_slice_in_dim(chain_bias, col_index * heads_here, heads_here, 0)
    scores = scores + pair_bias + head_offset[:, None, None] * same_chain[None]
    positions = jnp.arange(length_all, dtype=jnp.int32)
    query_ids = row_start + jnp.arange(rows_here, dtype=jnp.int32)
    allowed = (residue_mask[None, :] == 1) | (query_ids[:, None] == positions[None, :])
    allowed = allowed[None]
    highest = jnp.max(jnp.where(allowed, scores, -jnp.inf), axis=-1, keepdims=True)
    raised = jnp.where(allowed, jnp.exp(scores - highest), 0.0)
    weights = (raised / jnp.sum(raised, axis=-1, keepdims=True)).astype(BF16)
    gathered = jnp.einsum(
        "hij,jhd->ihd", weights, value_heads, preferred_element_type=F32
    ).reshape(rows_here, -1)
    mixed = (gate * gathered).astype(BF16)
    head_terms = jnp.dot(mixed, attention_out, preferred_element_type=F32).astype(BF16)
    update = jnp.sum(from_everyone(head_terms, "col").astype(F32), axis=0)
    sequence_out = (sequence.astype(F32) + update).astype(BF16)

    normed_out = layer_norm(sequence_out.astype(F32)).astype(BF16)
    outer_rows = jnp.dot(normed_out, outer_in, preferred_element_type=F32).astype(BF16)
    half_width = outer_rows.shape[1] // 2
    outer_all = from_everyone(outer_rows, ROW).reshape(length_all, -1)
    right_side = lax.dynamic_slice_in_dim(outer_all, col_start, cols_here, 0)
    right_side = right_side[:, half_width:].astype(F32)
    left_side = outer_rows[:, :half_width].astype(F32)
    outer_feat = jnp.concatenate(
        [
            left_side[:, None, :] * right_side[None, :, :],
            left_side[:, None, :] - right_side[None, :, :],
        ],
        axis=-1,
    ).astype(BF16)
    pair_mid = pair_wide.reshape(pairs_here, channels) + jnp.dot(
        outer_feat.reshape(pairs_here, 2 * half_width), outer_out, preferred_element_type=F32
    )
    normed_mid = layer_norm(pair_mid).astype(BF16)

    operand_in = triangle_in[:, :4].reshape(channels, 4 * channels)
    tri = lax.dot_general(
        operand_in, normed_mid, (((0,), (1,)), ((), ())), preferred_element_type=F32
    ).reshape(4, channels, pairs_here)
    live = residue_mask.astype(F32)
    row_live = lax.dynamic_slice_in_dim(live, row_start, rows_here, 0)
    col_live = lax.dynamic_slice_in_dim(live, col_start, cols_here, 0)
    pair_live = (row_live[:, None] * col_live[None, :]).reshape(1, pairs_here)
    left_op = (jax.nn.sigmoid(tri[0]) * tri[1] * pair_live).astype(BF16)
    right_op = (jax.nn.sigmoid(tri[2]) * tri[3] * pair_live).astype(BF16)
    out_gate = jax.nn.sigmoid(
        jnp.dot(normed_mid, triangle_in[:, 4], preferred_element_type=F32)
    )

    group = channels // col_count
    tiles = jnp.concatenate(
        [
            left_op.reshape(col_count, group, pairs_here),
            right_op.reshape(col_count, group, pairs_here),
        ],
        axis=1,
    )
    tiles = exchange(tiles, "col").reshape(K_PARTS, -1, 2, group, rows_here, cols_here)
    panels = jnp.transpose(tiles, (2, 0, 3, 4, 1, 5)).reshape(
        2, K_PARTS, 1, group, rows_here, length_all // K_PARTS
    )
    lefts = panels[0].reshape(K_PARTS, group, I_PARTS, rows_here // I_PARTS, -1)
    lefts = jnp.swapaxes(lefts, 1, 2)
    rights = jnp.broadcast_to(panels[1], (K_PARTS, I_PARTS, *panels.shape[3:]))
    panels = jnp.concatenate([lefts, rights], axis=3)
    panels = exchange(panels.reshape(row_count, -1, length_all // K_PARTS), ROW)
    few = rows_here // I_PARTS
    product = lax.dot_general(
        panels[:, :few].reshape(-1, length_all // K_PARTS),
        panels[:, few:].reshape(-1, length_all // K_PARTS),
        (((1,), (1,)), ((), ())),
        preferred_element_type=F32,
    ).astype(BF16)
    product = exchange(product.reshape(row_count, few, length_all), ROW)
    product = jnp.sum(
        product.reshape(K_PARTS, I_PARTS, group, few, length_all).astype(F32), axis=0
    ).astype(BF16)
    product = jnp.transpose(
        product.reshape(I_PARTS, group, few, col_count, cols_here), (3, 1, 0, 2, 4)
    ).reshape(col_count, group, pairs_here)
    product = exchange(product, "col").reshape(channels, pairs_here)

    normed_product = layer_norm(product.astype(F32), axis=0).astype(BF16)
    projected_product = lax.dot_general(
        normed_product, triangle_out, (((0,), (0,)), ((), ())), preferred_element_type=F32
    )
    pair_late = pair_mid + out_gate * projected_product
    normed_late = layer_norm(pair_late).astype(BF16)
    hidden = jax.nn.relu(
        jnp.dot(normed_late, transition_up, preferred_element_type=F32)
    ).astype(BF16)
    lowered = jnp.dot(hidden, transition_down, preferred_element_type=F32)
    pair_out = (pair_late + lowered).astype(BF16).reshape(rows_here, cols_here, channels)
    return (sequence_out, pair_out)


def solution(mesh):
    finer = Mesh(mesh.devices.reshape(4, 8, mesh.shape["col"]), ("row_0", "row_1", "col"))
    placed = (
        P(ROW, None),
        P(ROW, "col", None),
        P(),
        P(),
        P(None, None, "col"),
        P("col", None),
        P(),
        P(),
        P(),
        P(),
        P(),
        P(),
        P(),
        P(),
    )
    return jax.shard_map(
        per_device,
        mesh=finer,
        in_specs=placed,
        out_specs=(P(ROW, None), P(ROW, "col", None)),
        check_vma=False,
    )
```

```python
import math

import jax
import jax.numpy as jnp
from jax import lax
from jax.experimental import pallas as pl
from jax.experimental.pallas import tpu as pltpu
from jax.sharding import Mesh
from jax.sharding import PartitionSpec as P

ROW = ("row_0", "row_1")
BF16 = jnp.bfloat16
F32 = jnp.float32
K_PARTS = 2
I_PARTS = 2


def exchange(blocks, axis):
    return lax.all_to_all(blocks, axis, split_axis=0, concat_axis=0, tiled=True)


def from_everyone(value, axis):
    copies = jnp.broadcast_to(value, (lax.axis_size(axis), *value.shape))
    return exchange(copies, axis)


def layer_norm(values, axis=-1):
    center = values - jnp.mean(values, axis=axis, keepdims=True)
    spread = jnp.mean(center * center, axis=axis, keepdims=True)
    return center * lax.rsqrt(spread + 1e-05)


def local_kernel(body, out_shape, name, *operands, scalars=0):
    spaces = [pltpu.SMEM if k < scalars else pltpu.VMEM for k in range(len(operands))]
    held = [
        x if space is pltpu.SMEM else pltpu.with_memory_space_constraint(x, space)
        for x, space in zip(operands, spaces)
    ]
    return pl.pallas_call(
        body,
        out_shape=out_shape,
        in_specs=[pl.BlockSpec(memory_space=space) for space in spaces],
        out_specs=jax.tree.map(lambda _: pl.BlockSpec(memory_space=pltpu.VMEM), out_shape),
        name=name,
    )(*held)


def mm(a, b, over_a, over_b):
    return lax.dot_general(a, b, (((over_a,), (over_b,)), ((), ())), preferred_element_type=F32)


def settle_body(terms, sequence, outer_in, sequence_out, left_twice, right_copies):
    update = jnp.sum(terms[...].astype(F32), axis=0)
    summed = (sequence[...].astype(F32) + update).astype(BF16)
    sequence_out[...] = summed
    normed = layer_norm(summed.astype(F32)).astype(BF16)
    outer_rows = mm(normed, outer_in[...], 1, 0).astype(BF16).astype(F32)
    rows, width = outer_rows.shape
    half = width // 2
    first = lax.broadcasted_iota(jnp.int32, (rows, width), 1) < half
    turned = pltpu.roll(outer_rows, half, 1)
    left_twice[...] = jnp.where(first, outer_rows, turned)
    packed = jnp.where(first[: rows // 2], turned[: rows // 2], outer_rows[rows // 2 :])
    right_copies[...] = jnp.broadcast_to(packed.astype(BF16)[None], right_copies.shape)


def pair_body(start, rights, left_twice, pair, outer_out, gates_in, values_in, last_in, live, tiles, mid, out_gate):
    rows, cols, channels = pair.shape
    half = channels // 2
    taken = rights[pl.ds(start[0], cols // rows)].astype(F32)
    first = lax.broadcasted_iota(jnp.int32, (rows // 2, channels), 1) < half
    pieces = []
    for k in range(cols // rows):
        turned = pltpu.roll(taken[k], half, 1)
        pieces.append(jnp.where(first, taken[k], turned))
        pieces.append(jnp.where(first, turned, taken[k]))
    right_twice = jnp.concatenate(pieces, axis=0)
    left = left_twice[...][:, None, :]
    right = right_twice[None, :, :]
    lane = lax.broadcasted_iota(jnp.int32, (rows, cols, channels), 2)
    feat = jnp.where(lane < half, left * right, left - right).astype(BF16)
    feat = feat.reshape(rows * cols, channels)
    pair_mid = pair[...].astype(F32).reshape(rows * cols, channels) + mm(feat, outer_out[...], 1, 0)
    mid[...] = pair_mid
    normed = layer_norm(pair_mid).astype(BF16)
    opened = jax.nn.sigmoid(mm(gates_in[...], normed, 1, 1))
    operands = opened * mm(values_in[...], normed, 1, 1) * live[...]
    tiles[...] = operands.astype(BF16).reshape(tiles.shape)
    out_gate[...] = jax.nn.sigmoid(mm(normed, last_in[...], 1, 0))


def tail_body(product, mid, out_gate, triangle_out, transition_up, transition_down, out):
    normed_product = layer_norm(product[...].astype(F32), axis=0)
    normed_product = jnp.transpose(normed_product).astype(BF16)
    late = mid[...] + out_gate[...] * mm(normed_product, triangle_out[...], 1, 0)
    normed_late = layer_norm(late).astype(BF16)
    hidden = jnp.maximum(mm(normed_late, transition_up[...], 1, 0), 0.0).astype(BF16)
    out[...] = (late + mm(hidden, transition_down[...], 1, 0)).astype(BF16)


def per_device(
    sequence,
    pair_state,
    residue_mask,
    chain_index,
    attention_in,
    attention_out,
    bias_weight,
    chain_bias,
    outer_in,
    outer_out,
    triangle_in,
    triangle_out,
    transition_up,
    transition_down,
):
    rows_here, cols_here, channels = pair_state.shape
    length_all = residue_mask.shape[0]
    pairs_here = rows_here * cols_here
    row_index = lax.axis_index(ROW)
    col_index = lax.axis_index("col")
    row_count = lax.axis_size(ROW)
    col_count = lax.axis_size("col")
    row_start = row_index * rows_here
    col_start = col_index * cols_here

    normed_seq = layer_norm(sequence.astype(F32)).astype(BF16)
    projected = jnp.einsum("id,dpe->ipe", normed_seq, attention_in, preferred_element_type=F32)
    query = projected[:, 0].astype(BF16)
    key_values = projected[:, 1:3].astype(BF16).reshape(rows_here, -1)
    gate = jax.nn.sigmoid(projected[:, 3])
    key_values_all = from_everyone(key_values, ROW).reshape(length_all, -1)

    pair_wide = pair_state.astype(F32)
    normed_pair = layer_norm(pair_wide).astype(BF16)
    bias_tile = jnp.einsum("ijc,ch->hij", normed_pair, bias_weight, preferred_element_type=F32)
    one = (1 + jnp.minimum(col_index, 0)).astype(BF16)
    attention_out, outer_in, outer_out = attention_out * one, outer_in * one, outer_out * one
    triangle_out, transition_up = triangle_out * one, transition_up * one
    transition_down = transition_down * one
    group = channels // col_count
    by_channel = jnp.transpose(triangle_in, (1, 2, 0)) * one
    grouped = by_channel[:4].reshape(2, 2, col_count, group, channels)
    gates_in = jnp.swapaxes(grouped[:, 0], 0, 1).reshape(2 * channels, channels)
    values_in = jnp.swapaxes(grouped[:, 1], 0, 1).reshape(2 * channels, channels)
    last_in = triangle_in[:, 4] * one
    live = residue_mask.astype(F32)
    row_live = lax.dynamic_slice_in_dim(live, row_start, rows_here, 0)
    col_live = lax.dynamic_slice_in_dim(live, col_start, cols_here, 0)
    pair_live = (row_live[:, None] * col_live[None, :]).reshape(1, pairs_here)
    (
        key_values_all,
        bias_tile,
        attention_out,
        outer_in,
        outer_out,
        triangle_out,
        transition_up,
        transition_down,
        gates_in,
        values_in,
        last_in,
        pair_live,
    ) = lax.optimization_barrier(
        (
            key_values_all,
            bias_tile,
            attention_out,
            outer_in,
            outer_out,
            triangle_out,
            transition_up,
            transition_down,
            gates_in,
            values_in,
            last_in,
            pair_live,
        )
    )
    pair_bias = lax.all_to_all(bias_tile, "col", split_axis=0, concat_axis=2, tiled=True)
    heads_here = pair_bias.shape[0]

    width = query.shape[1]
    head_width = width // heads_here
    query_heads = query.reshape(rows_here, heads_here, head_width)
    key_heads = key_values_all[:, :width].reshape(length_all, heads_here, head_width)
    value_heads = key_values_all[:, width:].reshape(length_all, heads_here, head_width)
    scale = 1.0 / math.sqrt(head_width)
    scores = (
        jnp.einsum("ihd,jhd->hij", query_heads, key_heads, preferred_element_type=F32) * scale
    )
    chain_rows = lax.dynamic_slice_in_dim(chain_index, row_start, rows_here, 0)
    same_chain = (chain_rows[:, None] == chain_index[None, :]).astype(F32)
    head_offset = lax.dynamic_slice_in_dim(chain_bias, col_index * heads_here, heads_here, 0)
    scores = scores + pair_bias + head_offset[:, None, None] * same_chain[None]
    positions = jnp.arange(length_all, dtype=jnp.int32)
    query_ids = row_start + jnp.arange(rows_here, dtype=jnp.int32)
    allowed = (residue_mask[None, :] == 1) | (query_ids[:, None] == positions[None, :])
    allowed = allowed[None]
    highest = jnp.max(jnp.where(allowed, scores, -jnp.inf), axis=-1, keepdims=True)
    raised = jnp.where(allowed, jnp.exp(scores - highest), 0.0)
    weights = (raised / jnp.sum(raised, axis=-1, keepdims=True)).astype(BF16)
    gathered = jnp.einsum(
        "hij,jhd->ihd", weights, value_heads, preferred_element_type=F32
    ).reshape(rows_here, -1)
    mixed = (gate * gathered).astype(BF16)
    head_terms = jnp.dot(mixed, attention_out, preferred_element_type=F32).astype(BF16)
    terms = from_everyone(head_terms, "col")
    width = outer_in.shape[1]
    sequence_out, left_twice, right_copies = local_kernel(
        settle_body,
        (
            jax.ShapeDtypeStruct(sequence.shape, BF16),
            pltpu.VMEM((rows_here, width), F32),
            pltpu.VMEM((row_count, rows_here // 2, width), BF16),
        ),
        "settle",
        terms,
        sequence,
        outer_in,
    )
    rights = exchange(right_copies, ROW)
    tiles, pair_mid, out_gate = local_kernel(
        pair_body,
        (
            pltpu.VMEM((col_count, 2 * group, pairs_here), BF16),
            pltpu.VMEM((pairs_here, channels), F32),
            pltpu.VMEM((pairs_here, channels), F32),
        ),
        "pair",
        (col_index * (cols_here // rows_here)).reshape(1),
        rights,
        left_twice,
        pair_state,
        outer_out,
        gates_in,
        values_in,
        last_in,
        pair_live,
        scalars=1,
    )

    tiles = exchange(tiles, "col").reshape(K_PARTS, -1, 2, group, rows_here, cols_here)
    panels = jnp.transpose(tiles, (2, 0, 3, 4, 1, 5)).reshape(
        2, K_PARTS, 1, group, rows_here, length_all // K_PARTS
    )
    lefts = panels[0].reshape(K_PARTS, group, I_PARTS, rows_here // I_PARTS, -1)
    lefts = jnp.swapaxes(lefts, 1, 2)
    rights = jnp.broadcast_to(panels[1], (K_PARTS, I_PARTS, *panels.shape[3:]))
    panels = jnp.concatenate([lefts, rights], axis=3)
    panels = exchange(panels.reshape(row_count, -1, length_all // K_PARTS), ROW)
    few = rows_here // I_PARTS
    product = lax.dot_general(
        panels[:, :few].reshape(-1, length_all // K_PARTS),
        panels[:, few:].reshape(-1, length_all // K_PARTS),
        (((1,), (1,)), ((), ())),
        preferred_element_type=F32,
    ).astype(BF16)
    product = exchange(product.reshape(row_count, few, length_all), ROW)
    product = jnp.sum(
        product.reshape(K_PARTS, I_PARTS, group, few, length_all).astype(F32), axis=0
    ).astype(BF16)
    product = jnp.transpose(
        product.reshape(I_PARTS, group, few, col_count, cols_here), (3, 1, 0, 2, 4)
    ).reshape(col_count, group, pairs_here)
    product = exchange(product, "col").reshape(channels, pairs_here)

    pair_out = local_kernel(
        tail_body,
        jax.ShapeDtypeStruct((pairs_here, channels), BF16),
        "tail",
        product,
        pair_mid,
        out_gate,
        triangle_out,
        transition_up,
        transition_down,
    ).reshape(rows_here, cols_here, channels)
    return (sequence_out, pair_out)


def solution(mesh):
    finer = Mesh(mesh.devices.reshape(4, 8, mesh.shape["col"]), ("row_0", "row_1", "col"))
    placed = (
        P(ROW, None),
        P(ROW, "col", None),
        P(),
        P(),
        P(None, None, "col"),
        P("col", None),
        P(),
        P(),
        P(),
        P(),
        P(),
        P(),
        P(),
        P(),
    )
    return jax.shard_map(
        per_device,
        mesh=finer,
        in_specs=placed,
        out_specs=(P(ROW, None), P(ROW, "col", None)),
        check_vma=False,
    )
```

```python
import math

import jax
import jax.numpy as jnp
from jax import lax
from jax.experimental import pallas as pl
from jax.experimental.pallas import tpu as pltpu
from jax.sharding import Mesh
from jax.sharding import PartitionSpec as P

ROW = ("row_0", "row_1")
BF16 = jnp.bfloat16
F32 = jnp.float32
K_PARTS = 2
I_PARTS = 2
LANES = 128
GROUPS = 4


def exchange(blocks, axis):
    return lax.all_to_all(blocks, axis, split_axis=0, concat_axis=0, tiled=True)


def from_everyone(value, axis):
    copies = jnp.broadcast_to(value, (lax.axis_size(axis), *value.shape))
    return exchange(copies, axis)


def layer_norm(values, axis=-1):
    center = values - jnp.mean(values, axis=axis, keepdims=True)
    spread = jnp.mean(center * center, axis=axis, keepdims=True)
    return center * lax.rsqrt(spread + 1e-05)


def local_kernel(body, out_shape, name, *operands, scalars=0, scratch=()):
    spaces = [pltpu.SMEM if k < scalars else pltpu.VMEM for k in range(len(operands))]
    held = [
        x if space is pltpu.SMEM else pltpu.with_memory_space_constraint(x, space)
        for x, space in zip(operands, spaces)
    ]
    return pl.pallas_call(
        body,
        out_shape=out_shape,
        in_specs=[pl.BlockSpec(memory_space=space) for space in spaces],
        out_specs=jax.tree.map(lambda _: pl.BlockSpec(memory_space=pltpu.VMEM), out_shape),
        scratch_shapes=scratch,
        name=name,
    )(*held)


def mm(a, b, over_a, over_b):
    return lax.dot_general(a, b, (((over_a,), (over_b,)), ((), ())), preferred_element_type=F32)


def turn_lanes(value, groups):
    steps = groups % GROUPS
    return pltpu.roll(value, steps * (LANES // GROUPS), 1) if steps else value


def regroup(pick, shape):
    group = lax.broadcasted_iota(jnp.int32, shape, 1) // (LANES // GROUPS)
    tile = pick(0)
    for k in range(1, GROUPS):
        tile = jnp.where(group == k, pick(k), tile)
    return tile


def project_body(sequence, weights, key_values, query, gate):
    normed = layer_norm(sequence[...].astype(F32)).astype(BF16)
    projected = mm(normed, weights[...], 1, 1)
    rows = projected.shape[0]
    head, rest = projected[:, :LANES], projected[:, LANES:]
    first = lax.broadcasted_iota(jnp.int32, (rows, LANES), 1) < LANES // 2
    both = jnp.where(first, pltpu.roll(head, LANES // 2, 1), pltpu.roll(rest, LANES // 2, 1))
    key_values[...] = jnp.broadcast_to(both.astype(BF16)[None], key_values.shape)
    query[...] = jnp.where(first, head, 0.0).astype(BF16).astype(F32)
    gate[...] = jnp.where(first, 0.0, jax.nn.sigmoid(rest))


def bias_body(pair, bias_in, blocks):
    rows, cols, channels = pair.shape
    wide = pair[...].astype(F32)
    turned = jnp.concatenate([wide[GROUPS * (p % GROUPS) + p // GROUPS] for p in range(rows)], axis=0)
    normed = layer_norm(turned).astype(BF16)
    bias = mm(bias_in[...], normed, 1, 1)
    count = blocks.shape[0]
    for h in range(2):
        for t in range(GROUPS):
            part = bias[h * count : (h + 1) * count, t * LANES : (t + 1) * LANES]
            blocks[:, h * GROUPS + t, :] = part


def attention_body(
    start, offsets, blocks, key_values, query, gate, mask, chain, attention_out, copies, spread, joined
):
    count, eight, _ = blocks.shape
    four = eight // 2
    length = count * (LANES // GROUPS)
    rows = query.shape[0]
    lane = lax.broadcasted_iota(jnp.int32, (four, LANES), 1)
    for g in range(GROUPS):
        taken = query[g * four : (g + 1) * four, :]
        for h in range(2):
            own = (lane >= h * (LANES // 4)) & (lane < (h + 1) * (LANES // 4))
            spread[g * eight + h * four : g * eight + (h + 1) * four, :] = jnp.where(own, taken, 0.0)
    everyone = key_values[...].reshape(length, LANES)
    raw = mm(spread[...].astype(BF16), everyone, 1, 1)
    raw = raw * (1.0 / math.sqrt(LANES // 4))
    position = lax.broadcasted_iota(jnp.int32, (eight, length), 1)
    row = lax.broadcasted_iota(jnp.int32, (eight, length), 0)
    chains = jnp.broadcast_to(chain[...], (eight, length))
    kept = jnp.broadcast_to(mask[...], (eight, length)) == 1
    offset = jnp.where(row < four, offsets[0], offsets[1])
    weights = []
    for g in range(GROUPS):
        pieces = []
        for tile in range(count // GROUPS):
            pieces.append(
                regroup(
                    lambda k, tile=tile, g=g: turn_lanes(blocks[GROUPS * tile + k], k - g),
                    (eight, LANES),
                )
            )
        bias = jnp.concatenate(pieces, axis=1)
        here = position == start[0] + g * four + row % four
        own_chain = jnp.sum(jnp.where(here, chains, 0).astype(F32), axis=1, keepdims=True)
        same = chains.astype(F32) == own_chain
        scores = raw[g * eight : (g + 1) * eight] + bias + jnp.where(same, offset, 0.0)
        allowed = kept | here
        highest = jnp.max(jnp.where(allowed, scores, -jnp.inf), axis=1, keepdims=True)
        raised = jnp.where(allowed, jnp.exp(scores - highest), 0.0)
        weights.append(raised / jnp.sum(raised, axis=1, keepdims=True))
    mixed = mm(jnp.concatenate(weights, axis=0).astype(BF16), everyone, 1, 0)
    for g in range(GROUPS):
        upper = mixed[g * eight : g * eight + four]
        lower = mixed[g * eight + four : (g + 1) * eight]
        joined[g * four : (g + 1) * four, :] = jnp.where(lane < LANES * 3 // 4, upper, lower)
    gated = pltpu.roll(gate[...] * joined[...], LANES // 2, 1)[:, : LANES // 2].astype(BF16)
    terms = mm(gated, attention_out[...], 1, 0).astype(BF16)
    copies[...] = jnp.broadcast_to(terms[None], copies.shape)


def spread_body(tiles, order, panels):
    count, chans, pairs = tiles.shape
    rows = pairs // (LANES // GROUPS)
    per = count // GROUPS
    by_row = []
    for i in range(rows):
        at, g = i // GROUPS * LANES, i % GROUPS
        by_row.append(
            jnp.concatenate(
                [
                    regroup(
                        lambda k, tile=tile, g=g, at=at: turn_lanes(
                            tiles[GROUPS * tile + k, :, at : at + LANES].astype(F32), k - g
                        ),
                        (chans, LANES),
                    )
                    for tile in range(per)
                ],
                axis=1,
            )
        )
    turned = mm(order[...], jnp.concatenate(by_row, axis=0).astype(BF16), 1, 0).astype(BF16)
    half = chans // 2
    few = rows // I_PARTS
    wide = turned.shape[1] // K_PARTS
    for k in range(K_PARTS):
        for i in range(I_PARTS):
            for c in range(half):
                block = (k * I_PARTS + i) * half + c
                at = c * rows + i * few
                panels[block, :few, :] = turned[at : at + few, k * wide : (k + 1) * wide]
                at = (half + c) * rows
                panels[block, few:, :] = turned[at : at + rows, k * wide : (k + 1) * wide]


def gather_body(parts, order, blocks):
    total, few, length = parts.shape
    count, group, pairs = blocks.shape
    rows = pairs // (LANES // GROUPS)
    summed = mm(order[...], parts[...].reshape(total * few, length), 1, 0)
    for q in range(count):
        tile, s = q // GROUPS, q % GROUPS
        pieces = []
        for t in range(rows // GROUPS):
            pieces.append(
                regroup(
                    lambda k, t=t, tile=tile, s=s: turn_lanes(
                        summed[
                            (GROUPS * t + k) * group : (GROUPS * t + k + 1) * group,
                            tile * LANES : (tile + 1) * LANES,
                        ],
                        k - s,
                    ),
                    (group, LANES),
                )
            )
        blocks[q] = jnp.concatenate(pieces, axis=1).astype(BF16)


def settle_body(terms, sequence, outer_in, sequence_out, left_twice, right_copies):
    update = jnp.sum(terms[...].astype(F32), axis=0)
    summed = (sequence[...].astype(F32) + update).astype(BF16)
    sequence_out[...] = summed
    normed = layer_norm(summed.astype(F32)).astype(BF16)
    outer_rows = mm(normed, outer_in[...], 1, 0).astype(BF16).astype(F32)
    rows, width = outer_rows.shape
    half = width // 2
    first = lax.broadcasted_iota(jnp.int32, (rows, width), 1) < half
    turned = pltpu.roll(outer_rows, half, 1)
    left_twice[...] = jnp.where(first, outer_rows, turned)
    packed = jnp.where(first[: rows // 2], turned[: rows // 2], outer_rows[rows // 2 :])
    right_copies[...] = jnp.broadcast_to(packed.astype(BF16)[None], right_copies.shape)


def pair_body(start, rights, left_twice, pair, outer_out, gates_in, values_in, last_in, live, tiles, mid, out_gate):
    rows, cols, channels = pair.shape
    half = channels // 2
    taken = rights[pl.ds(start[0], cols // rows)].astype(F32)
    first = lax.broadcasted_iota(jnp.int32, (rows // 2, channels), 1) < half
    pieces = []
    for k in range(cols // rows):
        turned = pltpu.roll(taken[k], half, 1)
        pieces.append(jnp.where(first, taken[k], turned))
        pieces.append(jnp.where(first, turned, taken[k]))
    right_twice = jnp.concatenate(pieces, axis=0)
    left = left_twice[...][:, None, :]
    right = right_twice[None, :, :]
    lane = lax.broadcasted_iota(jnp.int32, (rows, cols, channels), 2)
    feat = jnp.where(lane < half, left * right, left - right).astype(BF16)
    feat = feat.reshape(rows * cols, channels)
    pair_mid = pair[...].astype(F32).reshape(rows * cols, channels) + mm(feat, outer_out[...], 1, 0)
    mid[...] = pair_mid
    normed = layer_norm(pair_mid).astype(BF16)
    opened = jax.nn.sigmoid(mm(gates_in[...], normed, 1, 1))
    operands = opened * mm(values_in[...], normed, 1, 1) * live[...]
    tiles[...] = operands.astype(BF16).reshape(tiles.shape)
    out_gate[...] = jax.nn.sigmoid(mm(normed, last_in[...], 1, 0))


def tail_body(product, mid, out_gate, triangle_out, transition_up, transition_down, out):
    normed_product = layer_norm(product[...].astype(F32), axis=0)
    normed_product = jnp.transpose(normed_product).astype(BF16)
    late = mid[...] + out_gate[...] * mm(normed_product, triangle_out[...], 1, 0)
    normed_late = layer_norm(late).astype(BF16)
    hidden = jnp.maximum(mm(normed_late, transition_up[...], 1, 0), 0.0).astype(BF16)
    out[...] = (late + mm(hidden, transition_down[...], 1, 0)).astype(BF16)


def per_device(
    sequence,
    pair_state,
    residue_mask,
    chain_index,
    attention_in,
    attention_out,
    bias_weight,
    chain_bias,
    outer_in,
    outer_out,
    triangle_in,
    triangle_out,
    transition_up,
    transition_down,
):
    rows_here, cols_here, channels = pair_state.shape
    length_all = residue_mask.shape[0]
    pairs_here = rows_here * cols_here
    row_index = lax.axis_index(ROW)
    col_index = lax.axis_index("col")
    row_count = lax.axis_size(ROW)
    col_count = lax.axis_size("col")
    row_start = row_index * rows_here
    col_start = col_index * cols_here

    group = channels // col_count
    heads_here = bias_weight.shape[1] // col_count

    weights = jnp.transpose(attention_in, (1, 2, 0)).reshape(-1, sequence.shape[1])
    key_values, query, gate = local_kernel(
        project_body,
        (
            pltpu.VMEM((row_count, rows_here, LANES), BF16),
            pltpu.VMEM((rows_here, LANES), F32),
            pltpu.VMEM((rows_here, LANES), F32),
        ),
        "project",
        sequence,
        weights,
    )
    key_values_all = exchange(key_values, ROW)

    bias_in = jnp.transpose(bias_weight.reshape(channels, col_count, heads_here), (2, 1, 0))
    bias_blocks = local_kernel(
        bias_body,
        pltpu.VMEM((col_count, heads_here * GROUPS, LANES), F32),
        "bias",
        pair_state,
        bias_in.reshape(-1, channels),
    )

    one = (1 + jnp.minimum(col_index, 0)).astype(BF16)
    attention_out, outer_in, outer_out = attention_out * one, outer_in * one, outer_out * one
    triangle_out, transition_up = triangle_out * one, transition_up * one
    transition_down = transition_down * one
    by_channel = jnp.transpose(triangle_in, (1, 2, 0)) * one
    grouped = by_channel[:4].reshape(2, 2, col_count, group, channels)
    gates_in = jnp.swapaxes(grouped[:, 0], 0, 1).reshape(2 * channels, channels)
    values_in = jnp.swapaxes(grouped[:, 1], 0, 1).reshape(2 * channels, channels)
    last_in = triangle_in[:, 4] * one
    rows_of = jnp.arange(2 * group * rows_here)
    spread_order = jax.nn.one_hot(
        rows_of % rows_here * (2 * group) + rows_of // rows_here, 2 * group * rows_here, dtype=BF16
    )
    few = rows_here // I_PARTS
    rows_of = jnp.arange(rows_here * group)
    source = (rows_of // group // few * group + rows_of % group) * few + rows_of // group % few
    gather_order = jnp.tile(
        jax.nn.one_hot(source, rows_here * group, dtype=BF16), (1, K_PARTS)
    )
    spread_order, gather_order = spread_order * one, gather_order * one
    whole = 1 + jnp.minimum(col_index, 0)
    mask_row = residue_mask.reshape(1, -1) * whole
    chain_row = chain_index.reshape(1, -1) * whole
    head_offset = lax.dynamic_slice_in_dim(chain_bias, col_index * heads_here, heads_here, 0)
    live = residue_mask.astype(F32)
    row_live = lax.dynamic_slice_in_dim(live, row_start, rows_here, 0)
    col_live = lax.dynamic_slice_in_dim(live, col_start, cols_here, 0)
    pair_live = (row_live[:, None] * col_live[None, :]).reshape(1, pairs_here)
    (
        key_values_all,
        bias_blocks,
        attention_out,
        outer_in,
        outer_out,
        triangle_out,
        transition_up,
        transition_down,
        gates_in,
        values_in,
        last_in,
        pair_live,
        spread_order,
        gather_order,
        mask_row,
        chain_row,
    ) = lax.optimization_barrier(
        (
            key_values_all,
            bias_blocks,
            attention_out,
            outer_in,
            outer_out,
            triangle_out,
            transition_up,
            transition_down,
            gates_in,
            values_in,
            last_in,
            pair_live,
            spread_order,
            gather_order,
            mask_row,
            chain_row,
        )
    )
    bias_blocks = exchange(bias_blocks, "col")
    terms = local_kernel(
        attention_body,
        pltpu.VMEM((col_count, *sequence.shape), BF16),
        "attention",
        row_start.reshape(1),
        head_offset,
        bias_blocks,
        key_values_all,
        query,
        gate,
        mask_row,
        chain_row,
        attention_out,
        scalars=2,
        scratch=(
            pltpu.VMEM((heads_here * rows_here, LANES), F32),
            pltpu.VMEM((rows_here, LANES), F32),
        ),
    )
    terms = exchange(terms, "col")
    width = outer_in.shape[1]
    sequence_out, left_twice, right_copies = local_kernel(
        settle_body,
        (
            jax.ShapeDtypeStruct(sequence.shape, BF16),
            pltpu.VMEM((rows_here, width), F32),
            pltpu.VMEM((row_count, rows_here // 2, width), BF16),
        ),
        "settle",
        terms,
        sequence,
        outer_in,
    )
    rights = exchange(right_copies, ROW)
    tiles, pair_mid, out_gate = local_kernel(
        pair_body,
        (
            pltpu.VMEM((col_count, 2 * group, pairs_here), BF16),
            pltpu.VMEM((pairs_here, channels), F32),
            pltpu.VMEM((pairs_here, channels), F32),
        ),
        "pair",
        (col_index * (cols_here // rows_here)).reshape(1),
        rights,
        left_twice,
        pair_state,
        outer_out,
        gates_in,
        values_in,
        last_in,
        pair_live,
        scalars=1,
    )

    tiles = exchange(tiles, "col")
    panels = local_kernel(
        spread_body,
        pltpu.VMEM((row_count, few + rows_here, length_all // K_PARTS), BF16),
        "spread",
        tiles,
        spread_order,
    )
    panels = exchange(panels, ROW)
    product = lax.dot_general(
        panels[:, :few].reshape(-1, length_all // K_PARTS),
        panels[:, few:].reshape(-1, length_all // K_PARTS),
        (((1,), (1,)), ((), ())),
        preferred_element_type=F32,
    ).astype(BF16)
    product = exchange(product.reshape(row_count, few, length_all), ROW)
    product = local_kernel(
        gather_body,
        pltpu.VMEM((col_count, group, pairs_here), BF16),
        "gather",
        product,
        gather_order,
    )
    product = exchange(product, "col").reshape(channels, pairs_here)

    pair_out = local_kernel(
        tail_body,
        jax.ShapeDtypeStruct((pairs_here, channels), BF16),
        "tail",
        product,
        pair_mid,
        out_gate,
        triangle_out,
        transition_up,
        transition_down,
    ).reshape(rows_here, cols_here, channels)
    return (sequence_out, pair_out)


def solution(mesh):
    finer = Mesh(mesh.devices.reshape(4, 8, mesh.shape["col"]), ("row_0", "row_1", "col"))
    placed = (
        P(ROW, None),
        P(ROW, "col", None),
        P(),
        P(),
        P(None, None, "col"),
        P("col", None),
        P(),
        P(),
        P(),
        P(),
        P(),
        P(),
        P(),
        P(),
    )
    return jax.shard_map(
        per_device,
        mesh=finer,
        in_specs=placed,
        out_specs=(P(ROW, None), P(ROW, "col", None)),
        check_vma=False,
    )
```

```python
import math

import jax
import jax.numpy as jnp
from jax import lax
from jax.experimental import pallas as pl
from jax.experimental.pallas import tpu as pltpu
from jax.sharding import Mesh
from jax.sharding import PartitionSpec as P

ROW = ("row_0", "row_1")
BF16 = jnp.bfloat16
F32 = jnp.float32
K_PARTS = 2
I_PARTS = 2
KEPT = (
    "pair",
    "mask",
    "chain",
    "attention_out",
    "outer_in",
    "outer_out",
    "triangle_out",
    "transition_up",
    "transition_down",
)
LANES = 128
GROUPS = 4


def exchange(blocks, axis):
    return lax.all_to_all(blocks, axis, split_axis=0, concat_axis=0, tiled=True)


def from_everyone(value, axis):
    copies = jnp.broadcast_to(value, (lax.axis_size(axis), *value.shape))
    return exchange(copies, axis)


def layer_norm(values, axis=-1):
    center = values - jnp.mean(values, axis=axis, keepdims=True)
    spread = jnp.mean(center * center, axis=axis, keepdims=True)
    return center * lax.rsqrt(spread + 1e-05)


def local_kernel(body, out_shape, name, *operands, scalars=0, scratch=(), far=False, out_space=None):
    space = pltpu.HBM if far else pltpu.VMEM
    spaces = [pltpu.SMEM if k < scalars else space for k in range(len(operands))]
    held = [
        pltpu.with_memory_space_constraint(x, space) if space is pltpu.VMEM else x
        for x, space in zip(operands, spaces)
    ]
    out_space = out_space or pltpu.VMEM
    return pl.pallas_call(
        body,
        out_shape=out_shape,
        in_specs=[pl.BlockSpec(memory_space=space) for space in spaces],
        out_specs=jax.tree.map(lambda _: pl.BlockSpec(memory_space=out_space), out_shape),
        scratch_shapes=scratch,
        name=name,
    )(*held)


def fetch(sources, targets, arrived):
    copies = [
        pltpu.make_async_copy(source, target, arrived.at[k])
        for k, (source, target) in enumerate(zip(sources, targets))
    ]
    for copy in copies:
        copy.start()
    return copies


def mm(a, b, over_a, over_b):
    return lax.dot_general(a, b, (((over_a,), (over_b,)), ((), ())), preferred_element_type=F32)


def turn_lanes(value, groups):
    steps = groups % GROUPS
    return pltpu.roll(value, steps * (LANES // GROUPS), 1) if steps else value


def regroup(pick, shape):
    group = lax.broadcasted_iota(jnp.int32, shape, 1) // (LANES // GROUPS)
    tile = pick(0)
    for k in range(1, GROUPS):
        tile = jnp.where(group == k, pick(k), tile)
    return tile


def project_body(sequence, weights, key_values, query, gate, near, held, arrived):
    first_copy, second_copy = fetch((sequence, weights), (near, held), arrived)
    first_copy.wait()
    normed = layer_norm(near[...].astype(F32)).astype(BF16)
    second_copy.wait()
    projected = mm(normed, held[...], 1, 1)
    rows = projected.shape[0]
    head, rest = projected[:, :LANES], projected[:, LANES:]
    first = lax.broadcasted_iota(jnp.int32, (rows, LANES), 1) < LANES // 2
    both = jnp.where(first, pltpu.roll(head, LANES // 2, 1), pltpu.roll(rest, LANES // 2, 1))
    key_values[...] = jnp.broadcast_to(both.astype(BF16)[None], key_values.shape)
    query[...] = jnp.where(first, head, 0.0).astype(BF16).astype(F32)
    gate[...] = jnp.where(first, 0.0, jax.nn.sigmoid(rest))


def prepare_body(row_start, col_start, *refs):
    count = len(KEPT)
    sources, targets = refs[: count + 2], refs[count + 2 : 2 * count + 2]
    blocks, gates_in, values_in, last_in, live, spread_order, gather_order = refs[2 * count + 2 : -4]
    bias_near, triangle_near, turned_bias, arrived = refs[-4:]
    copies = fetch(sources, (*targets, bias_near, triangle_near), arrived)
    near = dict(zip(KEPT, targets))
    landed = dict(zip((*KEPT, "bias_in", "triangle"), copies))

    size = spread_order.shape[0]
    n = lax.broadcasted_iota(jnp.int32, spread_order.shape, 0)
    m = lax.broadcasted_iota(jnp.int32, spread_order.shape, 1)
    rows = live.shape[1] // (LANES // GROUPS)
    wanted = n % rows * (size // rows) + n // rows
    spread_order[...] = jnp.where(m == wanted, 1.0, 0.0).astype(BF16)
    size = gather_order.shape[0]
    group, few = size // rows, rows // I_PARTS
    n = lax.broadcasted_iota(jnp.int32, gather_order.shape, 0)
    m = lax.broadcasted_iota(jnp.int32, gather_order.shape, 1)
    i, c = n // group, n % group
    wanted = (i // few * group + c) * few + i % few
    gather_order[...] = jnp.where(m % size == wanted, 1.0, 0.0).astype(BF16)

    landed["pair"].wait()
    landed["bias_in"].wait()
    wide = near["pair"][...].astype(F32)
    turned = jnp.concatenate([wide[GROUPS * (p % GROUPS) + p // GROUPS] for p in range(rows)], axis=0)
    normed = layer_norm(turned).astype(BF16)
    bias = mm(bias_near[...], normed, 1, 1)
    columns = blocks.shape[0]
    for t in range(GROUPS):
        turned_bias[t] = bias[:, t * LANES : (t + 1) * LANES]
        for h in range(2):
            blocks[:, h * GROUPS + t, :] = turned_bias[t, pl.ds(h, columns, stride=2), :]

    landed["mask"].wait()
    mask = near["mask"][...].astype(F32).astype(BF16)
    length = mask.shape[1]
    residue = lax.broadcasted_iota(jnp.int32, (length, live.shape[1]), 0)
    pair = lax.broadcasted_iota(jnp.int32, (length, live.shape[1]), 1)
    of_row = jnp.where(residue == row_start[0] + pair // (LANES // GROUPS), 1.0, 0.0).astype(BF16)
    of_col = jnp.where(residue == col_start[0] + pair % (LANES // GROUPS), 1.0, 0.0).astype(BF16)
    mask = jnp.broadcast_to(mask, (8, length))
    live[...] = (mm(mask, of_row, 1, 0) * mm(mask, of_col, 1, 0))[:1]

    landed["triangle"].wait()
    half = gates_in.shape[1] // 2
    for k, target in enumerate((gates_in, values_in, gates_in, values_in)):
        side = half * (k // 2)
        across = jnp.transpose(triangle_near[k].astype(F32)).astype(BF16)
        target[:, side : side + half, :] = across.reshape(target.shape[0], half, LANES)
    last_in[...] = triangle_near[4]
    for name in KEPT:
        if name not in ("pair", "mask"):
            landed[name].wait()


def attention_body(
    start, col, offsets, blocks, key_values, query, gate, mask, chain, attention_out, copies, spread, joined
):
    count, eight, _ = blocks.shape
    four = eight // 2
    length = count * (LANES // GROUPS)
    rows = query.shape[0]
    lane = lax.broadcasted_iota(jnp.int32, (four, LANES), 1)
    for g in range(GROUPS):
        taken = query[g * four : (g + 1) * four, :]
        for h in range(2):
            own = (lane >= h * (LANES // 4)) & (lane < (h + 1) * (LANES // 4))
            spread[g * eight + h * four : g * eight + (h + 1) * four, :] = jnp.where(own, taken, 0.0)
    everyone = key_values[...].reshape(length, LANES)
    raw = mm(spread[...].astype(BF16), everyone, 1, 1)
    raw = raw * (1.0 / math.sqrt(LANES // 4))
    position = lax.broadcasted_iota(jnp.int32, (eight, length), 1)
    row = lax.broadcasted_iota(jnp.int32, (eight, length), 0)
    chains = jnp.broadcast_to(chain[...], (eight, length))
    kept = jnp.broadcast_to(mask[...], (eight, length)) == 1
    offset = jnp.where(row < four, offsets[2 * col[0]], offsets[2 * col[0] + 1])
    weights = []
    for g in range(GROUPS):
        pieces = []
        for tile in range(count // GROUPS):
            pieces.append(
                regroup(
                    lambda k, tile=tile, g=g: turn_lanes(blocks[GROUPS * tile + k], k - g),
                    (eight, LANES),
                )
            )
        bias = jnp.concatenate(pieces, axis=1)
        here = position == start[0] + g * four + row % four
        own_chain = jnp.sum(jnp.where(here, chains, 0).astype(F32), axis=1, keepdims=True)
        same = chains.astype(F32) == own_chain
        scores = raw[g * eight : (g + 1) * eight] + bias + jnp.where(same, offset, 0.0)
        allowed = kept | here
        highest = jnp.max(jnp.where(allowed, scores, -jnp.inf), axis=1, keepdims=True)
        raised = jnp.where(allowed, jnp.exp(scores - highest), 0.0)
        weights.append(raised / jnp.sum(raised, axis=1, keepdims=True))
    mixed = mm(jnp.concatenate(weights, axis=0).astype(BF16), everyone, 1, 0)
    for g in range(GROUPS):
        upper = mixed[g * eight : g * eight + four]
        lower = mixed[g * eight + four : (g + 1) * eight]
        joined[g * four : (g + 1) * four, :] = jnp.where(lane < LANES * 3 // 4, upper, lower)
    gated = pltpu.roll(gate[...] * joined[...], LANES // 2, 1)[:, : LANES // 2].astype(BF16)
    terms = mm(gated, attention_out[...], 1, 0).astype(BF16)
    copies[...] = jnp.broadcast_to(terms[None], copies.shape)


def spread_body(tiles, order, panels):
    count, chans, pairs = tiles.shape
    rows = pairs // (LANES // GROUPS)
    per = count // GROUPS
    by_row = []
    for i in range(rows):
        at, g = i // GROUPS * LANES, i % GROUPS
        by_row.append(
            jnp.concatenate(
                [
                    regroup(
                        lambda k, tile=tile, g=g, at=at: turn_lanes(
                            tiles[GROUPS * tile + k, :, at : at + LANES].astype(F32), k - g
                        ),
                        (chans, LANES),
                    )
                    for tile in range(per)
                ],
                axis=1,
            )
        )
    turned = mm(order[...], jnp.concatenate(by_row, axis=0).astype(BF16), 1, 0).astype(BF16)
    half = chans // 2
    few = rows // I_PARTS
    wide = turned.shape[1] // K_PARTS
    for k in range(K_PARTS):
        for i in range(I_PARTS):
            for c in range(half):
                block = (k * I_PARTS + i) * half + c
                at = c * rows + i * few
                panels[block, :few, :] = turned[at : at + few, k * wide : (k + 1) * wide]
                at = (half + c) * rows
                panels[block, few:, :] = turned[at : at + rows, k * wide : (k + 1) * wide]


def gather_body(parts, order, blocks):
    total, few, length = parts.shape
    count, group, pairs = blocks.shape
    rows = pairs // (LANES // GROUPS)
    summed = mm(order[...], parts[...].reshape(total * few, length), 1, 0)
    for q in range(count):
        tile, s = q // GROUPS, q % GROUPS
        pieces = []
        for t in range(rows // GROUPS):
            pieces.append(
                regroup(
                    lambda k, t=t, tile=tile, s=s: turn_lanes(
                        summed[
                            (GROUPS * t + k) * group : (GROUPS * t + k + 1) * group,
                            tile * LANES : (tile + 1) * LANES,
                        ],
                        k - s,
                    ),
                    (group, LANES),
                )
            )
        blocks[q] = jnp.concatenate(pieces, axis=1).astype(BF16)


def settle_body(terms, sequence, outer_in, sequence_out, left_twice, right_copies):
    update = jnp.sum(terms[...].astype(F32), axis=0)
    summed = (sequence[...].astype(F32) + update).astype(BF16)
    sequence_out[...] = summed
    normed = layer_norm(summed.astype(F32)).astype(BF16)
    outer_rows = mm(normed, outer_in[...], 1, 0).astype(BF16).astype(F32)
    rows, width = outer_rows.shape
    half = width // 2
    first = lax.broadcasted_iota(jnp.int32, (rows, width), 1) < half
    turned = pltpu.roll(outer_rows, half, 1)
    left_twice[...] = jnp.where(first, outer_rows, turned)
    packed = jnp.where(first[: rows // 2], turned[: rows // 2], outer_rows[rows // 2 :])
    right_copies[...] = jnp.broadcast_to(packed.astype(BF16)[None], right_copies.shape)


def pair_body(col, rights, left_twice, pair, outer_out, gates_in, values_in, last_in, live, tiles, mid, out_gate):
    rows, cols, channels = pair.shape
    half = channels // 2
    taken = rights[pl.ds(col[0] * (cols // rows), cols // rows)].astype(F32)
    first = lax.broadcasted_iota(jnp.int32, (rows // 2, channels), 1) < half
    pieces = []
    for k in range(cols // rows):
        turned = pltpu.roll(taken[k], half, 1)
        pieces.append(jnp.where(first, taken[k], turned))
        pieces.append(jnp.where(first, turned, taken[k]))
    right_twice = jnp.concatenate(pieces, axis=0)
    left = left_twice[...][:, None, :]
    right = right_twice[None, :, :]
    lane = lax.broadcasted_iota(jnp.int32, (rows, cols, channels), 2)
    feat = jnp.where(lane < half, left * right, left - right).astype(BF16)
    feat = feat.reshape(rows * cols, channels)
    pair_mid = pair[...].astype(F32).reshape(rows * cols, channels) + mm(feat, outer_out[...], 1, 0)
    mid[...] = pair_mid
    normed = layer_norm(pair_mid).astype(BF16)
    flat = (-1, channels)
    opened = jax.nn.sigmoid(mm(gates_in[...].reshape(flat), normed, 1, 1))
    operands = opened * mm(values_in[...].reshape(flat), normed, 1, 1) * live[...]
    tiles[...] = operands.astype(BF16).reshape(tiles.shape)
    out_gate[...] = jax.nn.sigmoid(mm(normed, last_in[...], 1, 0))


def tail_body(product, mid, out_gate, triangle_out, transition_up, transition_down, out, held, left):
    pairs = mid.shape[0]
    copies = []
    for k in range(pairs // LANES):
        here = pl.ds(k * LANES, LANES)
        normed_product = layer_norm(product[:, here].astype(F32), axis=0)
        normed_product = jnp.transpose(normed_product).astype(BF16)
        late = mid[here] + out_gate[here] * mm(normed_product, triangle_out[...], 1, 0)
        normed_late = layer_norm(late).astype(BF16)
        hidden = jnp.maximum(mm(normed_late, transition_up[...], 1, 0), 0.0).astype(BF16)
        held[here] = (late + mm(hidden, transition_down[...], 1, 0)).astype(BF16)
        copies.append(pltpu.make_async_copy(held.at[here], out.at[here], left.at[k]))
        copies[-1].start()
    for copy in copies:
        copy.wait()


def per_device(
    sequence,
    pair_state,
    residue_mask,
    chain_index,
    attention_in,
    attention_out,
    bias_weight,
    chain_bias,
    outer_in,
    outer_out,
    triangle_in,
    triangle_out,
    transition_up,
    transition_down,
):
    rows_here, cols_here, channels = pair_state.shape
    length_all = residue_mask.shape[0]
    pairs_here = rows_here * cols_here
    row_index = lax.axis_index(ROW)
    col_index = lax.axis_index("col")
    row_count = lax.axis_size(ROW)
    col_count = lax.axis_size("col")
    row_start = row_index * rows_here
    col_start = col_index * cols_here

    group = channels // col_count
    heads_here = bias_weight.shape[1] // col_count

    weights = jnp.transpose(attention_in, (1, 2, 0)).reshape(-1, sequence.shape[1])
    key_values, query, gate, sequence_near = local_kernel(
        project_body,
        (
            pltpu.VMEM((row_count, rows_here, LANES), BF16),
            pltpu.VMEM((rows_here, LANES), F32),
            pltpu.VMEM((rows_here, LANES), F32),
            pltpu.VMEM(sequence.shape, BF16),
        ),
        "project",
        sequence,
        weights,
        scratch=(pltpu.VMEM(weights.shape, BF16), pltpu.SemaphoreType.DMA((2,))),
        far=True,
    )
    key_values_all = exchange(key_values, ROW)

    bias_in = jnp.transpose(bias_weight)
    triangle = jnp.transpose(triangle_in, (1, 0, 2))
    kept = dict(
        pair=pair_state,
        mask=residue_mask.reshape(1, -1),
        chain=chain_index.reshape(1, -1),
        attention_out=attention_out,
        outer_in=outer_in,
        outer_out=outer_out,
        triangle_out=triangle_out,
        transition_up=transition_up,
        transition_down=transition_down,
    )
    few = rows_here // I_PARTS
    near = local_kernel(
        prepare_body,
        (
            *[pltpu.VMEM(kept[k].shape, kept[k].dtype) for k in KEPT],
            pltpu.VMEM((col_count, heads_here * GROUPS, LANES), F32),
            pltpu.VMEM((col_count, 2 * group, channels), BF16),
            pltpu.VMEM((col_count, 2 * group, channels), BF16),
            pltpu.VMEM((channels, channels), BF16),
            pltpu.VMEM((1, pairs_here), F32),
            pltpu.VMEM((2 * group * rows_here,) * 2, BF16),
            pltpu.VMEM((group * rows_here, K_PARTS * group * rows_here), BF16),
        ),
        "prepare",
        row_start.reshape(1),
        col_start.reshape(1),
        *[kept[k] for k in KEPT],
        bias_in,
        triangle,
        scalars=2,
        scratch=(
            pltpu.VMEM(bias_in.shape, BF16),
            pltpu.VMEM(triangle.shape, BF16),
            pltpu.VMEM((GROUPS, bias_in.shape[0], LANES), F32),
            pltpu.SemaphoreType.DMA((len(KEPT) + 2,)),
        ),
        far=True,
    )
    near, made = dict(zip(KEPT, near)), near[len(KEPT) :]
    bias_blocks, gates_in, values_in, last_in, pair_live, spread_order, gather_order = made

    key_values_all, bias_blocks = lax.optimization_barrier((key_values_all, bias_blocks))
    bias_blocks = exchange(bias_blocks, "col")
    terms = local_kernel(
        attention_body,
        pltpu.VMEM((col_count, *sequence.shape), BF16),
        "attention",
        row_start.reshape(1),
        col_index.reshape(1),
        chain_bias,
        bias_blocks,
        key_values_all,
        query,
        gate,
        near["mask"],
        near["chain"],
        near["attention_out"],
        scalars=3,
        scratch=(
            pltpu.VMEM((heads_here * rows_here, LANES), F32),
            pltpu.VMEM((rows_here, LANES), F32),
        ),
    )
    terms = exchange(terms, "col")
    width = outer_in.shape[1]
    sequence_out, left_twice, right_copies = local_kernel(
        settle_body,
        (
            jax.ShapeDtypeStruct(sequence.shape, BF16),
            pltpu.VMEM((rows_here, width), F32),
            pltpu.VMEM((row_count, rows_here // 2, width), BF16),
        ),
        "settle",
        terms,
        sequence_near,
        near["outer_in"],
    )
    rights = exchange(right_copies, ROW)
    tiles, pair_mid, out_gate = local_kernel(
        pair_body,
        (
            pltpu.VMEM((col_count, 2 * group, pairs_here), BF16),
            pltpu.VMEM((pairs_here, channels), F32),
            pltpu.VMEM((pairs_here, channels), F32),
        ),
        "pair",
        col_index.reshape(1),
        rights,
        left_twice,
        near["pair"],
        near["outer_out"],
        gates_in,
        values_in,
        last_in,
        pair_live,
        scalars=1,
    )

    tiles = exchange(tiles, "col")
    panels = local_kernel(
        spread_body,
        pltpu.VMEM((row_count, few + rows_here, length_all // K_PARTS), BF16),
        "spread",
        tiles,
        spread_order,
    )
    panels = exchange(panels, ROW)
    product = lax.dot_general(
        panels[:, :few].reshape(-1, length_all // K_PARTS),
        panels[:, few:].reshape(-1, length_all // K_PARTS),
        (((1,), (1,)), ((), ())),
        preferred_element_type=F32,
    ).astype(BF16)
    product = exchange(product.reshape(row_count, few, length_all), ROW)
    product = local_kernel(
        gather_body,
        pltpu.VMEM((col_count, group, pairs_here), BF16),
        "gather",
        product,
        gather_order,
    )
    product = exchange(product, "col").reshape(channels, pairs_here)

    pair_out = local_kernel(
        tail_body,
        jax.ShapeDtypeStruct((pairs_here, channels), BF16),
        "tail",
        product,
        pair_mid,
        out_gate,
        near["triangle_out"],
        near["transition_up"],
        near["transition_down"],
        scratch=(
            pltpu.VMEM((pairs_here, channels), BF16),
            pltpu.SemaphoreType.DMA((pairs_here // LANES,)),
        ),
        out_space=pltpu.HBM,
    ).reshape(rows_here, cols_here, channels)
    return (sequence_out, pair_out)


def solution(mesh):
    finer = Mesh(mesh.devices.reshape(4, 8, mesh.shape["col"]), ("row_0", "row_1", "col"))
    placed = (
        P(ROW, None),
        P(ROW, "col", None),
        P(),
        P(),
        P(None, None, "col"),
        P("col", None),
        P(),
        P(),
        P(),
        P(),
        P(),
        P(),
        P(),
        P(),
    )
    return jax.shard_map(
        per_device,
        mesh=finer,
        in_specs=placed,
        out_specs=(P(ROW, None), P(ROW, "col", None)),
        check_vma=False,
    )
```

```python
import math

import jax
import jax.numpy as jnp
from jax import lax
from jax.experimental import pallas as pl
from jax.experimental.pallas import tpu as pltpu
from jax.sharding import Mesh
from jax.sharding import PartitionSpec as P

ROW = ("row_0", "row_1")
BF16 = jnp.bfloat16
F32 = jnp.float32
K_PARTS = 2
I_PARTS = 2
TAIL_PARTS = 2
KEPT = (
    "pair",
    "attention_out",
    "outer_in",
    "outer_out",
    "triangle_out",
    "transition_up",
    "transition_down",
)
LANES = 128
GROUPS = 4


def exchange(blocks, axis):
    return lax.all_to_all(blocks, axis, split_axis=0, concat_axis=0, tiled=True)


def from_everyone(value, axis):
    copies = jnp.broadcast_to(value, (lax.axis_size(axis), *value.shape))
    return exchange(copies, axis)


def layer_norm(values, axis=-1):
    center = values - jnp.mean(values, axis=axis, keepdims=True)
    spread = jnp.mean(center * center, axis=axis, keepdims=True)
    return center * lax.rsqrt(spread + 1e-05)


def local_kernel(body, out_shape, name, *operands, scalars=0, scratch=(), far=False):
    space = pltpu.HBM if far else pltpu.VMEM
    spaces = [pltpu.SMEM if k < scalars else space for k in range(len(operands))]
    held = [
        pltpu.with_memory_space_constraint(x, space) if space is pltpu.VMEM else x
        for x, space in zip(operands, spaces)
    ]
    in_hbm = lambda x: isinstance(x, jax.ShapeDtypeStruct)
    return pl.pallas_call(
        body,
        out_shape=out_shape,
        in_specs=[pl.BlockSpec(memory_space=space) for space in spaces],
        out_specs=jax.tree.map(
            lambda x: pl.BlockSpec(memory_space=pltpu.HBM if in_hbm(x) else pltpu.VMEM), out_shape
        ),
        scratch_shapes=scratch,
        name=name,
    )(*held)


def fetch(sources, targets, arrived):
    copies = [
        pltpu.make_async_copy(source, target, arrived.at[k])
        for k, (source, target) in enumerate(zip(sources, targets))
    ]
    for copy in copies:
        copy.start()
    return copies


def mm(a, b, over_a, over_b):
    return lax.dot_general(a, b, (((over_a,), (over_b,)), ((), ())), preferred_element_type=F32)


def turn_lanes(value, groups):
    steps = groups % GROUPS
    return pltpu.roll(value, steps * (LANES // GROUPS), 1) if steps else value


def regroup(pick, shape):
    group = lax.broadcasted_iota(jnp.int32, shape, 1) // (LANES // GROUPS)
    tile = pick(0)
    for k in range(1, GROUPS):
        tile = jnp.where(group == k, pick(k), tile)
    return tile


def project_body(sequence, weights, key_values, query, gate, near, held, arrived):
    halves = [pl.ds(k * LANES, LANES) for k in range(2)]
    first_copy, *weight_copies = fetch(
        (sequence, *[weights.at[half] for half in halves]),
        (near, *[held.at[half] for half in halves]),
        arrived,
    )
    first_copy.wait()
    normed = layer_norm(near[...].astype(F32)).astype(BF16)
    projected = []
    for half, copy in zip(halves, weight_copies):
        copy.wait()
        projected.append(mm(normed, held[half], 1, 1))
    head, rest = projected
    rows = head.shape[0]
    first = lax.broadcasted_iota(jnp.int32, (rows, LANES), 1) < LANES // 2
    both = jnp.where(first, pltpu.roll(head, LANES // 2, 1), pltpu.roll(rest, LANES // 2, 1))
    key_values[...] = jnp.broadcast_to(both.astype(BF16)[None], key_values.shape)
    query[...] = jnp.where(first, head, 0.0).astype(BF16).astype(F32)
    gate[...] = jnp.where(first, 0.0, jax.nn.sigmoid(rest))


def prepare_body(row_start, col, chain_bias, *refs):
    count = len(KEPT)
    sources, targets = refs[: count + 4], refs[count + 4 : 2 * count + 4]
    blocks, gates_in, values_in, last_in, live, spread_order, gather_order, extra, pick = refs[
        2 * count + 4 : -6
    ]
    mask_near, chain_near, bias_near, triangle_near, turned_bias, arrived = refs[-6:]
    copies = fetch(
        sources, (*targets, mask_near, chain_near, bias_near, triangle_near), arrived
    )
    near = dict(zip(KEPT, targets))
    landed = dict(zip((*KEPT, "mask", "chain", "bias_in", "triangle"), copies))

    size = spread_order.shape[0]
    n = lax.broadcasted_iota(jnp.int32, spread_order.shape, 0)
    m = lax.broadcasted_iota(jnp.int32, spread_order.shape, 1)
    rows = live.shape[1] // (LANES // GROUPS)
    wanted = n % rows * (size // rows) + n // rows
    spread_order[...] = jnp.where(m == wanted, 1.0, 0.0).astype(BF16)
    size = gather_order.shape[0]
    group, few = size // rows, rows // I_PARTS
    n = lax.broadcasted_iota(jnp.int32, gather_order.shape, 0)
    m = lax.broadcasted_iota(jnp.int32, gather_order.shape, 1)
    i, c = n // group, n % group
    wanted = (i // few * group + c) * few + i % few
    gather_order[...] = jnp.where(m % size == wanted, 1.0, 0.0).astype(BF16)

    n = lax.broadcasted_iota(jnp.int32, pick.shape, 0)
    m = lax.broadcasted_iota(jnp.int32, pick.shape, 1)
    pick[...] = jnp.where(m == col[0] * pick.shape[0] + n, 1.0, 0.0).astype(BF16)

    landed["pair"].wait()
    landed["bias_in"].wait()
    wide = near["pair"][...].astype(F32)
    turned = jnp.concatenate([wide[GROUPS * (p % GROUPS) + p // GROUPS] for p in range(rows)], axis=0)
    normed = layer_norm(turned).astype(BF16)
    bias = mm(bias_near[...], normed, 1, 1)
    columns = blocks.shape[0]
    for t in range(GROUPS):
        turned_bias[t] = bias[:, t * LANES : (t + 1) * LANES]
        for h in range(2):
            blocks[:, h * GROUPS + t, :] = turned_bias[t, pl.ds(h, columns, stride=2), :]

    landed["mask"].wait()
    mask = mask_near[...].astype(F32).astype(BF16)
    length = mask.shape[1]
    residue = lax.broadcasted_iota(jnp.int32, (length, live.shape[1]), 0)
    pair = lax.broadcasted_iota(jnp.int32, (length, live.shape[1]), 1)
    of_row = jnp.where(residue == row_start[0] + pair // (LANES // GROUPS), 1.0, 0.0).astype(BF16)
    of_col = jnp.where(residue == col[0] * (LANES // GROUPS) + pair % (LANES // GROUPS), 1.0, 0.0).astype(BF16)
    mask = jnp.broadcast_to(mask, (8, length))
    live[...] = (mm(mask, of_row, 1, 0) * mm(mask, of_col, 1, 0))[:1]

    landed["chain"].wait()
    eight = blocks.shape[1]
    four = eight // 2
    position = lax.broadcasted_iota(jnp.int32, (eight, length), 1)
    row = lax.broadcasted_iota(jnp.int32, (eight, length), 0)
    chains = jnp.broadcast_to(chain_near[...].astype(F32), (eight, length))
    kept = jnp.broadcast_to(mask_near[...], (eight, length)) == 1
    offset = jnp.where(row < four, chain_bias[2 * col[0]], chain_bias[2 * col[0] + 1])
    for g in range(GROUPS):
        here = position == row_start[0] + g * four + row % four
        own_chain = jnp.sum(jnp.where(here, chains, 0.0), axis=1, keepdims=True)
        added = jnp.where(chains == own_chain, offset, 0.0)
        extra[g * eight : (g + 1) * eight, :] = jnp.where(kept | here, added, -jnp.inf)

    landed["triangle"].wait()
    half = gates_in.shape[1] // 2
    for k, target in enumerate((gates_in, values_in, gates_in, values_in)):
        side = half * (k // 2)
        across = jnp.transpose(triangle_near[k].astype(F32)).astype(BF16)
        target[:, side : side + half, :] = across.reshape(target.shape[0], half, LANES)
    last_in[...] = triangle_near[4]
    for name in KEPT:
        if name != "pair":
            landed[name].wait()


def attention_body(blocks, extra, key_values, query, gate, attention_out, copies, spread, joined):
    count, eight, _ = blocks.shape
    four = eight // 2
    length = count * (LANES // GROUPS)
    lane = lax.broadcasted_iota(jnp.int32, (four, LANES), 1)
    for g in range(GROUPS):
        taken = query[g * four : (g + 1) * four, :]
        for h in range(2):
            own = (lane >= h * (LANES // 4)) & (lane < (h + 1) * (LANES // 4))
            spread[g * eight + h * four : g * eight + (h + 1) * four, :] = jnp.where(own, taken, 0.0)
    everyone = key_values[...].reshape(length, LANES)
    raw = mm(spread[...].astype(BF16), everyone, 1, 1)
    raw = raw * (1.0 / math.sqrt(LANES // 4))
    biases = []
    for g in range(GROUPS):
        pieces = []
        for tile in range(count // GROUPS):
            pieces.append(
                regroup(
                    lambda k, tile=tile, g=g: turn_lanes(blocks[GROUPS * tile + k], k - g),
                    (eight, LANES),
                )
            )
        biases.append(jnp.concatenate(pieces, axis=1))
    scores = raw + jnp.concatenate(biases, axis=0) + extra[...]
    raised = jnp.exp(scores - jnp.max(scores, axis=1, keepdims=True))
    weights = [raised / jnp.sum(raised, axis=1, keepdims=True)]
    mixed = mm(jnp.concatenate(weights, axis=0).astype(BF16), everyone, 1, 0)
    for g in range(GROUPS):
        upper = mixed[g * eight : g * eight + four]
        lower = mixed[g * eight + four : (g + 1) * eight]
        joined[g * four : (g + 1) * four, :] = jnp.where(lane < LANES * 3 // 4, upper, lower)
    gated = pltpu.roll(gate[...] * joined[...], LANES // 2, 1)[:, : LANES // 2].astype(BF16)
    terms = mm(gated, attention_out[...], 1, 0).astype(BF16)
    copies[...] = jnp.broadcast_to(terms[None], copies.shape)


def spread_body(tiles, order, panels):
    count, chans, pairs = tiles.shape
    rows = pairs // (LANES // GROUPS)
    per = count // GROUPS
    by_row = []
    for i in range(rows):
        at, g = i // GROUPS * LANES, i % GROUPS
        by_row.append(
            jnp.concatenate(
                [
                    regroup(
                        lambda k, tile=tile, g=g, at=at: turn_lanes(
                            tiles[GROUPS * tile + k, :, at : at + LANES].astype(F32), k - g
                        ),
                        (chans, LANES),
                    )
                    for tile in range(per)
                ],
                axis=1,
            )
        )
    turned = mm(order[...], jnp.concatenate(by_row, axis=0).astype(BF16), 1, 0).astype(BF16)
    half = chans // 2
    few = rows // I_PARTS
    wide = turned.shape[1] // K_PARTS
    for k in range(K_PARTS):
        for i in range(I_PARTS):
            for c in range(half):
                block = (k * I_PARTS + i) * half + c
                at = c * rows + i * few
                panels[block, :few, :] = turned[at : at + few, k * wide : (k + 1) * wide]
                at = (half + c) * rows
                panels[block, few:, :] = turned[at : at + rows, k * wide : (k + 1) * wide]


def gather_body(parts, order, blocks):
    total, few, length = parts.shape
    count, group, pairs = blocks.shape
    rows = pairs // (LANES // GROUPS)
    summed = mm(order[...], parts[...].reshape(total * few, length), 1, 0)
    for q in range(count):
        tile, s = q // GROUPS, q % GROUPS
        pieces = []
        for t in range(rows // GROUPS):
            pieces.append(
                regroup(
                    lambda k, t=t, tile=tile, s=s: turn_lanes(
                        summed[
                            (GROUPS * t + k) * group : (GROUPS * t + k + 1) * group,
                            tile * LANES : (tile + 1) * LANES,
                        ],
                        k - s,
                    ),
                    (group, LANES),
                )
            )
        blocks[q] = jnp.concatenate(pieces, axis=1).astype(BF16)


def settle_body(terms, sequence, outer_in, sequence_out, left_twice, right_copies):
    update = jnp.sum(terms[...].astype(F32), axis=0)
    summed = (sequence[...].astype(F32) + update).astype(BF16)
    sequence_out[...] = summed
    normed = layer_norm(summed.astype(F32)).astype(BF16)
    outer_rows = mm(normed, outer_in[...], 1, 0).astype(BF16).astype(F32)
    rows, width = outer_rows.shape
    half = width // 2
    first = lax.broadcasted_iota(jnp.int32, (rows, width), 1) < half
    turned = pltpu.roll(outer_rows, half, 1)
    left_twice[...] = jnp.where(first, outer_rows, turned)
    packed = jnp.where(first[: rows // 2], turned[: rows // 2], outer_rows[rows // 2 :])
    right_copies[...] = jnp.broadcast_to(packed.astype(BF16)[None], right_copies.shape)


def pair_body(
    sequence_near,
    rights,
    pick,
    left_twice,
    pair,
    outer_out,
    gates_in,
    values_in,
    last_in,
    live,
    sequence_out,
    tiles,
    mid,
    out_gate,
    left,
):
    sent = pltpu.make_async_copy(sequence_near, sequence_out, left.at[0])
    sent.start()
    rows, cols, channels = pair.shape
    half = channels // 2
    taken = mm(pick[...], rights[...].reshape(-1, channels), 1, 0)
    taken = taken.reshape(cols // rows, rows // 2, channels)
    first = lax.broadcasted_iota(jnp.int32, (rows // 2, channels), 1) < half
    pieces = []
    for k in range(cols // rows):
        turned = pltpu.roll(taken[k], half, 1)
        pieces.append(jnp.where(first, taken[k], turned))
        pieces.append(jnp.where(first, turned, taken[k]))
    right_twice = jnp.concatenate(pieces, axis=0)
    left = left_twice[...][:, None, :]
    right = right_twice[None, :, :]
    lane = lax.broadcasted_iota(jnp.int32, (rows, cols, channels), 2)
    feat = jnp.where(lane < half, left * right, left - right).astype(BF16)
    feat = feat.reshape(rows * cols, channels)
    pair_mid = pair[...].astype(F32).reshape(rows * cols, channels) + mm(feat, outer_out[...], 1, 0)
    mid[...] = pair_mid
    normed = layer_norm(pair_mid).astype(BF16)
    flat = (-1, channels)
    opened = jax.nn.sigmoid(mm(gates_in[...].reshape(flat), normed, 1, 1))
    operands = opened * mm(values_in[...].reshape(flat), normed, 1, 1) * live[...]
    tiles[...] = operands.astype(BF16).reshape(tiles.shape)
    out_gate[...] = jax.nn.sigmoid(mm(normed, last_in[...], 1, 0))
    sent.wait()


def tail_body(product, mid, out_gate, triangle_out, transition_up, transition_down, out, held, left):
    normed_product = layer_norm(product[...].astype(F32), axis=0)
    normed_product = jnp.transpose(normed_product).astype(BF16)
    late = mid[...] + out_gate[...] * mm(normed_product, triangle_out[...], 1, 0)
    normed_late = layer_norm(late).astype(BF16)
    hidden = jnp.maximum(mm(normed_late, transition_up[...], 1, 0), 0.0).astype(BF16)
    copies = []
    part = mid.shape[0] // TAIL_PARTS
    for k in range(TAIL_PARTS):
        here = slice(k * part, (k + 1) * part)
        held[here] = (late[here] + mm(hidden[here], transition_down[...], 1, 0)).astype(BF16)
        copies.append(pltpu.make_async_copy(held.at[here], out.at[here], left.at[k]))
        copies[-1].start()
    for copy in copies:
        copy.wait()


def per_device(
    sequence,
    pair_state,
    residue_mask,
    chain_index,
    attention_in,
    attention_out,
    bias_weight,
    chain_bias,
    outer_in,
    outer_out,
    triangle_in,
    triangle_out,
    transition_up,
    transition_down,
):
    rows_here, cols_here, channels = pair_state.shape
    length_all = residue_mask.shape[0]
    pairs_here = rows_here * cols_here
    row_index = lax.axis_index(ROW)
    col_index = lax.axis_index("col")
    row_count = lax.axis_size(ROW)
    col_count = lax.axis_size("col")
    row_start = row_index * rows_here

    group = channels // col_count
    heads_here = bias_weight.shape[1] // col_count

    weights = jnp.transpose(attention_in, (1, 2, 0)).reshape(-1, sequence.shape[1])
    key_values, query, gate, sequence_near = local_kernel(
        project_body,
        (
            pltpu.VMEM((row_count, rows_here, LANES), BF16),
            pltpu.VMEM((rows_here, LANES), F32),
            pltpu.VMEM((rows_here, LANES), F32),
            pltpu.VMEM(sequence.shape, BF16),
        ),
        "project",
        sequence,
        weights,
        scratch=(pltpu.VMEM(weights.shape, BF16), pltpu.SemaphoreType.DMA((3,))),
        far=True,
    )
    key_values_all = exchange(key_values, ROW)

    bias_in = jnp.transpose(bias_weight)
    triangle = jnp.transpose(triangle_in, (1, 0, 2))
    kept = dict(
        pair=pair_state,
        attention_out=attention_out,
        outer_in=outer_in,
        outer_out=outer_out,
        triangle_out=triangle_out,
        transition_up=transition_up,
        transition_down=transition_down,
    )
    few = rows_here // I_PARTS
    near = local_kernel(
        prepare_body,
        (
            *[pltpu.VMEM(kept[k].shape, kept[k].dtype) for k in KEPT],
            pltpu.VMEM((col_count, heads_here * GROUPS, LANES), F32),
            pltpu.VMEM((col_count, 2 * group, channels), BF16),
            pltpu.VMEM((col_count, 2 * group, channels), BF16),
            pltpu.VMEM((channels, channels), BF16),
            pltpu.VMEM((1, pairs_here), F32),
            pltpu.VMEM((2 * group * rows_here,) * 2, BF16),
            pltpu.VMEM((group * rows_here, K_PARTS * group * rows_here), BF16),
            pltpu.VMEM((heads_here * rows_here, length_all), F32),
            pltpu.VMEM((cols_here // 2, length_all // 2), BF16),
        ),
        "prepare",
        row_start.reshape(1),
        col_index.reshape(1),
        chain_bias,
        *[kept[k] for k in KEPT],
        residue_mask.reshape(1, -1),
        chain_index.reshape(1, -1),
        bias_in,
        triangle,
        scalars=3,
        scratch=(
            pltpu.VMEM((1, length_all), jnp.int32),
            pltpu.VMEM((1, length_all), jnp.int32),
            pltpu.VMEM(bias_in.shape, BF16),
            pltpu.VMEM(triangle.shape, BF16),
            pltpu.VMEM((GROUPS, bias_in.shape[0], LANES), F32),
            pltpu.SemaphoreType.DMA((len(KEPT) + 4,)),
        ),
        far=True,
    )
    near, made = dict(zip(KEPT, near)), near[len(KEPT) :]
    bias_blocks, gates_in, values_in, last_in, pair_live, spread_order, gather_order, extra, pick = made

    key_values_all, bias_blocks = lax.optimization_barrier((key_values_all, bias_blocks))
    bias_blocks = exchange(bias_blocks, "col")
    terms = local_kernel(
        attention_body,
        pltpu.VMEM((col_count, *sequence.shape), BF16),
        "attention",
        bias_blocks,
        extra,
        key_values_all,
        query,
        gate,
        near["attention_out"],
        scratch=(
            pltpu.VMEM((heads_here * rows_here, LANES), F32),
            pltpu.VMEM((rows_here, LANES), F32),
        ),
    )
    terms = exchange(terms, "col")
    width = outer_in.shape[1]
    sequence_summed, left_twice, right_copies = local_kernel(
        settle_body,
        (
            pltpu.VMEM(sequence.shape, BF16),
            pltpu.VMEM((rows_here, width), F32),
            pltpu.VMEM((row_count, rows_here // 2, width), BF16),
        ),
        "settle",
        terms,
        sequence_near,
        near["outer_in"],
    )
    rights = exchange(right_copies, ROW)
    sequence_out, tiles, pair_mid, out_gate = local_kernel(
        pair_body,
        (
            jax.ShapeDtypeStruct(sequence.shape, BF16),
            pltpu.VMEM((col_count, 2 * group, pairs_here), BF16),
            pltpu.VMEM((pairs_here, channels), F32),
            pltpu.VMEM((pairs_here, channels), F32),
        ),
        "pair",
        sequence_summed,
        rights,
        pick,
        left_twice,
        near["pair"],
        near["outer_out"],
        gates_in,
        values_in,
        last_in,
        pair_live,
        scratch=(pltpu.SemaphoreType.DMA((1,)),),
    )

    tiles = exchange(tiles, "col")
    panels = local_kernel(
        spread_body,
        pltpu.VMEM((row_count, few + rows_here, length_all // K_PARTS), BF16),
        "spread",
        tiles,
        spread_order,
    )
    panels = exchange(panels, ROW)
    product = lax.dot_general(
        panels[:, :few].reshape(-1, length_all // K_PARTS),
        panels[:, few:].reshape(-1, length_all // K_PARTS),
        (((1,), (1,)), ((), ())),
        preferred_element_type=F32,
    ).astype(BF16)
    product = exchange(product.reshape(row_count, few, length_all), ROW)
    product = local_kernel(
        gather_body,
        pltpu.VMEM((col_count, group, pairs_here), BF16),
        "gather",
        product,
        gather_order,
    )
    product = exchange(product, "col").reshape(channels, pairs_here)

    pair_out = local_kernel(
        tail_body,
        jax.ShapeDtypeStruct((pairs_here, channels), BF16),
        "tail",
        product,
        pair_mid,
        out_gate,
        near["triangle_out"],
        near["transition_up"],
        near["transition_down"],
        scratch=(
            pltpu.VMEM((pairs_here, channels), BF16),
            pltpu.SemaphoreType.DMA((TAIL_PARTS,)),
        ),
    ).reshape(rows_here, cols_here, channels)
    return (sequence_out, pair_out)


def solution(mesh):
    finer = Mesh(mesh.devices.reshape(4, 8, mesh.shape["col"]), ("row_0", "row_1", "col"))
    placed = (
        P(ROW, None),
        P(ROW, "col", None),
        P(),
        P(),
        P(None, None, "col"),
        P("col", None),
        P(),
        P(),
        P(),
        P(),
        P(),
        P(),
        P(),
        P(),
    )
    return jax.shard_map(
        per_device,
        mesh=finer,
        in_specs=placed,
        out_specs=(P(ROW, None), P(ROW, "col", None)),
        check_vma=False,
    )
```

```python
import math

import jax
import jax.numpy as jnp
from jax import lax
from jax.experimental import pallas as pl
from jax.experimental.pallas import tpu as pltpu
from jax.sharding import Mesh
from jax.sharding import PartitionSpec as P

ROW = ("row_0", "row_1")
ROW_TURN = 20
COL_TURN = 1
BF16 = jnp.bfloat16
F32 = jnp.float32
K_PARTS = 2
I_PARTS = 2
TAIL_PARTS = 4
KEPT = (
    "pair",
    "attention_out",
    "outer_in",
    "outer_out",
    "triangle_out",
    "transition_up",
    "transition_down",
)
LANES = 128
GROUPS = 4


def exchange(blocks, axis):
    rows, cols = lax.axis_size(ROW), lax.axis_size("col")
    if axis == "col":
        groups = [[r * cols + (p ^ COL_TURN) for p in range(cols)] for r in range(rows)]
    else:
        groups = [[(p ^ ROW_TURN) * cols + q for p in range(rows)] for q in range(cols)]
    return lax.all_to_all(
        blocks, (*ROW, "col"), split_axis=0, concat_axis=0, tiled=True, axis_index_groups=groups
    )


def layer_norm(values, axis=-1):
    center = values - jnp.mean(values, axis=axis, keepdims=True)
    spread = jnp.mean(center * center, axis=axis, keepdims=True)
    return center * lax.rsqrt(spread + 1e-05)


def local_kernel(body, out_shape, name, *operands, scalars=0, scratch=(), far=False):
    space = pltpu.HBM if far else pltpu.VMEM
    spaces = [pltpu.SMEM if k < scalars else space for k in range(len(operands))]
    held = [
        pltpu.with_memory_space_constraint(x, space) if space is pltpu.VMEM else x
        for x, space in zip(operands, spaces)
    ]
    in_hbm = lambda x: isinstance(x, jax.ShapeDtypeStruct)
    return pl.pallas_call(
        body,
        out_shape=out_shape,
        in_specs=[pl.BlockSpec(memory_space=space) for space in spaces],
        out_specs=jax.tree.map(
            lambda x: pl.BlockSpec(memory_space=pltpu.HBM if in_hbm(x) else pltpu.VMEM), out_shape
        ),
        scratch_shapes=scratch,
        name=name,
    )(*held)


def fetch(sources, targets, arrived):
    copies = [
        pltpu.make_async_copy(source, target, arrived.at[k])
        for k, (source, target) in enumerate(zip(sources, targets))
    ]
    for copy in copies:
        copy.start()
    return copies


def mm(a, b, over_a, over_b):
    return lax.dot_general(a, b, (((over_a,), (over_b,)), ((), ())), preferred_element_type=F32)


def turn_lanes(value, groups):
    steps = groups % GROUPS
    return pltpu.roll(value, steps * (LANES // GROUPS), 1) if steps else value


def regroup(pick, shape):
    group = lax.broadcasted_iota(jnp.int32, shape, 1) // (LANES // GROUPS)
    tile = pick(0)
    for k in range(1, GROUPS):
        tile = jnp.where(group == k, pick(k), tile)
    return tile


def project_body(sequence, weights, key_values, query, gate, near, held, arrived):
    halves = [pl.ds(k * LANES, LANES) for k in range(2)]
    first_copy, *weight_copies = fetch(
        (sequence, *[weights.at[half] for half in halves]),
        (near, *[held.at[half] for half in halves]),
        arrived,
    )
    first_copy.wait()
    normed = layer_norm(near[...].astype(F32)).astype(BF16)
    projected = []
    for half, copy in zip(halves, weight_copies):
        copy.wait()
        projected.append(mm(normed, held[half], 1, 1))
    head, rest = projected
    rows = head.shape[0]
    first = lax.broadcasted_iota(jnp.int32, (rows, LANES), 1) < LANES // 2
    both = jnp.where(first, pltpu.roll(head, LANES // 2, 1), pltpu.roll(rest, LANES // 2, 1))
    key_values[...] = jnp.broadcast_to(both.astype(BF16)[None], key_values.shape)
    query[...] = jnp.where(first, head, 0.0).astype(BF16).astype(F32)
    gate[...] = jnp.where(first, 0.0, jax.nn.sigmoid(rest))


def prepare_body(row_start, col, chain_bias, *refs):
    count = len(KEPT)
    sources, targets = refs[: count + 4], refs[count + 4 : 2 * count + 4]
    blocks, gates_in, values_in, last_in, live, spread_order, gather_order, extra, pick = refs[
        2 * count + 4 : -6
    ]
    mask_near, chain_near, bias_near, triangle_near, turned_bias, arrived = refs[-6:]
    copies = fetch(
        sources, (*targets, mask_near, chain_near, bias_near, triangle_near), arrived
    )
    near = dict(zip(KEPT, targets))
    landed = dict(zip((*KEPT, "mask", "chain", "bias_in", "triangle"), copies))

    size = spread_order.shape[0]
    n = lax.broadcasted_iota(jnp.int32, spread_order.shape, 0)
    m = lax.broadcasted_iota(jnp.int32, spread_order.shape, 1)
    rows = live.shape[1] // (LANES // GROUPS)
    wanted = n % rows * (size // rows) + n // rows
    spread_order[...] = jnp.where(m == wanted, 1.0, 0.0).astype(BF16)
    size = gather_order.shape[0]
    group, few = size // rows, rows // I_PARTS
    n = lax.broadcasted_iota(jnp.int32, gather_order.shape, 0)
    m = lax.broadcasted_iota(jnp.int32, gather_order.shape, 1)
    i, c = n // group, n % group
    wanted = (i // few * group + c) * few + i % few
    gather_order[...] = jnp.where(m % size == wanted, 1.0, 0.0).astype(BF16)

    n = lax.broadcasted_iota(jnp.int32, pick.shape, 0)
    m = lax.broadcasted_iota(jnp.int32, pick.shape, 1)
    pick[...] = jnp.where(m == (col[0] ^ (ROW_TURN // 2)) * pick.shape[0] + n, 1.0, 0.0).astype(BF16)

    landed["pair"].wait()
    landed["bias_in"].wait()
    wide = near["pair"][...].astype(F32)
    turned = jnp.concatenate([wide[GROUPS * (p % GROUPS) + p // GROUPS] for p in range(rows)], axis=0)
    normed = layer_norm(turned).astype(BF16)
    heads = bias_near.shape[0]
    n = lax.broadcasted_iota(jnp.int32, (heads, heads), 0)
    m = lax.broadcasted_iota(jnp.int32, (heads, heads), 1)
    by_place = jnp.where(m == n ^ (2 * COL_TURN), 1.0, 0.0).astype(BF16)
    bias = mm(mm(by_place, bias_near[...], 1, 0).astype(BF16), normed, 1, 1)
    columns = blocks.shape[0]
    for t in range(GROUPS):
        turned_bias[t] = bias[:, t * LANES : (t + 1) * LANES]
        for h in range(2):
            blocks[:, h * GROUPS + t, :] = turned_bias[t, pl.ds(h, columns, stride=2), :]

    landed["mask"].wait()
    mask = mask_near[...].astype(F32).astype(BF16)
    length = mask.shape[1]
    residue = lax.broadcasted_iota(jnp.int32, (length, live.shape[1]), 0)
    pair = lax.broadcasted_iota(jnp.int32, (length, live.shape[1]), 1)
    of_row = jnp.where(residue == row_start[0] + pair // (LANES // GROUPS), 1.0, 0.0).astype(BF16)
    of_col = jnp.where(residue == col[0] * (LANES // GROUPS) + pair % (LANES // GROUPS), 1.0, 0.0).astype(BF16)
    mask = jnp.broadcast_to(mask, (8, length))
    live[...] = (mm(mask, of_row, 1, 0) * mm(mask, of_col, 1, 0))[:1]

    landed["chain"].wait()
    eight = blocks.shape[1]
    four = eight // 2
    position = lax.broadcasted_iota(jnp.int32, (eight, length), 1)
    row = lax.broadcasted_iota(jnp.int32, (eight, length), 0)
    chains = jnp.broadcast_to(chain_near[...].astype(F32), (eight, length))
    kept = jnp.broadcast_to(mask_near[...], (eight, length)) == 1
    offset = jnp.where(row < four, chain_bias[2 * col[0]], chain_bias[2 * col[0] + 1])
    for g in range(GROUPS):
        here = position == row_start[0] + g * four + row % four
        own_chain = jnp.sum(jnp.where(here, chains, 0.0), axis=1, keepdims=True)
        added = jnp.where(chains == own_chain, offset, 0.0)
        extra[g * eight : (g + 1) * eight, :] = jnp.where(kept | here, added, -jnp.inf)

    landed["triangle"].wait()
    half = gates_in.shape[1] // 2
    for k, target in enumerate((gates_in, values_in, gates_in, values_in)):
        side = half * (k // 2)
        across = jnp.transpose(triangle_near[k].astype(F32)).astype(BF16)
        target[:, side : side + half, :] = across.reshape(target.shape[0], half, LANES)
    last_in[...] = triangle_near[4]
    for name in KEPT:
        if name != "pair":
            landed[name].wait()


def attention_body(blocks, extra, key_values, query, gate, attention_out, copies, spread, joined):
    count, eight, _ = blocks.shape
    four = eight // 2
    length = count * (LANES // GROUPS)
    lane = lax.broadcasted_iota(jnp.int32, (four, LANES), 1)
    for g in range(GROUPS):
        taken = query[g * four : (g + 1) * four, :]
        for h in range(2):
            own = (lane >= h * (LANES // 4)) & (lane < (h + 1) * (LANES // 4))
            spread[g * eight + h * four : g * eight + (h + 1) * four, :] = jnp.where(own, taken, 0.0)
    everyone = jnp.concatenate([key_values[r ^ ROW_TURN] for r in range(key_values.shape[0])], axis=0)
    raw = mm(spread[...].astype(BF16), everyone, 1, 1)
    raw = raw * (1.0 / math.sqrt(LANES // 4))
    biases = []
    for g in range(GROUPS):
        pieces = []
        for tile in range(count // GROUPS):
            pieces.append(
                regroup(
                    lambda k, tile=tile, g=g: turn_lanes(blocks[(GROUPS * tile + k) ^ COL_TURN], k - g),
                    (eight, LANES),
                )
            )
        biases.append(jnp.concatenate(pieces, axis=1))
    scores = raw + jnp.concatenate(biases, axis=0) + extra[...]
    raised = jnp.exp(scores - jnp.max(scores, axis=1, keepdims=True))
    weights = [raised / jnp.sum(raised, axis=1, keepdims=True)]
    mixed = mm(jnp.concatenate(weights, axis=0).astype(BF16), everyone, 1, 0)
    for g in range(GROUPS):
        upper = mixed[g * eight : g * eight + four]
        lower = mixed[g * eight + four : (g + 1) * eight]
        joined[g * four : (g + 1) * four, :] = jnp.where(lane < LANES * 3 // 4, upper, lower)
    gated = pltpu.roll(gate[...] * joined[...], LANES // 2, 1)[:, : LANES // 2].astype(BF16)
    terms = mm(gated, attention_out[...], 1, 0).astype(BF16)
    copies[...] = jnp.broadcast_to(terms[None], copies.shape)


def spread_body(tiles, order, panels):
    count, chans, pairs = tiles.shape
    rows = pairs // (LANES // GROUPS)
    per = count // GROUPS
    by_row = []
    for i in range(rows):
        at, g = i // GROUPS * LANES, i % GROUPS
        by_row.append(
            jnp.concatenate(
                [
                    regroup(
                        lambda k, tile=tile, g=g, at=at: turn_lanes(
                            tiles[(GROUPS * tile + k) ^ COL_TURN, :, at : at + LANES].astype(F32), k - g
                        ),
                        (chans, LANES),
                    )
                    for tile in range(per)
                ],
                axis=1,
            )
        )
    turned = mm(order[...], jnp.concatenate(by_row, axis=0).astype(BF16), 1, 0).astype(BF16)
    half = chans // 2
    few = rows // I_PARTS
    wide = turned.shape[1] // K_PARTS
    for k in range(K_PARTS):
        for i in range(I_PARTS):
            for c in range(half):
                block = (k * I_PARTS + i) * half + c
                at = c * rows + i * few
                panels[block, :few, :] = turned[at : at + few, k * wide : (k + 1) * wide]
                at = (half + c) * rows
                panels[block, few:, :] = turned[at : at + rows, k * wide : (k + 1) * wide]


def gather_body(parts, order, blocks):
    total, few, length = parts.shape
    count, group, pairs = blocks.shape
    rows = pairs // (LANES // GROUPS)
    summed = mm(order[...], parts[...].reshape(total * few, length), 1, 0)
    for q in range(count):
        place = q ^ COL_TURN ^ (ROW_TURN // 2)
        tile, s = place // GROUPS, place % GROUPS
        pieces = []
        for t in range(rows // GROUPS):
            pieces.append(
                regroup(
                    lambda k, t=t, tile=tile, s=s: turn_lanes(
                        summed[
                            (GROUPS * t + k) * group : (GROUPS * t + k + 1) * group,
                            tile * LANES : (tile + 1) * LANES,
                        ],
                        k - s,
                    ),
                    (group, LANES),
                )
            )
        blocks[q] = jnp.concatenate(pieces, axis=1).astype(BF16)


def settle_body(terms, sequence, outer_in, sequence_out, left_twice, right_copies):
    update = jnp.sum(terms[...].astype(F32), axis=0)
    summed = (sequence[...].astype(F32) + update).astype(BF16)
    sequence_out[...] = summed
    normed = layer_norm(summed.astype(F32)).astype(BF16)
    outer_rows = mm(normed, outer_in[...], 1, 0).astype(BF16).astype(F32)
    rows, width = outer_rows.shape
    half = width // 2
    first = lax.broadcasted_iota(jnp.int32, (rows, width), 1) < half
    turned = pltpu.roll(outer_rows, half, 1)
    left_twice[...] = jnp.where(first, outer_rows, turned)
    packed = jnp.where(first[: rows // 2], turned[: rows // 2], outer_rows[rows // 2 :])
    right_copies[...] = jnp.broadcast_to(packed.astype(BF16)[None], right_copies.shape)


def pair_body(
    rights,
    pick,
    left_twice,
    pair,
    outer_out,
    gates_in,
    values_in,
    last_in,
    live,
    tiles,
    mid,
    out_gate,
):
    rows, cols, channels = pair.shape
    half = channels // 2
    taken = mm(pick[...], rights[...].reshape(-1, channels), 1, 0)
    taken = taken.reshape(cols // rows, rows // 2, channels)
    first = lax.broadcasted_iota(jnp.int32, (rows // 2, channels), 1) < half
    pieces = []
    for k in range(cols // rows):
        turned = pltpu.roll(taken[k], half, 1)
        pieces.append(jnp.where(first, taken[k], turned))
        pieces.append(jnp.where(first, turned, taken[k]))
    right_twice = jnp.concatenate(pieces, axis=0)
    left = left_twice[...][:, None, :]
    right = right_twice[None, :, :]
    lane = lax.broadcasted_iota(jnp.int32, (rows, cols, channels), 2)
    feat = jnp.where(lane < half, left * right, left - right).astype(BF16)
    feat = feat.reshape(rows * cols, channels)
    pair_mid = pair[...].astype(F32).reshape(rows * cols, channels) + mm(feat, outer_out[...], 1, 0)
    mid[...] = pair_mid
    normed = layer_norm(pair_mid).astype(BF16)
    flat = (-1, channels)
    opened = jax.nn.sigmoid(mm(gates_in[...].reshape(flat), normed, 1, 1))
    operands = opened * mm(values_in[...].reshape(flat), normed, 1, 1) * live[...]
    tiles[...] = operands.astype(BF16).reshape(tiles.shape)
    out_gate[...] = jax.nn.sigmoid(mm(normed, last_in[...], 1, 0))


def tail_body(
    sequence_near,
    product,
    mid,
    out_gate,
    triangle_out,
    transition_up,
    transition_down,
    sequence_out,
    out,
    held,
    left,
):
    copies = [pltpu.make_async_copy(sequence_near, sequence_out, left.at[TAIL_PARTS])]
    copies[0].start()
    normed_product = layer_norm(product[...].astype(F32), axis=0)
    normed_product = jnp.transpose(normed_product).astype(BF16)
    late = mid[...] + out_gate[...] * mm(normed_product, triangle_out[...], 1, 0)
    normed_late = layer_norm(late).astype(BF16)
    hidden = jnp.maximum(mm(normed_late, transition_up[...], 1, 0), 0.0).astype(BF16)
    part = mid.shape[0] // TAIL_PARTS
    for k in range(TAIL_PARTS):
        here = slice(k * part, (k + 1) * part)
        held[here] = (late[here] + mm(hidden[here], transition_down[...], 1, 0)).astype(BF16)
        copies.append(pltpu.make_async_copy(held.at[here], out.at[here], left.at[k]))
        copies[-1].start()
    for copy in copies:
        copy.wait()


def per_device(
    sequence,
    pair_state,
    residue_mask,
    chain_index,
    attention_in,
    attention_out,
    bias_weight,
    chain_bias,
    outer_in,
    outer_out,
    triangle_in,
    triangle_out,
    transition_up,
    transition_down,
):
    rows_here, cols_here, channels = pair_state.shape
    length_all = residue_mask.shape[0]
    pairs_here = rows_here * cols_here
    row_index = lax.axis_index(ROW)
    col_index = lax.axis_index("col")
    row_count = lax.axis_size(ROW)
    col_count = lax.axis_size("col")
    row_start = row_index * rows_here

    group = channels // col_count
    heads_here = bias_weight.shape[1] // col_count

    weights = jnp.transpose(attention_in, (1, 2, 0)).reshape(-1, sequence.shape[1])
    key_values, query, gate, sequence_near = local_kernel(
        project_body,
        (
            pltpu.VMEM((row_count, rows_here, LANES), BF16),
            pltpu.VMEM((rows_here, LANES), F32),
            pltpu.VMEM((rows_here, LANES), F32),
            pltpu.VMEM(sequence.shape, BF16),
        ),
        "project",
        sequence,
        weights,
        scratch=(pltpu.VMEM(weights.shape, BF16), pltpu.SemaphoreType.DMA((3,))),
        far=True,
    )
    key_values_all = exchange(key_values, ROW)

    bias_in = jnp.transpose(bias_weight)
    triangle = jnp.transpose(triangle_in, (1, 0, 2))
    kept = dict(
        pair=pair_state,
        attention_out=attention_out,
        outer_in=outer_in,
        outer_out=outer_out,
        triangle_out=triangle_out,
        transition_up=transition_up,
        transition_down=transition_down,
    )
    few = rows_here // I_PARTS
    near = local_kernel(
        prepare_body,
        (
            *[pltpu.VMEM(kept[k].shape, kept[k].dtype) for k in KEPT],
            pltpu.VMEM((col_count, heads_here * GROUPS, LANES), F32),
            pltpu.VMEM((col_count, 2 * group, channels), BF16),
            pltpu.VMEM((col_count, 2 * group, channels), BF16),
            pltpu.VMEM((channels, channels), BF16),
            pltpu.VMEM((1, pairs_here), F32),
            pltpu.VMEM((2 * group * rows_here,) * 2, BF16),
            pltpu.VMEM((group * rows_here, K_PARTS * group * rows_here), BF16),
            pltpu.VMEM((heads_here * rows_here, length_all), F32),
            pltpu.VMEM((cols_here // 2, length_all // 2), BF16),
        ),
        "prepare",
        row_start.reshape(1),
        col_index.reshape(1),
        chain_bias,
        *[kept[k] for k in KEPT],
        residue_mask.reshape(1, -1),
        chain_index.reshape(1, -1),
        bias_in,
        triangle,
        scalars=3,
        scratch=(
            pltpu.VMEM((1, length_all), jnp.int32),
            pltpu.VMEM((1, length_all), jnp.int32),
            pltpu.VMEM(bias_in.shape, BF16),
            pltpu.VMEM(triangle.shape, BF16),
            pltpu.VMEM((GROUPS, bias_in.shape[0], LANES), F32),
            pltpu.SemaphoreType.DMA((len(KEPT) + 4,)),
        ),
        far=True,
    )
    near, made = dict(zip(KEPT, near)), near[len(KEPT) :]
    bias_blocks, gates_in, values_in, last_in, pair_live, spread_order, gather_order, extra, pick = made

    key_values_all, bias_blocks = lax.optimization_barrier((key_values_all, bias_blocks))
    bias_blocks = exchange(bias_blocks, "col")
    terms = local_kernel(
        attention_body,
        pltpu.VMEM((col_count, *sequence.shape), BF16),
        "attention",
        bias_blocks,
        extra,
        key_values_all,
        query,
        gate,
        near["attention_out"],
        scratch=(
            pltpu.VMEM((heads_here * rows_here, LANES), F32),
            pltpu.VMEM((rows_here, LANES), F32),
        ),
    )
    terms = exchange(terms, "col")
    width = outer_in.shape[1]
    sequence_summed, left_twice, right_copies = local_kernel(
        settle_body,
        (
            pltpu.VMEM(sequence.shape, BF16),
            pltpu.VMEM((rows_here, width), F32),
            pltpu.VMEM((row_count, rows_here // 2, width), BF16),
        ),
        "settle",
        terms,
        sequence_near,
        near["outer_in"],
    )
    rights = exchange(right_copies, ROW)
    tiles, pair_mid, out_gate = local_kernel(
        pair_body,
        (
            pltpu.VMEM((col_count, 2 * group, pairs_here), BF16),
            pltpu.VMEM((pairs_here, channels), F32),
            pltpu.VMEM((pairs_here, channels), F32),
        ),
        "pair",
        rights,
        pick,
        left_twice,
        near["pair"],
        near["outer_out"],
        gates_in,
        values_in,
        last_in,
        pair_live,
    )

    tiles = exchange(tiles, "col")
    panels = local_kernel(
        spread_body,
        pltpu.VMEM((row_count, few + rows_here, length_all // K_PARTS), BF16),
        "spread",
        tiles,
        spread_order,
    )
    panels = exchange(panels, ROW)
    product = lax.dot_general(
        panels[:, :few].reshape(-1, length_all // K_PARTS),
        panels[:, few:].reshape(-1, length_all // K_PARTS),
        (((1,), (1,)), ((), ())),
        preferred_element_type=F32,
    ).astype(BF16)
    product = exchange(product.reshape(row_count, few, length_all), ROW)
    product = local_kernel(
        gather_body,
        pltpu.VMEM((col_count, group, pairs_here), BF16),
        "gather",
        product,
        gather_order,
    )
    product = exchange(product, "col").reshape(channels, pairs_here)

    sequence_out, pair_out = local_kernel(
        tail_body,
        (
            jax.ShapeDtypeStruct(sequence.shape, BF16),
            jax.ShapeDtypeStruct((pairs_here, channels), BF16),
        ),
        "tail",
        sequence_summed,
        product,
        pair_mid,
        out_gate,
        near["triangle_out"],
        near["transition_up"],
        near["transition_down"],
        scratch=(
            pltpu.VMEM((pairs_here, channels), BF16),
            pltpu.SemaphoreType.DMA((TAIL_PARTS + 1,)),
        ),
    )
    pair_out = pair_out.reshape(rows_here, cols_here, channels)
    return (sequence_out, pair_out)


def solution(mesh):
    finer = Mesh(mesh.devices.reshape(4, 8, mesh.shape["col"]), ("row_0", "row_1", "col"))
    placed = (
        P(ROW, None),
        P(ROW, "col", None),
        P(),
        P(),
        P(None, None, "col"),
        P("col", None),
        P(),
        P(),
        P(),
        P(),
        P(),
        P(),
        P(),
        P(),
    )
    return jax.shard_map(
        per_device,
        mesh=finer,
        in_specs=placed,
        out_specs=(P(ROW, None), P(ROW, "col", None)),
        check_vma=False,
    )
```

```python
import math

import jax
import jax.numpy as jnp
from jax import lax
from jax.experimental import pallas as pl
from jax.experimental.pallas import tpu as pltpu
from jax.sharding import Mesh
from jax.sharding import PartitionSpec as P

ROW = ("row_0", "row_1")
PAIR_AT = tuple((u // 4 + u + 3) % 4 * 4 + (u + 2) % 4 for u in range(16))
PAIR_PLACE = tuple(PAIR_AT.index(q) for q in range(16))
ROW_AT = tuple(2 * q + k for q in PAIR_AT for k in range(2))
ROW_PLACE = tuple(ROW_AT.index(r) for r in range(32))
COL_AT = tuple(p % 4 * 4 + (p // 4 ^ 1) for p in range(16))
COL_PLACE = tuple(COL_AT.index(q) for q in range(16))
BF16 = jnp.bfloat16
F32 = jnp.float32
K_PARTS = 2
I_PARTS = 2
TAIL_PARTS = 4
KEPT = (
    "pair",
    "attention_out",
    "outer_in",
    "outer_out",
    "triangle_out",
    "transition_up",
    "transition_down",
)
LANES = 128
GROUPS = 4


def exchange(blocks, axis):
    rows, cols = lax.axis_size(ROW), lax.axis_size("col")
    if axis == "col":
        groups = [[r * cols + q for q in COL_AT] for r in range(rows)]
    else:
        groups = [[r * cols + q for r in ROW_AT] for q in range(cols)]
    return lax.all_to_all(
        blocks, (*ROW, "col"), split_axis=0, concat_axis=0, tiled=True, axis_index_groups=groups
    )


def layer_norm(values, axis=-1):
    center = values - jnp.mean(values, axis=axis, keepdims=True)
    spread = jnp.mean(center * center, axis=axis, keepdims=True)
    return center * lax.rsqrt(spread + 1e-05)


def local_kernel(body, out_shape, name, *operands, scalars=0, scratch=(), far=False):
    space = pltpu.HBM if far else pltpu.VMEM
    spaces = [pltpu.SMEM if k < scalars else space for k in range(len(operands))]
    held = [
        pltpu.with_memory_space_constraint(x, space) if space is pltpu.VMEM else x
        for x, space in zip(operands, spaces)
    ]
    in_hbm = lambda x: isinstance(x, jax.ShapeDtypeStruct)
    return pl.pallas_call(
        body,
        out_shape=out_shape,
        in_specs=[pl.BlockSpec(memory_space=space) for space in spaces],
        out_specs=jax.tree.map(
            lambda x: pl.BlockSpec(memory_space=pltpu.HBM if in_hbm(x) else pltpu.VMEM), out_shape
        ),
        scratch_shapes=scratch,
        name=name,
    )(*held)


def fetch(sources, targets, arrived):
    copies = [
        pltpu.make_async_copy(source, target, arrived.at[k])
        for k, (source, target) in enumerate(zip(sources, targets))
    ]
    for copy in copies:
        copy.start()
    return copies


def mm(a, b, over_a, over_b):
    return lax.dot_general(a, b, (((over_a,), (over_b,)), ((), ())), preferred_element_type=F32)


def turn_lanes(value, groups):
    steps = groups % GROUPS
    return pltpu.roll(value, steps * (LANES // GROUPS), 1) if steps else value


def regroup(pick, shape):
    group = lax.broadcasted_iota(jnp.int32, shape, 1) // (LANES // GROUPS)
    tile = pick(0)
    for k in range(1, GROUPS):
        tile = jnp.where(group == k, pick(k), tile)
    return tile


def project_body(sequence, weights, key_values, query, gate, near, held, arrived):
    each = LANES // 4
    parts = [pl.ds(k * each, each) for k in range(8)]
    first_copy, *weight_copies = fetch(
        (sequence, *[weights.at[part] for part in parts]),
        (near, *[held.at[part] for part in parts]),
        arrived,
    )
    first_copy.wait()
    normed = layer_norm(near[...].astype(F32)).astype(BF16)
    projected = []
    for half in range(2):
        for copy in weight_copies[half * 4 : half * 4 + 4]:
            copy.wait()
        projected.append(mm(normed, held[half * LANES : (half + 1) * LANES], 1, 1))
    head, rest = projected
    rows = head.shape[0]
    first = lax.broadcasted_iota(jnp.int32, (rows, LANES), 1) < LANES // 2
    both = jnp.where(first, pltpu.roll(head, LANES // 2, 1), pltpu.roll(rest, LANES // 2, 1))
    key_values[...] = jnp.broadcast_to(both.astype(BF16)[None], key_values.shape)
    query[...] = jnp.where(first, head, 0.0).astype(BF16).astype(F32)
    gate[...] = jnp.where(first, 0.0, jax.nn.sigmoid(rest))


def prepare_body(row_start, col, chain_bias, *refs):
    count = len(KEPT)
    sources, targets = refs[: count + 4], refs[count + 4 : 2 * count + 4]
    blocks, gates_in, values_in, last_in, live, spread_order, gather_order, extra, pick = refs[
        2 * count + 4 : -6
    ]
    mask_near, chain_near, bias_near, triangle_near, turned_bias, arrived = refs[-6:]
    copies = fetch(
        sources, (*targets, mask_near, chain_near, bias_near, triangle_near), arrived
    )
    near = dict(zip(KEPT, targets))
    landed = dict(zip((*KEPT, "mask", "chain", "bias_in", "triangle"), copies))

    size = spread_order.shape[0]
    n = lax.broadcasted_iota(jnp.int32, spread_order.shape, 0)
    m = lax.broadcasted_iota(jnp.int32, spread_order.shape, 1)
    rows = live.shape[1] // (LANES // GROUPS)
    wanted = n % rows * (size // rows) + n // rows
    spread_order[...] = jnp.where(m == wanted, 1.0, 0.0).astype(BF16)
    size = gather_order.shape[0]
    group, few = size // rows, rows // I_PARTS
    n = lax.broadcasted_iota(jnp.int32, gather_order.shape, 0)
    m = lax.broadcasted_iota(jnp.int32, gather_order.shape, 1)
    i, c = n // group, n % group
    wanted = (i // few * group + c) * few + i % few
    gather_order[...] = jnp.where(m % size == wanted, 1.0, 0.0).astype(BF16)

    n = lax.broadcasted_iota(jnp.int32, pick.shape, 0)
    m = lax.broadcasted_iota(jnp.int32, pick.shape, 1)
    place = jnp.zeros(pick.shape, jnp.int32)
    for q, u in enumerate(PAIR_PLACE):
        place = jnp.where(col[0] == q, u, place)
    pick[...] = jnp.where(m == place * pick.shape[0] + n, 1.0, 0.0).astype(BF16)

    landed["pair"].wait()
    landed["bias_in"].wait()
    wide = near["pair"][...].astype(F32)
    turned = jnp.concatenate([wide[GROUPS * (p % GROUPS) + p // GROUPS] for p in range(rows)], axis=0)
    normed = layer_norm(turned).astype(BF16)
    heads = bias_near.shape[0]
    n = lax.broadcasted_iota(jnp.int32, (heads, heads), 0)
    m = lax.broadcasted_iota(jnp.int32, (heads, heads), 1)
    place = n // 2
    by_place = jnp.where(m == (place % 4 * 4 + (place // 4 ^ 1)) * 2 + n % 2, 1.0, 0.0).astype(BF16)
    bias = mm(mm(by_place, bias_near[...], 1, 0).astype(BF16), normed, 1, 1)
    columns = blocks.shape[0]
    for t in range(GROUPS):
        turned_bias[t] = bias[:, t * LANES : (t + 1) * LANES]
        for h in range(2):
            blocks[:, h * GROUPS + t, :] = turned_bias[t, pl.ds(h, columns, stride=2), :]

    landed["mask"].wait()
    mask = mask_near[...].astype(F32).astype(BF16)
    length = mask.shape[1]
    residue = lax.broadcasted_iota(jnp.int32, (length, live.shape[1]), 0)
    pair = lax.broadcasted_iota(jnp.int32, (length, live.shape[1]), 1)
    of_row = jnp.where(residue == row_start[0] + pair // (LANES // GROUPS), 1.0, 0.0).astype(BF16)
    of_col = jnp.where(residue == col[0] * (LANES // GROUPS) + pair % (LANES // GROUPS), 1.0, 0.0).astype(BF16)
    mask = jnp.broadcast_to(mask, (8, length))
    live[...] = (mm(mask, of_row, 1, 0) * mm(mask, of_col, 1, 0))[:1]

    landed["chain"].wait()
    eight = blocks.shape[1]
    four = eight // 2
    position = lax.broadcasted_iota(jnp.int32, (eight, length), 1)
    row = lax.broadcasted_iota(jnp.int32, (eight, length), 0)
    chains = jnp.broadcast_to(chain_near[...].astype(F32), (eight, length))
    kept = jnp.broadcast_to(mask_near[...], (eight, length)) == 1
    offset = jnp.where(row < four, chain_bias[2 * col[0]], chain_bias[2 * col[0] + 1])
    for g in range(GROUPS):
        here = position == row_start[0] + g * four + row % four
        own_chain = jnp.sum(jnp.where(here, chains, 0.0), axis=1, keepdims=True)
        added = jnp.where(chains == own_chain, offset, 0.0)
        extra[g * eight : (g + 1) * eight, :] = jnp.where(kept | here, added, -jnp.inf)

    landed["triangle"].wait()
    half = gates_in.shape[1] // 2
    for k, target in enumerate((gates_in, values_in, gates_in, values_in)):
        side = half * (k // 2)
        across = jnp.transpose(triangle_near[k].astype(F32)).astype(BF16)
        target[:, side : side + half, :] = across.reshape(target.shape[0], half, LANES)
    last_in[...] = triangle_near[4]
    for name in KEPT:
        if name != "pair":
            landed[name].wait()


def attention_body(blocks, extra, key_values, query, gate, attention_out, copies, spread, joined):
    count, eight, _ = blocks.shape
    four = eight // 2
    length = count * (LANES // GROUPS)
    lane = lax.broadcasted_iota(jnp.int32, (four, LANES), 1)
    for g in range(GROUPS):
        taken = query[g * four : (g + 1) * four, :]
        for h in range(2):
            own = (lane >= h * (LANES // 4)) & (lane < (h + 1) * (LANES // 4))
            spread[g * eight + h * four : g * eight + (h + 1) * four, :] = jnp.where(own, taken, 0.0)
    everyone = jnp.concatenate([key_values[p] for p in ROW_PLACE], axis=0)
    raw = mm(spread[...].astype(BF16), everyone, 1, 1)
    raw = raw * (1.0 / math.sqrt(LANES // 4))
    biases = []
    for g in range(GROUPS):
        pieces = []
        for tile in range(count // GROUPS):
            pieces.append(
                regroup(
                    lambda k, tile=tile, g=g: turn_lanes(blocks[COL_PLACE[GROUPS * tile + k]], k - g),
                    (eight, LANES),
                )
            )
        biases.append(jnp.concatenate(pieces, axis=1))
    scores = raw + jnp.concatenate(biases, axis=0) + extra[...]
    raised = jnp.exp(scores - jnp.max(scores, axis=1, keepdims=True))
    weights = [raised / jnp.sum(raised, axis=1, keepdims=True)]
    mixed = mm(jnp.concatenate(weights, axis=0).astype(BF16), everyone, 1, 0)
    for g in range(GROUPS):
        upper = mixed[g * eight : g * eight + four]
        lower = mixed[g * eight + four : (g + 1) * eight]
        joined[g * four : (g + 1) * four, :] = jnp.where(lane < LANES * 3 // 4, upper, lower)
    gated = pltpu.roll(gate[...] * joined[...], LANES // 2, 1)[:, : LANES // 2].astype(BF16)
    terms = mm(gated, attention_out[...], 1, 0).astype(BF16)
    copies[...] = jnp.broadcast_to(terms[None], copies.shape)


def spread_body(tiles, order, panels):
    count, chans, pairs = tiles.shape
    rows = pairs // (LANES // GROUPS)
    per = count // GROUPS
    by_row = []
    for i in range(rows):
        at, g = i // GROUPS * LANES, i % GROUPS
        by_row.append(
            jnp.concatenate(
                [
                    regroup(
                        lambda k, tile=tile, g=g, at=at: turn_lanes(
                            tiles[COL_PLACE[GROUPS * tile + k], :, at : at + LANES].astype(F32), k - g
                        ),
                        (chans, LANES),
                    )
                    for tile in range(per)
                ],
                axis=1,
            )
        )
    turned = mm(order[...], jnp.concatenate(by_row, axis=0).astype(BF16), 1, 0).astype(BF16)
    half = chans // 2
    few = rows // I_PARTS
    wide = turned.shape[1] // K_PARTS
    for k in range(K_PARTS):
        for i in range(I_PARTS):
            for c in range(half):
                block = (k * I_PARTS + i) * half + c
                at = c * rows + i * few
                panels[block, :few, :] = turned[at : at + few, k * wide : (k + 1) * wide]
                at = (half + c) * rows
                panels[block, few:, :] = turned[at : at + rows, k * wide : (k + 1) * wide]


def gather_body(parts, order, blocks):
    total, few, length = parts.shape
    count, group, pairs = blocks.shape
    rows = pairs // (LANES // GROUPS)
    summed = mm(order[...], parts[...].reshape(total * few, length), 1, 0)
    for q in range(count):
        place = PAIR_PLACE[COL_AT[q]]
        tile, s = place // GROUPS, place % GROUPS
        pieces = []
        for t in range(rows // GROUPS):
            pieces.append(
                regroup(
                    lambda k, t=t, tile=tile, s=s: turn_lanes(
                        summed[
                            (GROUPS * t + k) * group : (GROUPS * t + k + 1) * group,
                            tile * LANES : (tile + 1) * LANES,
                        ],
                        k - s,
                    ),
                    (group, LANES),
                )
            )
        blocks[q] = jnp.concatenate(pieces, axis=1).astype(BF16)


def settle_body(terms, sequence, outer_in, sequence_out, left_twice, right_copies):
    update = jnp.sum(terms[...].astype(F32), axis=0)
    summed = (sequence[...].astype(F32) + update).astype(BF16)
    sequence_out[...] = summed
    normed = layer_norm(summed.astype(F32)).astype(BF16)
    outer_rows = mm(normed, outer_in[...], 1, 0).astype(BF16).astype(F32)
    rows, width = outer_rows.shape
    half = width // 2
    first = lax.broadcasted_iota(jnp.int32, (rows, width), 1) < half
    turned = pltpu.roll(outer_rows, half, 1)
    left_twice[...] = jnp.where(first, outer_rows, turned)
    packed = jnp.where(first[: rows // 2], turned[: rows // 2], outer_rows[rows // 2 :])
    right_copies[...] = jnp.broadcast_to(packed.astype(BF16)[None], right_copies.shape)


def pair_body(
    rights,
    pick,
    left_twice,
    pair,
    outer_out,
    gates_in,
    values_in,
    last_in,
    live,
    tiles,
    mid,
    out_gate,
):
    rows, cols, channels = pair.shape
    half = channels // 2
    taken = mm(pick[...], rights[...].reshape(-1, channels), 1, 0)
    taken = taken.reshape(cols // rows, rows // 2, channels)
    first = lax.broadcasted_iota(jnp.int32, (rows // 2, channels), 1) < half
    pieces = []
    for k in range(cols // rows):
        turned = pltpu.roll(taken[k], half, 1)
        pieces.append(jnp.where(first, taken[k], turned))
        pieces.append(jnp.where(first, turned, taken[k]))
    right_twice = jnp.concatenate(pieces, axis=0)
    left = left_twice[...][:, None, :]
    right = right_twice[None, :, :]
    lane = lax.broadcasted_iota(jnp.int32, (rows, cols, channels), 2)
    feat = jnp.where(lane < half, left * right, left - right).astype(BF16)
    feat = feat.reshape(rows * cols, channels)
    pair_mid = pair[...].astype(F32).reshape(rows * cols, channels) + mm(feat, outer_out[...], 1, 0)
    mid[...] = pair_mid
    normed = layer_norm(pair_mid).astype(BF16)
    flat = (-1, channels)
    opened = jax.nn.sigmoid(mm(gates_in[...].reshape(flat), normed, 1, 1))
    operands = opened * mm(values_in[...].reshape(flat), normed, 1, 1) * live[...]
    tiles[...] = operands.astype(BF16).reshape(tiles.shape)
    out_gate[...] = jax.nn.sigmoid(mm(normed, last_in[...], 1, 0))


def tail_body(
    sequence_near,
    product,
    mid,
    out_gate,
    triangle_out,
    transition_up,
    transition_down,
    sequence_out,
    out,
    held,
    left,
):
    copies = [pltpu.make_async_copy(sequence_near, sequence_out, left.at[TAIL_PARTS])]
    copies[0].start()
    normed_product = layer_norm(product[...].astype(F32), axis=0)
    normed_product = jnp.transpose(normed_product).astype(BF16)
    late = mid[...] + out_gate[...] * mm(normed_product, triangle_out[...], 1, 0)
    normed_late = layer_norm(late).astype(BF16)
    hidden = jnp.maximum(mm(normed_late, transition_up[...], 1, 0), 0.0).astype(BF16)
    part = mid.shape[0] // TAIL_PARTS
    for k in range(TAIL_PARTS):
        here = slice(k * part, (k + 1) * part)
        held[here] = (late[here] + mm(hidden[here], transition_down[...], 1, 0)).astype(BF16)
        copies.append(pltpu.make_async_copy(held.at[here], out.at[here], left.at[k]))
        copies[-1].start()
    for copy in copies:
        copy.wait()


def per_device(
    sequence,
    pair_state,
    residue_mask,
    chain_index,
    attention_in,
    attention_out,
    bias_weight,
    chain_bias,
    outer_in,
    outer_out,
    triangle_in,
    triangle_out,
    transition_up,
    transition_down,
):
    rows_here, cols_here, channels = pair_state.shape
    length_all = residue_mask.shape[0]
    pairs_here = rows_here * cols_here
    row_index = lax.axis_index(ROW)
    col_index = lax.axis_index("col")
    row_count = lax.axis_size(ROW)
    col_count = lax.axis_size("col")
    row_start = row_index * rows_here

    group = channels // col_count
    heads_here = bias_weight.shape[1] // col_count

    weights = jnp.transpose(attention_in, (1, 2, 0)).reshape(-1, sequence.shape[1])
    key_values, query, gate, sequence_near = local_kernel(
        project_body,
        (
            pltpu.VMEM((row_count, rows_here, LANES), BF16),
            pltpu.VMEM((rows_here, LANES), F32),
            pltpu.VMEM((rows_here, LANES), F32),
            pltpu.VMEM(sequence.shape, BF16),
        ),
        "project",
        sequence,
        weights,
        scratch=(pltpu.VMEM(weights.shape, BF16), pltpu.SemaphoreType.DMA((9,))),
        far=True,
    )
    key_values_all = exchange(key_values, ROW)

    bias_in = jnp.transpose(bias_weight)
    triangle = jnp.transpose(triangle_in, (1, 0, 2))
    kept = dict(
        pair=pair_state,
        attention_out=attention_out,
        outer_in=outer_in,
        outer_out=outer_out,
        triangle_out=triangle_out,
        transition_up=transition_up,
        transition_down=transition_down,
    )
    few = rows_here // I_PARTS
    near = local_kernel(
        prepare_body,
        (
            *[pltpu.VMEM(kept[k].shape, kept[k].dtype) for k in KEPT],
            pltpu.VMEM((col_count, heads_here * GROUPS, LANES), F32),
            pltpu.VMEM((col_count, 2 * group, channels), BF16),
            pltpu.VMEM((col_count, 2 * group, channels), BF16),
            pltpu.VMEM((channels, channels), BF16),
            pltpu.VMEM((1, pairs_here), F32),
            pltpu.VMEM((2 * group * rows_here,) * 2, BF16),
            pltpu.VMEM((group * rows_here, K_PARTS * group * rows_here), BF16),
            pltpu.VMEM((heads_here * rows_here, length_all), F32),
            pltpu.VMEM((cols_here // 2, length_all // 2), BF16),
        ),
        "prepare",
        row_start.reshape(1),
        col_index.reshape(1),
        chain_bias,
        *[kept[k] for k in KEPT],
        residue_mask.reshape(1, -1),
        chain_index.reshape(1, -1),
        bias_in,
        triangle,
        scalars=3,
        scratch=(
            pltpu.VMEM((1, length_all), jnp.int32),
            pltpu.VMEM((1, length_all), jnp.int32),
            pltpu.VMEM(bias_in.shape, BF16),
            pltpu.VMEM(triangle.shape, BF16),
            pltpu.VMEM((GROUPS, bias_in.shape[0], LANES), F32),
            pltpu.SemaphoreType.DMA((len(KEPT) + 4,)),
        ),
        far=True,
    )
    near, made = dict(zip(KEPT, near)), near[len(KEPT) :]
    bias_blocks, gates_in, values_in, last_in, pair_live, spread_order, gather_order, extra, pick = made

    key_values_all, bias_blocks = lax.optimization_barrier((key_values_all, bias_blocks))
    bias_blocks = exchange(bias_blocks, "col")
    terms = local_kernel(
        attention_body,
        pltpu.VMEM((col_count, *sequence.shape), BF16),
        "attention",
        bias_blocks,
        extra,
        key_values_all,
        query,
        gate,
        near["attention_out"],
        scratch=(
            pltpu.VMEM((heads_here * rows_here, LANES), F32),
            pltpu.VMEM((rows_here, LANES), F32),
        ),
    )
    terms = exchange(terms, "col")
    width = outer_in.shape[1]
    sequence_summed, left_twice, right_copies = local_kernel(
        settle_body,
        (
            pltpu.VMEM(sequence.shape, BF16),
            pltpu.VMEM((rows_here, width), F32),
            pltpu.VMEM((row_count, rows_here // 2, width), BF16),
        ),
        "settle",
        terms,
        sequence_near,
        near["outer_in"],
    )
    rights = exchange(right_copies, ROW)
    tiles, pair_mid, out_gate = local_kernel(
        pair_body,
        (
            pltpu.VMEM((col_count, 2 * group, pairs_here), BF16),
            pltpu.VMEM((pairs_here, channels), F32),
            pltpu.VMEM((pairs_here, channels), F32),
        ),
        "pair",
        rights,
        pick,
        left_twice,
        near["pair"],
        near["outer_out"],
        gates_in,
        values_in,
        last_in,
        pair_live,
    )

    tiles = exchange(tiles, "col")
    panels = local_kernel(
        spread_body,
        pltpu.VMEM((row_count, few + rows_here, length_all // K_PARTS), BF16),
        "spread",
        tiles,
        spread_order,
    )
    panels = exchange(panels, ROW)
    product = lax.dot_general(
        panels[:, :few].reshape(-1, length_all // K_PARTS),
        panels[:, few:].reshape(-1, length_all // K_PARTS),
        (((1,), (1,)), ((), ())),
        preferred_element_type=F32,
    ).astype(BF16)
    product = exchange(product.reshape(row_count, few, length_all), ROW)
    product = local_kernel(
        gather_body,
        pltpu.VMEM((col_count, group, pairs_here), BF16),
        "gather",
        product,
        gather_order,
    )
    product = exchange(product, "col").reshape(channels, pairs_here)

    sequence_out, pair_out = local_kernel(
        tail_body,
        (
            jax.ShapeDtypeStruct(sequence.shape, BF16),
            jax.ShapeDtypeStruct((pairs_here, channels), BF16),
        ),
        "tail",
        sequence_summed,
        product,
        pair_mid,
        out_gate,
        near["triangle_out"],
        near["transition_up"],
        near["transition_down"],
        scratch=(
            pltpu.VMEM((pairs_here, channels), BF16),
            pltpu.SemaphoreType.DMA((TAIL_PARTS + 1,)),
        ),
    )
    pair_out = pair_out.reshape(rows_here, cols_here, channels)
    return (sequence_out, pair_out)


def solution(mesh):
    finer = Mesh(mesh.devices.reshape(4, 8, mesh.shape["col"]), ("row_0", "row_1", "col"))
    placed = (
        P(ROW, None),
        P(ROW, "col", None),
        P(),
        P(),
        P(None, None, "col"),
        P("col", None),
        P(),
        P(),
        P(),
        P(),
        P(),
        P(),
        P(),
        P(),
    )
    return jax.shard_map(
        per_device,
        mesh=finer,
        in_specs=placed,
        out_specs=(P(ROW, None), P(ROW, "col", None)),
        check_vma=False,
    )
```

```python
import math

import jax
import jax.numpy as jnp
from jax import lax
from jax.experimental import pallas as pl
from jax.experimental.pallas import tpu as pltpu
from jax.sharding import Mesh
from jax.sharding import PartitionSpec as P

ROW = ("row_0", "row_1")
PAIR_AT = tuple(u ^ 14 for u in range(16))
PAIR_PLACE = tuple(PAIR_AT.index(q) for q in range(16))
ROW_AT = tuple(2 * q + k for q in PAIR_AT for k in range(2))
ROW_PLACE = tuple(ROW_AT.index(r) for r in range(32))
COL_AT = tuple(p % 4 * 4 + (p // 4 ^ 1) for p in range(16))
COL_PLACE = tuple(COL_AT.index(q) for q in range(16))
BF16 = jnp.bfloat16
F32 = jnp.float32
K_PARTS = 2
I_PARTS = 2
TAIL_PARTS = 4
KEPT = (
    "pair",
    "attention_out",
    "outer_in",
    "outer_out",
    "triangle_out",
    "transition_up",
    "transition_down",
)
LANES = 128
GROUPS = 4


def exchange(blocks, axis):
    rows, cols = lax.axis_size(ROW), lax.axis_size("col")
    if axis == "col":
        groups = [[r * cols + q for q in COL_AT] for r in range(rows)]
    else:
        groups = [[r * cols + q for r in ROW_AT] for q in range(cols)]
    return lax.all_to_all(
        blocks, (*ROW, "col"), split_axis=0, concat_axis=0, tiled=True, axis_index_groups=groups
    )


def layer_norm(values, axis=-1):
    center = values - jnp.mean(values, axis=axis, keepdims=True)
    spread = jnp.mean(center * center, axis=axis, keepdims=True)
    return center * lax.rsqrt(spread + 1e-05)


def local_kernel(body, out_shape, name, *operands, scalars=0, scratch=(), far=False):
    space = pltpu.HBM if far else pltpu.VMEM
    spaces = [pltpu.SMEM if k < scalars else space for k in range(len(operands))]
    held = [
        pltpu.with_memory_space_constraint(x, space) if space is pltpu.VMEM else x
        for x, space in zip(operands, spaces)
    ]
    in_hbm = lambda x: isinstance(x, jax.ShapeDtypeStruct)
    return pl.pallas_call(
        body,
        out_shape=out_shape,
        in_specs=[pl.BlockSpec(memory_space=space) for space in spaces],
        out_specs=jax.tree.map(
            lambda x: pl.BlockSpec(memory_space=pltpu.HBM if in_hbm(x) else pltpu.VMEM), out_shape
        ),
        scratch_shapes=scratch,
        name=name,
    )(*held)


def fetch(sources, targets, arrived):
    copies = [
        pltpu.make_async_copy(source, target, arrived.at[k])
        for k, (source, target) in enumerate(zip(sources, targets))
    ]
    for copy in copies:
        copy.start()
    return copies


def mm(a, b, over_a, over_b):
    return lax.dot_general(a, b, (((over_a,), (over_b,)), ((), ())), preferred_element_type=F32)


def turn_lanes(value, groups):
    steps = groups % GROUPS
    return pltpu.roll(value, steps * (LANES // GROUPS), 1) if steps else value


def regroup(pick, shape):
    group = lax.broadcasted_iota(jnp.int32, shape, 1) // (LANES // GROUPS)
    tile = pick(0)
    for k in range(1, GROUPS):
        tile = jnp.where(group == k, pick(k), tile)
    return tile


def project_body(sequence, weights, key_values, query, gate, near, held, arrived):
    each = LANES // 4
    parts = [pl.ds(k * each, each) for k in range(8)]
    first_copy, *weight_copies = fetch(
        (sequence, *[weights.at[part] for part in parts]),
        (near, *[held.at[part] for part in parts]),
        arrived,
    )
    first_copy.wait()
    normed = layer_norm(near[...].astype(F32)).astype(BF16)
    projected = []
    for half in range(2):
        for copy in weight_copies[half * 4 : half * 4 + 4]:
            copy.wait()
        projected.append(mm(normed, held[half * LANES : (half + 1) * LANES], 1, 1))
    head, rest = projected
    rows = head.shape[0]
    first = lax.broadcasted_iota(jnp.int32, (rows, LANES), 1) < LANES // 2
    both = jnp.where(first, pltpu.roll(head, LANES // 2, 1), pltpu.roll(rest, LANES // 2, 1))
    key_values[...] = jnp.broadcast_to(both.astype(BF16)[None], key_values.shape)
    query[...] = jnp.where(first, head, 0.0).astype(BF16).astype(F32)
    gate[...] = jnp.where(first, 0.0, jax.nn.sigmoid(rest))


def prepare_body(row_start, col, chain_bias, *refs):
    count = len(KEPT)
    sources, targets = refs[: count + 4], refs[count + 4 : 2 * count + 4]
    blocks, gates_in, values_in, last_in, live, spread_order, gather_order, extra, pick = refs[
        2 * count + 4 : -6
    ]
    mask_near, chain_near, bias_near, triangle_near, turned_bias, arrived = refs[-6:]
    copies = fetch(
        sources, (*targets, mask_near, chain_near, bias_near, triangle_near), arrived
    )
    near = dict(zip(KEPT, targets))
    landed = dict(zip((*KEPT, "mask", "chain", "bias_in", "triangle"), copies))

    size = spread_order.shape[0]
    n = lax.broadcasted_iota(jnp.int32, spread_order.shape, 0)
    m = lax.broadcasted_iota(jnp.int32, spread_order.shape, 1)
    rows = live.shape[1] // (LANES // GROUPS)
    wanted = n % rows * (size // rows) + n // rows
    spread_order[...] = jnp.where(m == wanted, 1.0, 0.0).astype(BF16)
    size = gather_order.shape[0]
    group, few = size // rows, rows // I_PARTS
    n = lax.broadcasted_iota(jnp.int32, gather_order.shape, 0)
    m = lax.broadcasted_iota(jnp.int32, gather_order.shape, 1)
    i, c = n // group, n % group
    wanted = (i // few * group + c) * few + i % few
    gather_order[...] = jnp.where(m % size == wanted, 1.0, 0.0).astype(BF16)

    n = lax.broadcasted_iota(jnp.int32, pick.shape, 0)
    m = lax.broadcasted_iota(jnp.int32, pick.shape, 1)
    place = jnp.zeros(pick.shape, jnp.int32)
    for q, u in enumerate(PAIR_PLACE):
        place = jnp.where(col[0] == q, u, place)
    pick[...] = jnp.where(m == place * pick.shape[0] + n, 1.0, 0.0).astype(BF16)

    landed["pair"].wait()
    landed["bias_in"].wait()
    wide = near["pair"][...].astype(F32)
    turned = jnp.concatenate([wide[GROUPS * (p % GROUPS) + p // GROUPS] for p in range(rows)], axis=0)
    normed = layer_norm(turned).astype(BF16)
    heads = bias_near.shape[0]
    n = lax.broadcasted_iota(jnp.int32, (heads, heads), 0)
    m = lax.broadcasted_iota(jnp.int32, (heads, heads), 1)
    place = n // 2
    by_place = jnp.where(m == (place % 4 * 4 + (place // 4 ^ 1)) * 2 + n % 2, 1.0, 0.0).astype(BF16)
    bias = mm(mm(by_place, bias_near[...], 1, 0).astype(BF16), normed, 1, 1)
    columns = blocks.shape[0]
    for t in range(GROUPS):
        turned_bias[t] = bias[:, t * LANES : (t + 1) * LANES]
        for h in range(2):
            blocks[:, h * GROUPS + t, :] = turned_bias[t, pl.ds(h, columns, stride=2), :]

    landed["mask"].wait()
    mask = mask_near[...].astype(F32).astype(BF16)
    length = mask.shape[1]
    residue = lax.broadcasted_iota(jnp.int32, (length, live.shape[1]), 0)
    pair = lax.broadcasted_iota(jnp.int32, (length, live.shape[1]), 1)
    of_row = jnp.where(residue == row_start[0] + pair // (LANES // GROUPS), 1.0, 0.0).astype(BF16)
    of_col = jnp.where(residue == col[0] * (LANES // GROUPS) + pair % (LANES // GROUPS), 1.0, 0.0).astype(BF16)
    mask = jnp.broadcast_to(mask, (8, length))
    live[...] = (mm(mask, of_row, 1, 0) * mm(mask, of_col, 1, 0))[:1]

    landed["chain"].wait()
    eight = blocks.shape[1]
    four = eight // 2
    position = lax.broadcasted_iota(jnp.int32, (eight, length), 1)
    row = lax.broadcasted_iota(jnp.int32, (eight, length), 0)
    chains = jnp.broadcast_to(chain_near[...].astype(F32), (eight, length))
    kept = jnp.broadcast_to(mask_near[...], (eight, length)) == 1
    offset = jnp.where(row < four, chain_bias[2 * col[0]], chain_bias[2 * col[0] + 1])
    for g in range(GROUPS):
        here = position == row_start[0] + g * four + row % four
        own_chain = jnp.sum(jnp.where(here, chains, 0.0), axis=1, keepdims=True)
        added = jnp.where(chains == own_chain, offset, 0.0)
        extra[g * eight : (g + 1) * eight, :] = jnp.where(kept | here, added, -jnp.inf)

    landed["triangle"].wait()
    half = gates_in.shape[1] // 2
    for k, target in enumerate((gates_in, values_in, gates_in, values_in)):
        side = half * (k // 2)
        across = jnp.transpose(triangle_near[k].astype(F32)).astype(BF16)
        target[:, side : side + half, :] = across.reshape(target.shape[0], half, LANES)
    last_in[...] = triangle_near[4]
    for name in KEPT:
        if name != "pair":
            landed[name].wait()


def attention_body(blocks, extra, key_values, query, gate, attention_out, copies, spread, joined):
    count, eight, _ = blocks.shape
    four = eight // 2
    length = count * (LANES // GROUPS)
    lane = lax.broadcasted_iota(jnp.int32, (four, LANES), 1)
    for g in range(GROUPS):
        taken = query[g * four : (g + 1) * four, :]
        for h in range(2):
            own = (lane >= h * (LANES // 4)) & (lane < (h + 1) * (LANES // 4))
            spread[g * eight + h * four : g * eight + (h + 1) * four, :] = jnp.where(own, taken, 0.0)
    everyone = jnp.concatenate([key_values[p] for p in ROW_PLACE], axis=0)
    raw = mm(spread[...].astype(BF16), everyone, 1, 1)
    raw = raw * (1.0 / math.sqrt(LANES // 4))
    biases = []
    for g in range(GROUPS):
        pieces = []
        for tile in range(count // GROUPS):
            pieces.append(
                regroup(
                    lambda k, tile=tile, g=g: turn_lanes(blocks[COL_PLACE[GROUPS * tile + k]], k - g),
                    (eight, LANES),
                )
            )
        biases.append(jnp.concatenate(pieces, axis=1))
    scores = raw + jnp.concatenate(biases, axis=0) + extra[...]
    raised = jnp.exp(scores - jnp.max(scores, axis=1, keepdims=True))
    weights = [raised / jnp.sum(raised, axis=1, keepdims=True)]
    mixed = mm(jnp.concatenate(weights, axis=0).astype(BF16), everyone, 1, 0)
    for g in range(GROUPS):
        upper = mixed[g * eight : g * eight + four]
        lower = mixed[g * eight + four : (g + 1) * eight]
        joined[g * four : (g + 1) * four, :] = jnp.where(lane < LANES * 3 // 4, upper, lower)
    gated = pltpu.roll(gate[...] * joined[...], LANES // 2, 1)[:, : LANES // 2].astype(BF16)
    terms = mm(gated, attention_out[...], 1, 0).astype(BF16)
    copies[...] = jnp.broadcast_to(terms[None], copies.shape)


def spread_body(tiles, order, panels):
    count, chans, pairs = tiles.shape
    rows = pairs // (LANES // GROUPS)
    per = count // GROUPS
    by_row = []
    for i in range(rows):
        at, g = i // GROUPS * LANES, i % GROUPS
        by_row.append(
            jnp.concatenate(
                [
                    regroup(
                        lambda k, tile=tile, g=g, at=at: turn_lanes(
                            tiles[COL_PLACE[GROUPS * tile + k], :, at : at + LANES].astype(F32), k - g
                        ),
                        (chans, LANES),
                    )
                    for tile in range(per)
                ],
                axis=1,
            )
        )
    turned = mm(order[...], jnp.concatenate(by_row, axis=0).astype(BF16), 1, 0).astype(BF16)
    half = chans // 2
    few = rows // I_PARTS
    wide = turned.shape[1] // K_PARTS
    for k in range(K_PARTS):
        for i in range(I_PARTS):
            for c in range(half):
                block = (k * I_PARTS + i) * half + c
                at = c * rows + i * few
                panels[block, :few, :] = turned[at : at + few, k * wide : (k + 1) * wide]
                at = (half + c) * rows
                panels[block, few:, :] = turned[at : at + rows, k * wide : (k + 1) * wide]


def gather_body(parts, order, blocks):
    total, few, length = parts.shape
    count, group, pairs = blocks.shape
    rows = pairs // (LANES // GROUPS)
    summed = mm(order[...], parts[...].reshape(total * few, length), 1, 0)
    for q in range(count):
        place = PAIR_PLACE[COL_AT[q]]
        tile, s = place // GROUPS, place % GROUPS
        pieces = []
        for t in range(rows // GROUPS):
            pieces.append(
                regroup(
                    lambda k, t=t, tile=tile, s=s: turn_lanes(
                        summed[
                            (GROUPS * t + k) * group : (GROUPS * t + k + 1) * group,
                            tile * LANES : (tile + 1) * LANES,
                        ],
                        k - s,
                    ),
                    (group, LANES),
                )
            )
        blocks[q] = jnp.concatenate(pieces, axis=1).astype(BF16)


def settle_body(terms, sequence, outer_in, sequence_out, left_twice, right_copies):
    update = jnp.sum(terms[...].astype(F32), axis=0)
    summed = (sequence[...].astype(F32) + update).astype(BF16)
    sequence_out[...] = summed
    normed = layer_norm(summed.astype(F32)).astype(BF16)
    outer_rows = mm(normed, outer_in[...], 1, 0).astype(BF16).astype(F32)
    rows, width = outer_rows.shape
    half = width // 2
    first = lax.broadcasted_iota(jnp.int32, (rows, width), 1) < half
    turned = pltpu.roll(outer_rows, half, 1)
    left_twice[...] = jnp.where(first, outer_rows, turned)
    packed = jnp.where(first[: rows // 2], turned[: rows // 2], outer_rows[rows // 2 :])
    right_copies[...] = jnp.broadcast_to(packed.astype(BF16)[None], right_copies.shape)


def pair_body(
    rights,
    pick,
    left_twice,
    pair,
    outer_out,
    gates_in,
    values_in,
    last_in,
    live,
    tiles,
    mid,
    out_gate,
):
    rows, cols, channels = pair.shape
    half = channels // 2
    taken = mm(pick[...], rights[...].reshape(-1, channels), 1, 0)
    taken = taken.reshape(cols // rows, rows // 2, channels)
    first = lax.broadcasted_iota(jnp.int32, (rows // 2, channels), 1) < half
    pieces = []
    for k in range(cols // rows):
        turned = pltpu.roll(taken[k], half, 1)
        pieces.append(jnp.where(first, taken[k], turned))
        pieces.append(jnp.where(first, turned, taken[k]))
    right_twice = jnp.concatenate(pieces, axis=0)
    left = left_twice[...][:, None, :]
    right = right_twice[None, :, :]
    lane = lax.broadcasted_iota(jnp.int32, (rows, cols, channels), 2)
    feat = jnp.where(lane < half, left * right, left - right).astype(BF16)
    feat = feat.reshape(rows * cols, channels)
    pair_mid = pair[...].astype(F32).reshape(rows * cols, channels) + mm(feat, outer_out[...], 1, 0)
    mid[...] = pair_mid
    normed = layer_norm(pair_mid).astype(BF16)
    flat = (-1, channels)
    opened = jax.nn.sigmoid(mm(gates_in[...].reshape(flat), normed, 1, 1))
    operands = opened * mm(values_in[...].reshape(flat), normed, 1, 1) * live[...]
    tiles[...] = operands.astype(BF16).reshape(tiles.shape)
    out_gate[...] = jax.nn.sigmoid(mm(normed, last_in[...], 1, 0))


def tail_body(
    sequence_near,
    product,
    mid,
    out_gate,
    triangle_out,
    transition_up,
    transition_down,
    sequence_out,
    out,
    held,
    left,
):
    copies = [pltpu.make_async_copy(sequence_near, sequence_out, left.at[TAIL_PARTS])]
    copies[0].start()
    normed_product = layer_norm(product[...].astype(F32), axis=0)
    normed_product = jnp.transpose(normed_product).astype(BF16)
    late = mid[...] + out_gate[...] * mm(normed_product, triangle_out[...], 1, 0)
    normed_late = layer_norm(late).astype(BF16)
    hidden = jnp.maximum(mm(normed_late, transition_up[...], 1, 0), 0.0).astype(BF16)
    part = mid.shape[0] // TAIL_PARTS
    for k in range(TAIL_PARTS):
        here = slice(k * part, (k + 1) * part)
        held[here] = (late[here] + mm(hidden[here], transition_down[...], 1, 0)).astype(BF16)
        copies.append(pltpu.make_async_copy(held.at[here], out.at[here], left.at[k]))
        copies[-1].start()
    for copy in copies:
        copy.wait()


def per_device(
    sequence,
    pair_state,
    residue_mask,
    chain_index,
    attention_in,
    attention_out,
    bias_weight,
    chain_bias,
    outer_in,
    outer_out,
    triangle_in,
    triangle_out,
    transition_up,
    transition_down,
):
    rows_here, cols_here, channels = pair_state.shape
    length_all = residue_mask.shape[0]
    pairs_here = rows_here * cols_here
    row_index = lax.axis_index(ROW)
    col_index = lax.axis_index("col")
    row_count = lax.axis_size(ROW)
    col_count = lax.axis_size("col")
    row_start = row_index * rows_here

    group = channels // col_count
    heads_here = bias_weight.shape[1] // col_count

    weights = jnp.transpose(attention_in, (1, 2, 0)).reshape(-1, sequence.shape[1])
    key_values, query, gate, sequence_near = local_kernel(
        project_body,
        (
            pltpu.VMEM((row_count, rows_here, LANES), BF16),
            pltpu.VMEM((rows_here, LANES), F32),
            pltpu.VMEM((rows_here, LANES), F32),
            pltpu.VMEM(sequence.shape, BF16),
        ),
        "project",
        sequence,
        weights,
        scratch=(pltpu.VMEM(weights.shape, BF16), pltpu.SemaphoreType.DMA((9,))),
        far=True,
    )
    key_values_all = exchange(key_values, ROW)

    bias_in = jnp.transpose(bias_weight)
    triangle = jnp.transpose(triangle_in, (1, 0, 2))
    kept = dict(
        pair=pair_state,
        attention_out=attention_out,
        outer_in=outer_in,
        outer_out=outer_out,
        triangle_out=triangle_out,
        transition_up=transition_up,
        transition_down=transition_down,
    )
    few = rows_here // I_PARTS
    near = local_kernel(
        prepare_body,
        (
            *[pltpu.VMEM(kept[k].shape, kept[k].dtype) for k in KEPT],
            pltpu.VMEM((col_count, heads_here * GROUPS, LANES), F32),
            pltpu.VMEM((col_count, 2 * group, channels), BF16),
            pltpu.VMEM((col_count, 2 * group, channels), BF16),
            pltpu.VMEM((channels, channels), BF16),
            pltpu.VMEM((1, pairs_here), F32),
            pltpu.VMEM((2 * group * rows_here,) * 2, BF16),
            pltpu.VMEM((group * rows_here, K_PARTS * group * rows_here), BF16),
            pltpu.VMEM((heads_here * rows_here, length_all), F32),
            pltpu.VMEM((cols_here // 2, length_all // 2), BF16),
        ),
        "prepare",
        row_start.reshape(1),
        col_index.reshape(1),
        chain_bias,
        *[kept[k] for k in KEPT],
        residue_mask.reshape(1, -1),
        chain_index.reshape(1, -1),
        bias_in,
        triangle,
        scalars=3,
        scratch=(
            pltpu.VMEM((1, length_all), jnp.int32),
            pltpu.VMEM((1, length_all), jnp.int32),
            pltpu.VMEM(bias_in.shape, BF16),
            pltpu.VMEM(triangle.shape, BF16),
            pltpu.VMEM((GROUPS, bias_in.shape[0], LANES), F32),
            pltpu.SemaphoreType.DMA((len(KEPT) + 4,)),
        ),
        far=True,
    )
    near, made = dict(zip(KEPT, near)), near[len(KEPT) :]
    bias_blocks, gates_in, values_in, last_in, pair_live, spread_order, gather_order, extra, pick = made

    key_values_all, bias_blocks = lax.optimization_barrier((key_values_all, bias_blocks))
    bias_blocks = exchange(bias_blocks, "col")
    terms = local_kernel(
        attention_body,
        pltpu.VMEM((col_count, *sequence.shape), BF16),
        "attention",
        bias_blocks,
        extra,
        key_values_all,
        query,
        gate,
        near["attention_out"],
        scratch=(
            pltpu.VMEM((heads_here * rows_here, LANES), F32),
            pltpu.VMEM((rows_here, LANES), F32),
        ),
    )
    terms = exchange(terms, "col")
    width = outer_in.shape[1]
    sequence_summed, left_twice, right_copies = local_kernel(
        settle_body,
        (
            pltpu.VMEM(sequence.shape, BF16),
            pltpu.VMEM((rows_here, width), F32),
            pltpu.VMEM((row_count, rows_here // 2, width), BF16),
        ),
        "settle",
        terms,
        sequence_near,
        near["outer_in"],
    )
    rights = exchange(right_copies, ROW)
    tiles, pair_mid, out_gate = local_kernel(
        pair_body,
        (
            pltpu.VMEM((col_count, 2 * group, pairs_here), BF16),
            pltpu.VMEM((pairs_here, channels), F32),
            pltpu.VMEM((pairs_here, channels), F32),
        ),
        "pair",
        rights,
        pick,
        left_twice,
        near["pair"],
        near["outer_out"],
        gates_in,
        values_in,
        last_in,
        pair_live,
    )

    tiles = exchange(tiles, "col")
    panels = local_kernel(
        spread_body,
        pltpu.VMEM((row_count, few + rows_here, length_all // K_PARTS), BF16),
        "spread",
        tiles,
        spread_order,
    )
    panels = exchange(panels, ROW)
    product = lax.dot_general(
        panels[:, :few].reshape(-1, length_all // K_PARTS),
        panels[:, few:].reshape(-1, length_all // K_PARTS),
        (((1,), (1,)), ((), ())),
        preferred_element_type=F32,
    ).astype(BF16)
    product = exchange(product.reshape(row_count, few, length_all), ROW)
    product = local_kernel(
        gather_body,
        pltpu.VMEM((col_count, group, pairs_here), BF16),
        "gather",
        product,
        gather_order,
    )
    product = exchange(product, "col").reshape(channels, pairs_here)

    sequence_out, pair_out = local_kernel(
        tail_body,
        (
            jax.ShapeDtypeStruct(sequence.shape, BF16),
            jax.ShapeDtypeStruct((pairs_here, channels), BF16),
        ),
        "tail",
        sequence_summed,
        product,
        pair_mid,
        out_gate,
        near["triangle_out"],
        near["transition_up"],
        near["transition_down"],
        scratch=(
            pltpu.VMEM((pairs_here, channels), BF16),
            pltpu.SemaphoreType.DMA((TAIL_PARTS + 1,)),
        ),
    )
    pair_out = pair_out.reshape(rows_here, cols_here, channels)
    return (sequence_out, pair_out)


def solution(mesh):
    finer = Mesh(mesh.devices.reshape(4, 8, mesh.shape["col"]), ("row_0", "row_1", "col"))
    placed = (
        P(ROW, None),
        P(ROW, "col", None),
        P(),
        P(),
        P(None, None, "col"),
        P("col", None),
        P(),
        P(),
        P(),
        P(),
        P(),
        P(),
        P(),
        P(),
    )
    return jax.shard_map(
        per_device,
        mesh=finer,
        in_specs=placed,
        out_specs=(P(ROW, None), P(ROW, "col", None)),
        check_vma=False,
    )
```

```python
import math

import jax
import jax.numpy as jnp
from jax import lax
from jax.experimental import pallas as pl
from jax.experimental.pallas import tpu as pltpu
from jax.sharding import Mesh
from jax.sharding import PartitionSpec as P

ROW = ("row_0", "row_1")
PAIR_AT = tuple(u ^ 10 for u in range(16))
PAIR_PLACE = tuple(PAIR_AT.index(q) for q in range(16))
ROW_AT = tuple(2 * q + k for q in PAIR_AT for k in range(2))
ROW_PLACE = tuple(ROW_AT.index(r) for r in range(32))
COL_AT = tuple(p % 4 * 4 + (p // 4 ^ 1) for p in range(16))
COL_PLACE = tuple(COL_AT.index(q) for q in range(16))
BF16 = jnp.bfloat16
F32 = jnp.float32
K_PARTS = 2
I_PARTS = 2
TAIL_PARTS = 4
KEPT = (
    "pair",
    "attention_out",
    "outer_in",
    "outer_out",
    "triangle_out",
    "transition_up",
    "transition_down",
)
LANES = 128
GROUPS = 4


def exchange(blocks, axis):
    rows, cols = lax.axis_size(ROW), lax.axis_size("col")
    if axis == "col":
        groups = [[r * cols + q for q in COL_AT] for r in range(rows)]
    else:
        groups = [[r * cols + q for r in ROW_AT] for q in range(cols)]
    return lax.all_to_all(
        blocks, (*ROW, "col"), split_axis=0, concat_axis=0, tiled=True, axis_index_groups=groups
    )


def layer_norm(values, axis=-1):
    center = values - jnp.mean(values, axis=axis, keepdims=True)
    spread = jnp.mean(center * center, axis=axis, keepdims=True)
    return center * lax.rsqrt(spread + 1e-05)


def local_kernel(body, out_shape, name, *operands, scalars=0, scratch=(), far=False):
    space = pltpu.HBM if far else pltpu.VMEM
    spaces = [pltpu.SMEM if k < scalars else space for k in range(len(operands))]
    held = [
        pltpu.with_memory_space_constraint(x, space) if space is pltpu.VMEM else x
        for x, space in zip(operands, spaces)
    ]
    in_hbm = lambda x: isinstance(x, jax.ShapeDtypeStruct)
    return pl.pallas_call(
        body,
        out_shape=out_shape,
        in_specs=[pl.BlockSpec(memory_space=space) for space in spaces],
        out_specs=jax.tree.map(
            lambda x: pl.BlockSpec(memory_space=pltpu.HBM if in_hbm(x) else pltpu.VMEM), out_shape
        ),
        scratch_shapes=scratch,
        name=name,
    )(*held)


def fetch(sources, targets, arrived):
    copies = [
        pltpu.make_async_copy(source, target, arrived.at[k])
        for k, (source, target) in enumerate(zip(sources, targets))
    ]
    for copy in copies:
        copy.start()
    return copies


def mm(a, b, over_a, over_b):
    return lax.dot_general(a, b, (((over_a,), (over_b,)), ((), ())), preferred_element_type=F32)


def turn_lanes(value, groups):
    steps = groups % GROUPS
    return pltpu.roll(value, steps * (LANES // GROUPS), 1) if steps else value


def regroup(pick, shape):
    group = lax.broadcasted_iota(jnp.int32, shape, 1) // (LANES // GROUPS)
    tile = pick(0)
    for k in range(1, GROUPS):
        tile = jnp.where(group == k, pick(k), tile)
    return tile


def project_body(sequence, weights, key_values, query, gate, near, held, arrived):
    parts = [pl.ds(k * LANES, LANES) for k in range(2)]
    first_copy, *weight_copies = fetch(
        (sequence, *[weights.at[part] for part in parts]),
        (near, *[held.at[part] for part in parts]),
        arrived,
    )
    first_copy.wait()
    normed = layer_norm(near[...].astype(F32)).astype(BF16)
    projected = []
    for part, copy in zip(parts, weight_copies):
        copy.wait()
        projected.append(mm(normed, held[part], 1, 1))
    head, rest = projected
    rows = head.shape[0]
    first = lax.broadcasted_iota(jnp.int32, (rows, LANES), 1) < LANES // 2
    both = jnp.where(first, pltpu.roll(head, LANES // 2, 1), pltpu.roll(rest, LANES // 2, 1))
    key_values[...] = jnp.broadcast_to(both.astype(BF16)[None], key_values.shape)
    query[...] = jnp.where(first, head, 0.0).astype(BF16).astype(F32)
    gate[...] = jnp.where(first, 0.0, jax.nn.sigmoid(rest))


def prepare_body(row_start, col, chain_bias, *refs):
    count = len(KEPT)
    sources, targets = refs[: count + 4], refs[count + 4 : 2 * count + 4]
    blocks, gates_in, values_in, last_in, live, spread_order, gather_order, extra, pick = refs[
        2 * count + 4 : -6
    ]
    mask_near, chain_near, bias_near, triangle_near, turned_bias, arrived = refs[-6:]
    copies = fetch(
        sources, (*targets, mask_near, chain_near, bias_near, triangle_near), arrived
    )
    near = dict(zip(KEPT, targets))
    landed = dict(zip((*KEPT, "mask", "chain", "bias_in", "triangle"), copies))

    size = spread_order.shape[0]
    n = lax.broadcasted_iota(jnp.int32, spread_order.shape, 0)
    m = lax.broadcasted_iota(jnp.int32, spread_order.shape, 1)
    rows = live.shape[1] // (LANES // GROUPS)
    wanted = n % rows * (size // rows) + n // rows
    spread_order[...] = jnp.where(m == wanted, 1.0, 0.0).astype(BF16)
    size = gather_order.shape[0]
    group, few = size // rows, rows // I_PARTS
    n = lax.broadcasted_iota(jnp.int32, gather_order.shape, 0)
    m = lax.broadcasted_iota(jnp.int32, gather_order.shape, 1)
    i, c = n // group, n % group
    wanted = (i // few * group + c) * few + i % few
    gather_order[...] = jnp.where(m % size == wanted, 1.0, 0.0).astype(BF16)

    n = lax.broadcasted_iota(jnp.int32, pick.shape, 0)
    m = lax.broadcasted_iota(jnp.int32, pick.shape, 1)
    place = jnp.zeros(pick.shape, jnp.int32)
    for q, u in enumerate(PAIR_PLACE):
        place = jnp.where(col[0] == q, u, place)
    pick[...] = jnp.where(m == place * pick.shape[0] + n, 1.0, 0.0).astype(BF16)

    landed["pair"].wait()
    landed["bias_in"].wait()
    wide = near["pair"][...].astype(F32)
    turned = jnp.concatenate([wide[GROUPS * (p % GROUPS) + p // GROUPS] for p in range(rows)], axis=0)
    normed = layer_norm(turned).astype(BF16)
    heads = bias_near.shape[0]
    n = lax.broadcasted_iota(jnp.int32, (heads, heads), 0)
    m = lax.broadcasted_iota(jnp.int32, (heads, heads), 1)
    place = n // 2
    by_place = jnp.where(m == (place % 4 * 4 + (place // 4 ^ 1)) * 2 + n % 2, 1.0, 0.0).astype(BF16)
    bias = mm(mm(by_place, bias_near[...], 1, 0).astype(BF16), normed, 1, 1)
    columns = blocks.shape[0]
    for t in range(GROUPS):
        turned_bias[t] = bias[:, t * LANES : (t + 1) * LANES]
        for h in range(2):
            blocks[:, h * GROUPS + t, :] = turned_bias[t, pl.ds(h, columns, stride=2), :]

    landed["mask"].wait()
    mask = mask_near[...].astype(F32).astype(BF16)
    length = mask.shape[1]
    residue = lax.broadcasted_iota(jnp.int32, (length, live.shape[1]), 0)
    pair = lax.broadcasted_iota(jnp.int32, (length, live.shape[1]), 1)
    of_row = jnp.where(residue == row_start[0] + pair // (LANES // GROUPS), 1.0, 0.0).astype(BF16)
    of_col = jnp.where(residue == col[0] * (LANES // GROUPS) + pair % (LANES // GROUPS), 1.0, 0.0).astype(BF16)
    mask = jnp.broadcast_to(mask, (8, length))
    live[...] = (mm(mask, of_row, 1, 0) * mm(mask, of_col, 1, 0))[:1]

    landed["chain"].wait()
    eight = blocks.shape[1]
    four = eight // 2
    position = lax.broadcasted_iota(jnp.int32, (eight, length), 1)
    row = lax.broadcasted_iota(jnp.int32, (eight, length), 0)
    chains = jnp.broadcast_to(chain_near[...].astype(F32), (eight, length))
    kept = jnp.broadcast_to(mask_near[...], (eight, length)) == 1
    offset = jnp.where(row < four, chain_bias[2 * col[0]], chain_bias[2 * col[0] + 1])
    for g in range(GROUPS):
        here = position == row_start[0] + g * four + row % four
        own_chain = jnp.sum(jnp.where(here, chains, 0.0), axis=1, keepdims=True)
        added = jnp.where(chains == own_chain, offset, 0.0)
        extra[g * eight : (g + 1) * eight, :] = jnp.where(kept | here, added, -jnp.inf)

    landed["triangle"].wait()
    half = gates_in.shape[1] // 2
    for k, target in enumerate((gates_in, values_in, gates_in, values_in)):
        side = half * (k // 2)
        across = jnp.transpose(triangle_near[k].astype(F32)).astype(BF16)
        target[:, side : side + half, :] = across.reshape(target.shape[0], half, LANES)
    last_in[...] = triangle_near[4]
    for name in KEPT:
        if name != "pair":
            landed[name].wait()


def attention_body(blocks, extra, key_values, query, gate, attention_out, copies, spread, joined):
    count, eight, _ = blocks.shape
    four = eight // 2
    length = count * (LANES // GROUPS)
    lane = lax.broadcasted_iota(jnp.int32, (four, LANES), 1)
    for g in range(GROUPS):
        taken = query[g * four : (g + 1) * four, :]
        for h in range(2):
            own = (lane >= h * (LANES // 4)) & (lane < (h + 1) * (LANES // 4))
            spread[g * eight + h * four : g * eight + (h + 1) * four, :] = jnp.where(own, taken, 0.0)
    everyone = jnp.concatenate([key_values[p] for p in ROW_PLACE], axis=0)
    raw = mm(spread[...].astype(BF16), everyone, 1, 1)
    raw = raw * (1.0 / math.sqrt(LANES // 4))
    biases = []
    for g in range(GROUPS):
        pieces = []
        for tile in range(count // GROUPS):
            pieces.append(
                regroup(
                    lambda k, tile=tile, g=g: turn_lanes(blocks[COL_PLACE[GROUPS * tile + k]], k - g),
                    (eight, LANES),
                )
            )
        biases.append(jnp.concatenate(pieces, axis=1))
    scores = raw + jnp.concatenate(biases, axis=0) + extra[...]
    raised = jnp.exp(scores - jnp.max(scores, axis=1, keepdims=True))
    weights = [raised / jnp.sum(raised, axis=1, keepdims=True)]
    mixed = mm(jnp.concatenate(weights, axis=0).astype(BF16), everyone, 1, 0)
    for g in range(GROUPS):
        upper = mixed[g * eight : g * eight + four]
        lower = mixed[g * eight + four : (g + 1) * eight]
        joined[g * four : (g + 1) * four, :] = jnp.where(lane < LANES * 3 // 4, upper, lower)
    gated = pltpu.roll(gate[...] * joined[...], LANES // 2, 1)[:, : LANES // 2].astype(BF16)
    terms = mm(gated, attention_out[...], 1, 0).astype(BF16)
    copies[...] = jnp.broadcast_to(terms[None], copies.shape)


def spread_body(tiles, order, panels):
    count, chans, pairs = tiles.shape
    rows = pairs // (LANES // GROUPS)
    per = count // GROUPS
    by_row = []
    for i in range(rows):
        at, g = i // GROUPS * LANES, i % GROUPS
        by_row.append(
            jnp.concatenate(
                [
                    regroup(
                        lambda k, tile=tile, g=g, at=at: turn_lanes(
                            tiles[COL_PLACE[GROUPS * tile + k], :, at : at + LANES].astype(F32), k - g
                        ),
                        (chans, LANES),
                    )
                    for tile in range(per)
                ],
                axis=1,
            )
        )
    turned = mm(order[...], jnp.concatenate(by_row, axis=0).astype(BF16), 1, 0).astype(BF16)
    half = chans // 2
    few = rows // I_PARTS
    wide = turned.shape[1] // K_PARTS
    for k in range(K_PARTS):
        for i in range(I_PARTS):
            for c in range(half):
                block = (k * I_PARTS + i) * half + c
                at = c * rows + i * few
                panels[block, :few, :] = turned[at : at + few, k * wide : (k + 1) * wide]
                at = (half + c) * rows
                panels[block, few:, :] = turned[at : at + rows, k * wide : (k + 1) * wide]


def gather_body(parts, order, blocks):
    total, few, length = parts.shape
    count, group, pairs = blocks.shape
    rows = pairs // (LANES // GROUPS)
    summed = mm(order[...], parts[...].reshape(total * few, length), 1, 0)
    for q in range(count):
        place = PAIR_PLACE[COL_AT[q]]
        tile, s = place // GROUPS, place % GROUPS
        pieces = []
        for t in range(rows // GROUPS):
            pieces.append(
                regroup(
                    lambda k, t=t, tile=tile, s=s: turn_lanes(
                        summed[
                            (GROUPS * t + k) * group : (GROUPS * t + k + 1) * group,
                            tile * LANES : (tile + 1) * LANES,
                        ],
                        k - s,
                    ),
                    (group, LANES),
                )
            )
        blocks[q] = jnp.concatenate(pieces, axis=1).astype(BF16)


def settle_body(terms, sequence, outer_in, sequence_out, left_twice, right_copies):
    update = jnp.sum(terms[...].astype(F32), axis=0)
    summed = (sequence[...].astype(F32) + update).astype(BF16)
    sequence_out[...] = summed
    normed = layer_norm(summed.astype(F32)).astype(BF16)
    outer_rows = mm(normed, outer_in[...], 1, 0).astype(BF16).astype(F32)
    rows, width = outer_rows.shape
    half = width // 2
    first = lax.broadcasted_iota(jnp.int32, (rows, width), 1) < half
    turned = pltpu.roll(outer_rows, half, 1)
    left_twice[...] = jnp.where(first, outer_rows, turned)
    packed = jnp.where(first[: rows // 2], turned[: rows // 2], outer_rows[rows // 2 :])
    right_copies[...] = jnp.broadcast_to(packed.astype(BF16)[None], right_copies.shape)


def pair_body(
    rights,
    pick,
    left_twice,
    pair,
    outer_out,
    gates_in,
    values_in,
    last_in,
    live,
    tiles,
    mid,
    out_gate,
):
    rows, cols, channels = pair.shape
    half = channels // 2
    taken = mm(pick[...], rights[...].reshape(-1, channels), 1, 0)
    taken = taken.reshape(cols // rows, rows // 2, channels)
    first = lax.broadcasted_iota(jnp.int32, (rows // 2, channels), 1) < half
    pieces = []
    for k in range(cols // rows):
        turned = pltpu.roll(taken[k], half, 1)
        pieces.append(jnp.where(first, taken[k], turned))
        pieces.append(jnp.where(first, turned, taken[k]))
    right_twice = jnp.concatenate(pieces, axis=0)
    left = left_twice[...][:, None, :]
    right = right_twice[None, :, :]
    lane = lax.broadcasted_iota(jnp.int32, (rows, cols, channels), 2)
    feat = jnp.where(lane < half, left * right, left - right).astype(BF16)
    feat = feat.reshape(rows * cols, channels)
    pair_mid = pair[...].astype(F32).reshape(rows * cols, channels) + mm(feat, outer_out[...], 1, 0)
    mid[...] = pair_mid
    normed = layer_norm(pair_mid).astype(BF16)
    flat = (-1, channels)
    opened = jax.nn.sigmoid(mm(gates_in[...].reshape(flat), normed, 1, 1))
    operands = opened * mm(values_in[...].reshape(flat), normed, 1, 1) * live[...]
    tiles[...] = operands.astype(BF16).reshape(tiles.shape)
    out_gate[...] = jax.nn.sigmoid(mm(normed, last_in[...], 1, 0))


def tail_body(
    sequence_near,
    product,
    mid,
    out_gate,
    triangle_out,
    transition_up,
    transition_down,
    sequence_out,
    out,
    held,
    left,
):
    copies = [pltpu.make_async_copy(sequence_near, sequence_out, left.at[TAIL_PARTS])]
    copies[0].start()
    normed_product = layer_norm(product[...].astype(F32), axis=0)
    normed_product = jnp.transpose(normed_product).astype(BF16)
    late = mid[...] + out_gate[...] * mm(normed_product, triangle_out[...], 1, 0)
    normed_late = layer_norm(late).astype(BF16)
    hidden = jnp.maximum(mm(normed_late, transition_up[...], 1, 0), 0.0).astype(BF16)
    part = mid.shape[0] // TAIL_PARTS
    for k in range(TAIL_PARTS):
        here = slice(k * part, (k + 1) * part)
        held[here] = (late[here] + mm(hidden[here], transition_down[...], 1, 0)).astype(BF16)
        copies.append(pltpu.make_async_copy(held.at[here], out.at[here], left.at[k]))
        copies[-1].start()
    for copy in copies:
        copy.wait()


def per_device(
    sequence,
    pair_state,
    residue_mask,
    chain_index,
    attention_in,
    attention_out,
    bias_weight,
    chain_bias,
    outer_in,
    outer_out,
    triangle_in,
    triangle_out,
    transition_up,
    transition_down,
):
    rows_here, cols_here, channels = pair_state.shape
    length_all = residue_mask.shape[0]
    pairs_here = rows_here * cols_here
    row_index = lax.axis_index(ROW)
    col_index = lax.axis_index("col")
    row_count = lax.axis_size(ROW)
    col_count = lax.axis_size("col")
    row_start = row_index * rows_here

    group = channels // col_count
    heads_here = bias_weight.shape[1] // col_count

    weights = jnp.transpose(attention_in, (1, 2, 0)).reshape(-1, sequence.shape[1])
    key_values, query, gate, sequence_near = local_kernel(
        project_body,
        (
            pltpu.VMEM((row_count, rows_here, LANES), BF16),
            pltpu.VMEM((rows_here, LANES), F32),
            pltpu.VMEM((rows_here, LANES), F32),
            pltpu.VMEM(sequence.shape, BF16),
        ),
        "project",
        sequence,
        weights,
        scratch=(pltpu.VMEM(weights.shape, BF16), pltpu.SemaphoreType.DMA((3,))),
        far=True,
    )
    key_values_all = exchange(key_values, ROW)

    bias_in = jnp.transpose(bias_weight)
    triangle = jnp.transpose(triangle_in, (1, 0, 2))
    kept = dict(
        pair=pair_state,
        attention_out=attention_out,
        outer_in=outer_in,
        outer_out=outer_out,
        triangle_out=triangle_out,
        transition_up=transition_up,
        transition_down=transition_down,
    )
    few = rows_here // I_PARTS
    near = local_kernel(
        prepare_body,
        (
            *[pltpu.VMEM(kept[k].shape, kept[k].dtype) for k in KEPT],
            pltpu.VMEM((col_count, heads_here * GROUPS, LANES), F32),
            pltpu.VMEM((col_count, 2 * group, channels), BF16),
            pltpu.VMEM((col_count, 2 * group, channels), BF16),
            pltpu.VMEM((channels, channels), BF16),
            pltpu.VMEM((1, pairs_here), F32),
            pltpu.VMEM((2 * group * rows_here,) * 2, BF16),
            pltpu.VMEM((group * rows_here, K_PARTS * group * rows_here), BF16),
            pltpu.VMEM((heads_here * rows_here, length_all), F32),
            pltpu.VMEM((cols_here // 2, length_all // 2), BF16),
        ),
        "prepare",
        row_start.reshape(1),
        col_index.reshape(1),
        chain_bias,
        *[kept[k] for k in KEPT],
        residue_mask.reshape(1, -1),
        chain_index.reshape(1, -1),
        bias_in,
        triangle,
        scalars=3,
        scratch=(
            pltpu.VMEM((1, length_all), jnp.int32),
            pltpu.VMEM((1, length_all), jnp.int32),
            pltpu.VMEM(bias_in.shape, BF16),
            pltpu.VMEM(triangle.shape, BF16),
            pltpu.VMEM((GROUPS, bias_in.shape[0], LANES), F32),
            pltpu.SemaphoreType.DMA((len(KEPT) + 4,)),
        ),
        far=True,
    )
    near, made = dict(zip(KEPT, near)), near[len(KEPT) :]
    bias_blocks, gates_in, values_in, last_in, pair_live, spread_order, gather_order, extra, pick = made

    key_values_all, bias_blocks = lax.optimization_barrier((key_values_all, bias_blocks))
    bias_blocks = exchange(bias_blocks, "col")
    terms = local_kernel(
        attention_body,
        pltpu.VMEM((col_count, *sequence.shape), BF16),
        "attention",
        bias_blocks,
        extra,
        key_values_all,
        query,
        gate,
        near["attention_out"],
        scratch=(
            pltpu.VMEM((heads_here * rows_here, LANES), F32),
            pltpu.VMEM((rows_here, LANES), F32),
        ),
    )
    terms = exchange(terms, "col")
    width = outer_in.shape[1]
    sequence_summed, left_twice, right_copies = local_kernel(
        settle_body,
        (
            pltpu.VMEM(sequence.shape, BF16),
            pltpu.VMEM((rows_here, width), F32),
            pltpu.VMEM((row_count, rows_here // 2, width), BF16),
        ),
        "settle",
        terms,
        sequence_near,
        near["outer_in"],
    )
    rights = exchange(right_copies, ROW)
    tiles, pair_mid, out_gate = local_kernel(
        pair_body,
        (
            pltpu.VMEM((col_count, 2 * group, pairs_here), BF16),
            pltpu.VMEM((pairs_here, channels), F32),
            pltpu.VMEM((pairs_here, channels), F32),
        ),
        "pair",
        rights,
        pick,
        left_twice,
        near["pair"],
        near["outer_out"],
        gates_in,
        values_in,
        last_in,
        pair_live,
    )

    tiles = exchange(tiles, "col")
    panels = local_kernel(
        spread_body,
        pltpu.VMEM((row_count, few + rows_here, length_all // K_PARTS), BF16),
        "spread",
        tiles,
        spread_order,
    )
    panels = exchange(panels, ROW)
    product = lax.dot_general(
        panels[:, :few].reshape(-1, length_all // K_PARTS),
        panels[:, few:].reshape(-1, length_all // K_PARTS),
        (((1,), (1,)), ((), ())),
        preferred_element_type=F32,
    ).astype(BF16)
    product = exchange(product.reshape(row_count, few, length_all), ROW)
    product = local_kernel(
        gather_body,
        pltpu.VMEM((col_count, group, pairs_here), BF16),
        "gather",
        product,
        gather_order,
    )
    product = exchange(product, "col").reshape(channels, pairs_here)

    sequence_out, pair_out = local_kernel(
        tail_body,
        (
            jax.ShapeDtypeStruct(sequence.shape, BF16),
            jax.ShapeDtypeStruct((pairs_here, channels), BF16),
        ),
        "tail",
        sequence_summed,
        product,
        pair_mid,
        out_gate,
        near["triangle_out"],
        near["transition_up"],
        near["transition_down"],
        scratch=(
            pltpu.VMEM((pairs_here, channels), BF16),
            pltpu.SemaphoreType.DMA((TAIL_PARTS + 1,)),
        ),
    )
    pair_out = pair_out.reshape(rows_here, cols_here, channels)
    return (sequence_out, pair_out)


def solution(mesh):
    finer = Mesh(mesh.devices.reshape(4, 8, mesh.shape["col"]), ("row_0", "row_1", "col"))
    placed = (
        P(ROW, None),
        P(ROW, "col", None),
        P(),
        P(),
        P(None, None, "col"),
        P("col", None),
        P(),
        P(),
        P(),
        P(),
        P(),
        P(),
        P(),
        P(),
    )
    return jax.shard_map(
        per_device,
        mesh=finer,
        in_specs=placed,
        out_specs=(P(ROW, None), P(ROW, "col", None)),
        check_vma=False,
    )
```

```python
import math

import jax
import jax.numpy as jnp
from jax import lax
from jax.experimental import pallas as pl
from jax.experimental.pallas import tpu as pltpu
from jax.sharding import Mesh
from jax.sharding import PartitionSpec as P

ROW = ("row_0", "row_1")
PAIR_AT = tuple(u ^ 4 for u in range(16))
PAIR_PLACE = tuple(PAIR_AT.index(q) for q in range(16))
ROW_AT = tuple(2 * q + k for q in PAIR_AT for k in range(2))
ROW_PLACE = tuple(ROW_AT.index(r) for r in range(32))
COL_AT = tuple(p % 4 * 4 + (p // 4 ^ 1) for p in range(16))
COL_PLACE = tuple(COL_AT.index(q) for q in range(16))
BF16 = jnp.bfloat16
F32 = jnp.float32
K_PARTS = 2
I_PARTS = 2
TAIL_PARTS = 4
KEPT = (
    "pair",
    "attention_out",
    "outer_in",
    "outer_out",
    "triangle_out",
    "transition_up",
    "transition_down",
)
LANES = 128
GROUPS = 4


def exchange(blocks, axis):
    rows, cols = lax.axis_size(ROW), lax.axis_size("col")
    if axis == "col":
        groups = [[r * cols + q for q in COL_AT] for r in range(rows)]
    else:
        groups = [[r * cols + q for r in ROW_AT] for q in range(cols)]
    return lax.all_to_all(
        blocks, (*ROW, "col"), split_axis=0, concat_axis=0, tiled=True, axis_index_groups=groups
    )


def layer_norm(values, axis=-1):
    center = values - jnp.mean(values, axis=axis, keepdims=True)
    spread = jnp.mean(center * center, axis=axis, keepdims=True)
    return center * lax.rsqrt(spread + 1e-05)


def local_kernel(body, out_shape, name, *operands, scalars=0, scratch=(), far=False):
    space = pltpu.HBM if far else pltpu.VMEM
    spaces = [pltpu.SMEM if k < scalars else space for k in range(len(operands))]
    held = [
        pltpu.with_memory_space_constraint(x, space) if space is pltpu.VMEM else x
        for x, space in zip(operands, spaces)
    ]
    in_hbm = lambda x: isinstance(x, jax.ShapeDtypeStruct)
    return pl.pallas_call(
        body,
        out_shape=out_shape,
        in_specs=[pl.BlockSpec(memory_space=space) for space in spaces],
        out_specs=jax.tree.map(
            lambda x: pl.BlockSpec(memory_space=pltpu.HBM if in_hbm(x) else pltpu.VMEM), out_shape
        ),
        scratch_shapes=scratch,
        name=name,
    )(*held)


def fetch(sources, targets, arrived):
    copies = [
        pltpu.make_async_copy(source, target, arrived.at[k])
        for k, (source, target) in enumerate(zip(sources, targets))
    ]
    for copy in copies:
        copy.start()
    return copies


def mm(a, b, over_a, over_b):
    return lax.dot_general(a, b, (((over_a,), (over_b,)), ((), ())), preferred_element_type=F32)


def turn_lanes(value, groups):
    steps = groups % GROUPS
    return pltpu.roll(value, steps * (LANES // GROUPS), 1) if steps else value


def regroup(pick, shape):
    group = lax.broadcasted_iota(jnp.int32, shape, 1) // (LANES // GROUPS)
    tile = pick(0)
    for k in range(1, GROUPS):
        tile = jnp.where(group == k, pick(k), tile)
    return tile


def project_body(sequence, weights, key_values, query, gate, near, held, arrived):
    parts = [pl.ds(k * LANES, LANES) for k in range(2)]
    first_copy, *weight_copies = fetch(
        (sequence, *[weights.at[part] for part in parts]),
        (near, *[held.at[part] for part in parts]),
        arrived,
    )
    first_copy.wait()
    normed = layer_norm(near[...].astype(F32)).astype(BF16)
    projected = []
    for part, copy in zip(parts, weight_copies):
        copy.wait()
        projected.append(mm(normed, held[part], 1, 1))
    head, rest = projected
    rows = head.shape[0]
    first = lax.broadcasted_iota(jnp.int32, (rows, LANES), 1) < LANES // 2
    both = jnp.where(first, pltpu.roll(head, LANES // 2, 1), pltpu.roll(rest, LANES // 2, 1))
    key_values[...] = jnp.broadcast_to(both.astype(BF16)[None], key_values.shape)
    query[...] = jnp.where(first, head, 0.0).astype(BF16).astype(F32)
    gate[...] = jnp.where(first, 0.0, jax.nn.sigmoid(rest))


def prepare_body(row_start, col, chain_bias, *refs):
    count = len(KEPT)
    sources, targets = refs[: count + 4], refs[count + 4 : 2 * count + 4]
    blocks, gates_in, values_in, last_in, live, spread_order, gather_order, extra, pick = refs[
        2 * count + 4 : -6
    ]
    mask_near, chain_near, bias_near, triangle_near, turned_bias, arrived = refs[-6:]
    copies = fetch(
        sources, (*targets, mask_near, chain_near, bias_near, triangle_near), arrived
    )
    near = dict(zip(KEPT, targets))
    landed = dict(zip((*KEPT, "mask", "chain", "bias_in", "triangle"), copies))

    size = spread_order.shape[0]
    n = lax.broadcasted_iota(jnp.int32, spread_order.shape, 0)
    m = lax.broadcasted_iota(jnp.int32, spread_order.shape, 1)
    rows = live.shape[1] // (LANES // GROUPS)
    wanted = n % rows * (size // rows) + n // rows
    spread_order[...] = jnp.where(m == wanted, 1.0, 0.0).astype(BF16)
    size = gather_order.shape[0]
    group, few = size // rows, rows // I_PARTS
    n = lax.broadcasted_iota(jnp.int32, gather_order.shape, 0)
    m = lax.broadcasted_iota(jnp.int32, gather_order.shape, 1)
    i, c = n // group, n % group
    wanted = (i // few * group + c) * few + i % few
    gather_order[...] = jnp.where(m % size == wanted, 1.0, 0.0).astype(BF16)

    n = lax.broadcasted_iota(jnp.int32, pick.shape, 0)
    m = lax.broadcasted_iota(jnp.int32, pick.shape, 1)
    place = jnp.zeros(pick.shape, jnp.int32)
    for q, u in enumerate(PAIR_PLACE):
        place = jnp.where(col[0] == q, u, place)
    pick[...] = jnp.where(m == place * pick.shape[0] + n, 1.0, 0.0).astype(BF16)

    landed["pair"].wait()
    landed["bias_in"].wait()
    wide = near["pair"][...].astype(F32)
    turned = jnp.concatenate([wide[GROUPS * (p % GROUPS) + p // GROUPS] for p in range(rows)], axis=0)
    normed = layer_norm(turned).astype(BF16)
    heads = bias_near.shape[0]
    n = lax.broadcasted_iota(jnp.int32, (heads, heads), 0)
    m = lax.broadcasted_iota(jnp.int32, (heads, heads), 1)
    place = n // 2
    by_place = jnp.where(m == (place % 4 * 4 + (place // 4 ^ 1)) * 2 + n % 2, 1.0, 0.0).astype(BF16)
    bias = mm(mm(by_place, bias_near[...], 1, 0).astype(BF16), normed, 1, 1)
    columns = blocks.shape[0]
    for t in range(GROUPS):
        turned_bias[t] = bias[:, t * LANES : (t + 1) * LANES]
        for h in range(2):
            blocks[:, h * GROUPS + t, :] = turned_bias[t, pl.ds(h, columns, stride=2), :]

    landed["mask"].wait()
    mask = mask_near[...].astype(F32).astype(BF16)
    length = mask.shape[1]
    residue = lax.broadcasted_iota(jnp.int32, (length, live.shape[1]), 0)
    pair = lax.broadcasted_iota(jnp.int32, (length, live.shape[1]), 1)
    of_row = jnp.where(residue == row_start[0] + pair // (LANES // GROUPS), 1.0, 0.0).astype(BF16)
    of_col = jnp.where(residue == col[0] * (LANES // GROUPS) + pair % (LANES // GROUPS), 1.0, 0.0).astype(BF16)
    mask = jnp.broadcast_to(mask, (8, length))
    live[...] = (mm(mask, of_row, 1, 0) * mm(mask, of_col, 1, 0))[:1]

    landed["chain"].wait()
    eight = blocks.shape[1]
    four = eight // 2
    position = lax.broadcasted_iota(jnp.int32, (eight, length), 1)
    row = lax.broadcasted_iota(jnp.int32, (eight, length), 0)
    chains = jnp.broadcast_to(chain_near[...].astype(F32), (eight, length))
    kept = jnp.broadcast_to(mask_near[...], (eight, length)) == 1
    offset = jnp.where(row < four, chain_bias[2 * col[0]], chain_bias[2 * col[0] + 1])
    for g in range(GROUPS):
        here = position == row_start[0] + g * four + row % four
        own_chain = jnp.sum(jnp.where(here, chains, 0.0), axis=1, keepdims=True)
        added = jnp.where(chains == own_chain, offset, 0.0)
        extra[g * eight : (g + 1) * eight, :] = jnp.where(kept | here, added, -jnp.inf)

    landed["triangle"].wait()
    half = gates_in.shape[1] // 2
    for k, target in enumerate((gates_in, values_in, gates_in, values_in)):
        side = half * (k // 2)
        across = jnp.transpose(triangle_near[k].astype(F32)).astype(BF16)
        target[:, side : side + half, :] = across.reshape(target.shape[0], half, LANES)
    last_in[...] = triangle_near[4]
    for name in KEPT:
        if name != "pair":
            landed[name].wait()


def attention_body(blocks, extra, key_values, query, gate, attention_out, copies, spread, joined):
    count, eight, _ = blocks.shape
    four = eight // 2
    length = count * (LANES // GROUPS)
    lane = lax.broadcasted_iota(jnp.int32, (four, LANES), 1)
    for g in range(GROUPS):
        taken = query[g * four : (g + 1) * four, :]
        for h in range(2):
            own = (lane >= h * (LANES // 4)) & (lane < (h + 1) * (LANES // 4))
            spread[g * eight + h * four : g * eight + (h + 1) * four, :] = jnp.where(own, taken, 0.0)
    everyone = jnp.concatenate([key_values[p] for p in ROW_PLACE], axis=0)
    raw = mm(spread[...].astype(BF16), everyone, 1, 1)
    raw = raw * (1.0 / math.sqrt(LANES // 4))
    biases = []
    for g in range(GROUPS):
        pieces = []
        for tile in range(count // GROUPS):
            pieces.append(
                regroup(
                    lambda k, tile=tile, g=g: turn_lanes(blocks[COL_PLACE[GROUPS * tile + k]], k - g),
                    (eight, LANES),
                )
            )
        biases.append(jnp.concatenate(pieces, axis=1))
    scores = raw + jnp.concatenate(biases, axis=0) + extra[...]
    raised = jnp.exp(scores - jnp.max(scores, axis=1, keepdims=True))
    weights = [raised / jnp.sum(raised, axis=1, keepdims=True)]
    mixed = mm(jnp.concatenate(weights, axis=0).astype(BF16), everyone, 1, 0)
    for g in range(GROUPS):
        upper = mixed[g * eight : g * eight + four]
        lower = mixed[g * eight + four : (g + 1) * eight]
        joined[g * four : (g + 1) * four, :] = jnp.where(lane < LANES * 3 // 4, upper, lower)
    gated = pltpu.roll(gate[...] * joined[...], LANES // 2, 1)[:, : LANES // 2].astype(BF16)
    terms = mm(gated, attention_out[...], 1, 0).astype(BF16)
    copies[...] = jnp.broadcast_to(terms[None], copies.shape)


def spread_body(tiles, order, panels):
    count, chans, pairs = tiles.shape
    rows = pairs // (LANES // GROUPS)
    per = count // GROUPS
    by_row = []
    for i in range(rows):
        at, g = i // GROUPS * LANES, i % GROUPS
        by_row.append(
            jnp.concatenate(
                [
                    regroup(
                        lambda k, tile=tile, g=g, at=at: turn_lanes(
                            tiles[COL_PLACE[GROUPS * tile + k], :, at : at + LANES].astype(F32), k - g
                        ),
                        (chans, LANES),
                    )
                    for tile in range(per)
                ],
                axis=1,
            )
        )
    turned = mm(order[...], jnp.concatenate(by_row, axis=0).astype(BF16), 1, 0).astype(BF16)
    half = chans // 2
    few = rows // I_PARTS
    wide = turned.shape[1] // K_PARTS
    for k in range(K_PARTS):
        for i in range(I_PARTS):
            for c in range(half):
                block = (k * I_PARTS + i) * half + c
                at = c * rows + i * few
                panels[block, :few, :] = turned[at : at + few, k * wide : (k + 1) * wide]
                at = (half + c) * rows
                panels[block, few:, :] = turned[at : at + rows, k * wide : (k + 1) * wide]


def gather_body(parts, order, blocks):
    total, few, length = parts.shape
    count, group, pairs = blocks.shape
    rows = pairs // (LANES // GROUPS)
    summed = mm(order[...], parts[...].reshape(total * few, length), 1, 0)
    for q in range(count):
        place = PAIR_PLACE[COL_AT[q]]
        tile, s = place // GROUPS, place % GROUPS
        pieces = []
        for t in range(rows // GROUPS):
            pieces.append(
                regroup(
                    lambda k, t=t, tile=tile, s=s: turn_lanes(
                        summed[
                            (GROUPS * t + k) * group : (GROUPS * t + k + 1) * group,
                            tile * LANES : (tile + 1) * LANES,
                        ],
                        k - s,
                    ),
                    (group, LANES),
                )
            )
        blocks[q] = jnp.concatenate(pieces, axis=1).astype(BF16)


def settle_body(terms, sequence, outer_in, sequence_out, left_twice, right_copies):
    update = jnp.sum(terms[...].astype(F32), axis=0)
    summed = (sequence[...].astype(F32) + update).astype(BF16)
    sequence_out[...] = summed
    normed = layer_norm(summed.astype(F32)).astype(BF16)
    outer_rows = mm(normed, outer_in[...], 1, 0).astype(BF16).astype(F32)
    rows, width = outer_rows.shape
    half = width // 2
    first = lax.broadcasted_iota(jnp.int32, (rows, width), 1) < half
    turned = pltpu.roll(outer_rows, half, 1)
    left_twice[...] = jnp.where(first, outer_rows, turned)
    packed = jnp.where(first[: rows // 2], turned[: rows // 2], outer_rows[rows // 2 :])
    right_copies[...] = jnp.broadcast_to(packed.astype(BF16)[None], right_copies.shape)


def pair_body(
    rights,
    pick,
    left_twice,
    pair,
    outer_out,
    gates_in,
    values_in,
    last_in,
    live,
    tiles,
    mid,
    out_gate,
):
    rows, cols, channels = pair.shape
    half = channels // 2
    taken = mm(pick[...], rights[...].reshape(-1, channels), 1, 0)
    taken = taken.reshape(cols // rows, rows // 2, channels)
    first = lax.broadcasted_iota(jnp.int32, (rows // 2, channels), 1) < half
    pieces = []
    for k in range(cols // rows):
        turned = pltpu.roll(taken[k], half, 1)
        pieces.append(jnp.where(first, taken[k], turned))
        pieces.append(jnp.where(first, turned, taken[k]))
    right_twice = jnp.concatenate(pieces, axis=0)
    left = left_twice[...][:, None, :]
    right = right_twice[None, :, :]
    lane = lax.broadcasted_iota(jnp.int32, (rows, cols, channels), 2)
    feat = jnp.where(lane < half, left * right, left - right).astype(BF16)
    feat = feat.reshape(rows * cols, channels)
    pair_mid = pair[...].astype(F32).reshape(rows * cols, channels) + mm(feat, outer_out[...], 1, 0)
    mid[...] = pair_mid
    normed = layer_norm(pair_mid).astype(BF16)
    flat = (-1, channels)
    opened = jax.nn.sigmoid(mm(gates_in[...].reshape(flat), normed, 1, 1))
    operands = opened * mm(values_in[...].reshape(flat), normed, 1, 1) * live[...]
    tiles[...] = operands.astype(BF16).reshape(tiles.shape)
    out_gate[...] = jax.nn.sigmoid(mm(normed, last_in[...], 1, 0))


def tail_body(
    sequence_near,
    product,
    mid,
    out_gate,
    triangle_out,
    transition_up,
    transition_down,
    sequence_out,
    out,
    held,
    left,
):
    copies = [pltpu.make_async_copy(sequence_near, sequence_out, left.at[TAIL_PARTS])]
    copies[0].start()
    normed_product = layer_norm(product[...].astype(F32), axis=0)
    normed_product = jnp.transpose(normed_product).astype(BF16)
    late = mid[...] + out_gate[...] * mm(normed_product, triangle_out[...], 1, 0)
    normed_late = layer_norm(late).astype(BF16)
    hidden = jnp.maximum(mm(normed_late, transition_up[...], 1, 0), 0.0).astype(BF16)
    part = mid.shape[0] // TAIL_PARTS
    for k in range(TAIL_PARTS):
        here = slice(k * part, (k + 1) * part)
        held[here] = (late[here] + mm(hidden[here], transition_down[...], 1, 0)).astype(BF16)
        copies.append(pltpu.make_async_copy(held.at[here], out.at[here], left.at[k]))
        copies[-1].start()
    for copy in copies:
        copy.wait()


def per_device(
    sequence,
    pair_state,
    residue_mask,
    chain_index,
    attention_in,
    attention_out,
    bias_weight,
    chain_bias,
    outer_in,
    outer_out,
    triangle_in,
    triangle_out,
    transition_up,
    transition_down,
):
    rows_here, cols_here, channels = pair_state.shape
    length_all = residue_mask.shape[0]
    pairs_here = rows_here * cols_here
    row_index = lax.axis_index(ROW)
    col_index = lax.axis_index("col")
    row_count = lax.axis_size(ROW)
    col_count = lax.axis_size("col")
    row_start = row_index * rows_here

    group = channels // col_count
    heads_here = bias_weight.shape[1] // col_count

    weights = jnp.transpose(attention_in, (1, 2, 0)).reshape(-1, sequence.shape[1])
    key_values, query, gate, sequence_near = local_kernel(
        project_body,
        (
            pltpu.VMEM((row_count, rows_here, LANES), BF16),
            pltpu.VMEM((rows_here, LANES), F32),
            pltpu.VMEM((rows_here, LANES), F32),
            pltpu.VMEM(sequence.shape, BF16),
        ),
        "project",
        sequence,
        weights,
        scratch=(pltpu.VMEM(weights.shape, BF16), pltpu.SemaphoreType.DMA((3,))),
        far=True,
    )
    key_values_all = exchange(key_values, ROW)

    bias_in = jnp.transpose(bias_weight)
    triangle = jnp.transpose(triangle_in, (1, 0, 2))
    kept = dict(
        pair=pair_state,
        attention_out=attention_out,
        outer_in=outer_in,
        outer_out=outer_out,
        triangle_out=triangle_out,
        transition_up=transition_up,
        transition_down=transition_down,
    )
    few = rows_here // I_PARTS
    near = local_kernel(
        prepare_body,
        (
            *[pltpu.VMEM(kept[k].shape, kept[k].dtype) for k in KEPT],
            pltpu.VMEM((col_count, heads_here * GROUPS, LANES), F32),
            pltpu.VMEM((col_count, 2 * group, channels), BF16),
            pltpu.VMEM((col_count, 2 * group, channels), BF16),
            pltpu.VMEM((channels, channels), BF16),
            pltpu.VMEM((1, pairs_here), F32),
            pltpu.VMEM((2 * group * rows_here,) * 2, BF16),
            pltpu.VMEM((group * rows_here, K_PARTS * group * rows_here), BF16),
            pltpu.VMEM((heads_here * rows_here, length_all), F32),
            pltpu.VMEM((cols_here // 2, length_all // 2), BF16),
        ),
        "prepare",
        row_start.reshape(1),
        col_index.reshape(1),
        chain_bias,
        *[kept[k] for k in KEPT],
        residue_mask.reshape(1, -1),
        chain_index.reshape(1, -1),
        bias_in,
        triangle,
        scalars=3,
        scratch=(
            pltpu.VMEM((1, length_all), jnp.int32),
            pltpu.VMEM((1, length_all), jnp.int32),
            pltpu.VMEM(bias_in.shape, BF16),
            pltpu.VMEM(triangle.shape, BF16),
            pltpu.VMEM((GROUPS, bias_in.shape[0], LANES), F32),
            pltpu.SemaphoreType.DMA((len(KEPT) + 4,)),
        ),
        far=True,
    )
    near, made = dict(zip(KEPT, near)), near[len(KEPT) :]
    bias_blocks, gates_in, values_in, last_in, pair_live, spread_order, gather_order, extra, pick = made

    key_values_all, bias_blocks = lax.optimization_barrier((key_values_all, bias_blocks))
    bias_blocks = exchange(bias_blocks, "col")
    terms = local_kernel(
        attention_body,
        pltpu.VMEM((col_count, *sequence.shape), BF16),
        "attention",
        bias_blocks,
        extra,
        key_values_all,
        query,
        gate,
        near["attention_out"],
        scratch=(
            pltpu.VMEM((heads_here * rows_here, LANES), F32),
            pltpu.VMEM((rows_here, LANES), F32),
        ),
    )
    terms = exchange(terms, "col")
    width = outer_in.shape[1]
    sequence_summed, left_twice, right_copies = local_kernel(
        settle_body,
        (
            pltpu.VMEM(sequence.shape, BF16),
            pltpu.VMEM((rows_here, width), F32),
            pltpu.VMEM((row_count, rows_here // 2, width), BF16),
        ),
        "settle",
        terms,
        sequence_near,
        near["outer_in"],
    )
    rights = exchange(right_copies, ROW)
    tiles, pair_mid, out_gate = local_kernel(
        pair_body,
        (
            pltpu.VMEM((col_count, 2 * group, pairs_here), BF16),
            pltpu.VMEM((pairs_here, channels), F32),
            pltpu.VMEM((pairs_here, channels), F32),
        ),
        "pair",
        rights,
        pick,
        left_twice,
        near["pair"],
        near["outer_out"],
        gates_in,
        values_in,
        last_in,
        pair_live,
    )

    tiles = exchange(tiles, "col")
    panels = local_kernel(
        spread_body,
        pltpu.VMEM((row_count, few + rows_here, length_all // K_PARTS), BF16),
        "spread",
        tiles,
        spread_order,
    )
    panels = exchange(panels, ROW)
    product = lax.dot_general(
        panels[:, :few].reshape(-1, length_all // K_PARTS),
        panels[:, few:].reshape(-1, length_all // K_PARTS),
        (((1,), (1,)), ((), ())),
        preferred_element_type=F32,
    ).astype(BF16)
    product = exchange(product.reshape(row_count, few, length_all), ROW)
    product = local_kernel(
        gather_body,
        pltpu.VMEM((col_count, group, pairs_here), BF16),
        "gather",
        product,
        gather_order,
    )
    product = exchange(product, "col").reshape(channels, pairs_here)

    sequence_out, pair_out = local_kernel(
        tail_body,
        (
            jax.ShapeDtypeStruct(sequence.shape, BF16),
            jax.ShapeDtypeStruct((pairs_here, channels), BF16),
        ),
        "tail",
        sequence_summed,
        product,
        pair_mid,
        out_gate,
        near["triangle_out"],
        near["transition_up"],
        near["transition_down"],
        scratch=(
            pltpu.VMEM((pairs_here, channels), BF16),
            pltpu.SemaphoreType.DMA((TAIL_PARTS + 1,)),
        ),
    )
    pair_out = pair_out.reshape(rows_here, cols_here, channels)
    return (sequence_out, pair_out)


def solution(mesh):
    finer = Mesh(mesh.devices.reshape(4, 8, mesh.shape["col"]), ("row_0", "row_1", "col"))
    placed = (
        P(ROW, None),
        P(ROW, "col", None),
        P(),
        P(),
        P(None, None, "col"),
        P("col", None),
        P(),
        P(),
        P(),
        P(),
        P(),
        P(),
        P(),
        P(),
    )
    return jax.shard_map(
        per_device,
        mesh=finer,
        in_specs=placed,
        out_specs=(P(ROW, None), P(ROW, "col", None)),
        check_vma=False,
    )
```

```python
import math

import jax
import jax.numpy as jnp
from jax import lax
from jax.experimental import pallas as pl
from jax.experimental.pallas import tpu as pltpu
from jax.sharding import Mesh
from jax.sharding import PartitionSpec as P

ROW = ("row_0", "row_1")
PAIR_AT = tuple(u ^ 10 for u in range(16))
PAIR_PLACE = tuple(PAIR_AT.index(q) for q in range(16))
ROW_AT = tuple(2 * q + k for q in PAIR_AT for k in range(2))
ROW_PLACE = tuple(ROW_AT.index(r) for r in range(32))
COL_AT = tuple((p + 2) % 4 * 4 + (p // 4 ^ 1) for p in range(16))
COL_PLACE = tuple(COL_AT.index(q) for q in range(16))
BF16 = jnp.bfloat16
F32 = jnp.float32
K_PARTS = 2
I_PARTS = 2
TAIL_PARTS = 4
KEPT = (
    "pair",
    "attention_out",
    "outer_in",
    "outer_out",
    "triangle_out",
    "transition_up",
    "transition_down",
)
LANES = 128
GROUPS = 4


def exchange(blocks, axis):
    rows, cols = lax.axis_size(ROW), lax.axis_size("col")
    if axis == "col":
        groups = [[r * cols + q for q in COL_AT] for r in range(rows)]
    else:
        groups = [[r * cols + q for r in ROW_AT] for q in range(cols)]
    return lax.all_to_all(
        blocks, (*ROW, "col"), split_axis=0, concat_axis=0, tiled=True, axis_index_groups=groups
    )


def layer_norm(values, axis=-1):
    center = values - jnp.mean(values, axis=axis, keepdims=True)
    spread = jnp.mean(center * center, axis=axis, keepdims=True)
    return center * lax.rsqrt(spread + 1e-05)


def local_kernel(body, out_shape, name, *operands, scalars=0, scratch=(), far=False):
    space = pltpu.HBM if far else pltpu.VMEM
    spaces = [pltpu.SMEM if k < scalars else space for k in range(len(operands))]
    held = [
        pltpu.with_memory_space_constraint(x, space) if space is pltpu.VMEM else x
        for x, space in zip(operands, spaces)
    ]
    in_hbm = lambda x: isinstance(x, jax.ShapeDtypeStruct)
    return pl.pallas_call(
        body,
        out_shape=out_shape,
        in_specs=[pl.BlockSpec(memory_space=space) for space in spaces],
        out_specs=jax.tree.map(
            lambda x: pl.BlockSpec(memory_space=pltpu.HBM if in_hbm(x) else pltpu.VMEM), out_shape
        ),
        scratch_shapes=scratch,
        name=name,
    )(*held)


def fetch(sources, targets, arrived):
    copies = [
        pltpu.make_async_copy(source, target, arrived.at[k])
        for k, (source, target) in enumerate(zip(sources, targets))
    ]
    for copy in copies:
        copy.start()
    return copies


def mm(a, b, over_a, over_b):
    return lax.dot_general(a, b, (((over_a,), (over_b,)), ((), ())), preferred_element_type=F32)


def turn_lanes(value, groups):
    steps = groups % GROUPS
    return pltpu.roll(value, steps * (LANES // GROUPS), 1) if steps else value


def regroup(pick, shape):
    group = lax.broadcasted_iota(jnp.int32, shape, 1) // (LANES // GROUPS)
    tile = pick(0)
    for k in range(1, GROUPS):
        tile = jnp.where(group == k, pick(k), tile)
    return tile


def project_body(sequence, weights, key_values, query, gate, near, held, arrived):
    parts = [pl.ds(k * LANES, LANES) for k in range(2)]
    first_copy, *weight_copies = fetch(
        (sequence, *[weights.at[part] for part in parts]),
        (near, *[held.at[part] for part in parts]),
        arrived,
    )
    first_copy.wait()
    normed = layer_norm(near[...].astype(F32)).astype(BF16)
    projected = []
    for part, copy in zip(parts, weight_copies):
        copy.wait()
        projected.append(mm(normed, held[part], 1, 1))
    head, rest = projected
    rows = head.shape[0]
    first = lax.broadcasted_iota(jnp.int32, (rows, LANES), 1) < LANES // 2
    both = jnp.where(first, pltpu.roll(head, LANES // 2, 1), pltpu.roll(rest, LANES // 2, 1))
    key_values[...] = jnp.broadcast_to(both.astype(BF16)[None], key_values.shape)
    query[...] = jnp.where(first, head, 0.0).astype(BF16).astype(F32)
    gate[...] = jnp.where(first, 0.0, jax.nn.sigmoid(rest))


def prepare_body(row_start, col, chain_bias, *refs):
    count = len(KEPT)
    sources, targets = refs[: count + 4], refs[count + 4 : 2 * count + 4]
    blocks, gates_in, values_in, last_in, live, spread_order, gather_order, extra, pick = refs[
        2 * count + 4 : -6
    ]
    mask_near, chain_near, bias_near, triangle_near, turned_bias, arrived = refs[-6:]
    copies = fetch(
        sources, (*targets, mask_near, chain_near, bias_near, triangle_near), arrived
    )
    near = dict(zip(KEPT, targets))
    landed = dict(zip((*KEPT, "mask", "chain", "bias_in", "triangle"), copies))

    size = spread_order.shape[0]
    n = lax.broadcasted_iota(jnp.int32, spread_order.shape, 0)
    m = lax.broadcasted_iota(jnp.int32, spread_order.shape, 1)
    rows = live.shape[1] // (LANES // GROUPS)
    wanted = n % rows * (size // rows) + n // rows
    spread_order[...] = jnp.where(m == wanted, 1.0, 0.0).astype(BF16)
    size = gather_order.shape[0]
    group, few = size // rows, rows // I_PARTS
    n = lax.broadcasted_iota(jnp.int32, gather_order.shape, 0)
    m = lax.broadcasted_iota(jnp.int32, gather_order.shape, 1)
    i, c = n // group, n % group
    wanted = (i // few * group + c) * few + i % few
    gather_order[...] = jnp.where(m % size == wanted, 1.0, 0.0).astype(BF16)

    n = lax.broadcasted_iota(jnp.int32, pick.shape, 0)
    m = lax.broadcasted_iota(jnp.int32, pick.shape, 1)
    place = jnp.zeros(pick.shape, jnp.int32)
    for q, u in enumerate(PAIR_PLACE):
        place = jnp.where(col[0] == q, u, place)
    pick[...] = jnp.where(m == place * pick.shape[0] + n, 1.0, 0.0).astype(BF16)

    landed["pair"].wait()
    landed["bias_in"].wait()
    wide = near["pair"][...].astype(F32)
    turned = jnp.concatenate([wide[GROUPS * (p % GROUPS) + p // GROUPS] for p in range(rows)], axis=0)
    normed = layer_norm(turned).astype(BF16)
    heads = bias_near.shape[0]
    n = lax.broadcasted_iota(jnp.int32, (heads, heads), 0)
    m = lax.broadcasted_iota(jnp.int32, (heads, heads), 1)
    place = n // 2
    by_place = jnp.where(m == ((place + 2) % 4 * 4 + (place // 4 ^ 1)) * 2 + n % 2, 1.0, 0.0).astype(BF16)
    bias = mm(mm(by_place, bias_near[...], 1, 0).astype(BF16), normed, 1, 1)
    columns = blocks.shape[0]
    for t in range(GROUPS):
        turned_bias[t] = bias[:, t * LANES : (t + 1) * LANES]
        for h in range(2):
            blocks[:, h * GROUPS + t, :] = turned_bias[t, pl.ds(h, columns, stride=2), :]

    landed["mask"].wait()
    mask = mask_near[...].astype(F32).astype(BF16)
    length = mask.shape[1]
    residue = lax.broadcasted_iota(jnp.int32, (length, live.shape[1]), 0)
    pair = lax.broadcasted_iota(jnp.int32, (length, live.shape[1]), 1)
    of_row = jnp.where(residue == row_start[0] + pair // (LANES // GROUPS), 1.0, 0.0).astype(BF16)
    of_col = jnp.where(residue == col[0] * (LANES // GROUPS) + pair % (LANES // GROUPS), 1.0, 0.0).astype(BF16)
    mask = jnp.broadcast_to(mask, (8, length))
    live[...] = (mm(mask, of_row, 1, 0) * mm(mask, of_col, 1, 0))[:1]

    landed["chain"].wait()
    eight = blocks.shape[1]
    four = eight // 2
    position = lax.broadcasted_iota(jnp.int32, (eight, length), 1)
    row = lax.broadcasted_iota(jnp.int32, (eight, length), 0)
    chains = jnp.broadcast_to(chain_near[...].astype(F32), (eight, length))
    kept = jnp.broadcast_to(mask_near[...], (eight, length)) == 1
    offset = jnp.where(row < four, chain_bias[2 * col[0]], chain_bias[2 * col[0] + 1])
    for g in range(GROUPS):
        here = position == row_start[0] + g * four + row % four
        own_chain = jnp.sum(jnp.where(here, chains, 0.0), axis=1, keepdims=True)
        added = jnp.where(chains == own_chain, offset, 0.0)
        extra[g * eight : (g + 1) * eight, :] = jnp.where(kept | here, added, -jnp.inf)

    landed["triangle"].wait()
    half = gates_in.shape[1] // 2
    for k, target in enumerate((gates_in, values_in, gates_in, values_in)):
        side = half * (k // 2)
        across = jnp.transpose(triangle_near[k].astype(F32)).astype(BF16)
        target[:, side : side + half, :] = across.reshape(target.shape[0], half, LANES)
    last_in[...] = triangle_near[4]
    for name in KEPT:
        if name != "pair":
            landed[name].wait()


def attention_body(blocks, extra, key_values, query, gate, attention_out, copies, spread, joined):
    count, eight, _ = blocks.shape
    four = eight // 2
    length = count * (LANES // GROUPS)
    lane = lax.broadcasted_iota(jnp.int32, (four, LANES), 1)
    for g in range(GROUPS):
        taken = query[g * four : (g + 1) * four, :]
        for h in range(2):
            own = (lane >= h * (LANES // 4)) & (lane < (h + 1) * (LANES // 4))
            spread[g * eight + h * four : g * eight + (h + 1) * four, :] = jnp.where(own, taken, 0.0)
    everyone = jnp.concatenate([key_values[p] for p in ROW_PLACE], axis=0)
    raw = mm(spread[...].astype(BF16), everyone, 1, 1)
    raw = raw * (1.0 / math.sqrt(LANES // 4))
    biases = []
    for g in range(GROUPS):
        pieces = []
        for tile in range(count // GROUPS):
            pieces.append(
                regroup(
                    lambda k, tile=tile, g=g: turn_lanes(blocks[COL_PLACE[GROUPS * tile + k]], k - g),
                    (eight, LANES),
                )
            )
        biases.append(jnp.concatenate(pieces, axis=1))
    scores = raw + jnp.concatenate(biases, axis=0) + extra[...]
    raised = jnp.exp(scores - jnp.max(scores, axis=1, keepdims=True))
    weights = [raised / jnp.sum(raised, axis=1, keepdims=True)]
    mixed = mm(jnp.concatenate(weights, axis=0).astype(BF16), everyone, 1, 0)
    for g in range(GROUPS):
        upper = mixed[g * eight : g * eight + four]
        lower = mixed[g * eight + four : (g + 1) * eight]
        joined[g * four : (g + 1) * four, :] = jnp.where(lane < LANES * 3 // 4, upper, lower)
    gated = pltpu.roll(gate[...] * joined[...], LANES // 2, 1)[:, : LANES // 2].astype(BF16)
    terms = mm(gated, attention_out[...], 1, 0).astype(BF16)
    copies[...] = jnp.broadcast_to(terms[None], copies.shape)


def spread_body(tiles, order, panels):
    count, chans, pairs = tiles.shape
    rows = pairs // (LANES // GROUPS)
    per = count // GROUPS
    by_row = []
    for i in range(rows):
        at, g = i // GROUPS * LANES, i % GROUPS
        by_row.append(
            jnp.concatenate(
                [
                    regroup(
                        lambda k, tile=tile, g=g, at=at: turn_lanes(
                            tiles[COL_PLACE[GROUPS * tile + k], :, at : at + LANES].astype(F32), k - g
                        ),
                        (chans, LANES),
                    )
                    for tile in range(per)
                ],
                axis=1,
            )
        )
    turned = mm(order[...], jnp.concatenate(by_row, axis=0).astype(BF16), 1, 0).astype(BF16)
    half = chans // 2
    few = rows // I_PARTS
    wide = turned.shape[1] // K_PARTS
    for k in range(K_PARTS):
        for i in range(I_PARTS):
            for c in range(half):
                block = (k * I_PARTS + i) * half + c
                at = c * rows + i * few
                panels[block, :few, :] = turned[at : at + few, k * wide : (k + 1) * wide]
                at = (half + c) * rows
                panels[block, few:, :] = turned[at : at + rows, k * wide : (k + 1) * wide]


def gather_body(parts, order, blocks):
    total, few, length = parts.shape
    count, group, pairs = blocks.shape
    rows = pairs // (LANES // GROUPS)
    summed = mm(order[...], parts[...].reshape(total * few, length), 1, 0)
    for q in range(count):
        place = PAIR_PLACE[COL_AT[q]]
        tile, s = place // GROUPS, place % GROUPS
        pieces = []
        for t in range(rows // GROUPS):
            pieces.append(
                regroup(
                    lambda k, t=t, tile=tile, s=s: turn_lanes(
                        summed[
                            (GROUPS * t + k) * group : (GROUPS * t + k + 1) * group,
                            tile * LANES : (tile + 1) * LANES,
                        ],
                        k - s,
                    ),
                    (group, LANES),
                )
            )
        blocks[q] = jnp.concatenate(pieces, axis=1).astype(BF16)


def settle_body(terms, sequence, outer_in, sequence_out, left_twice, right_copies):
    update = jnp.sum(terms[...].astype(F32), axis=0)
    summed = (sequence[...].astype(F32) + update).astype(BF16)
    sequence_out[...] = summed
    normed = layer_norm(summed.astype(F32)).astype(BF16)
    outer_rows = mm(normed, outer_in[...], 1, 0).astype(BF16).astype(F32)
    rows, width = outer_rows.shape
    half = width // 2
    first = lax.broadcasted_iota(jnp.int32, (rows, width), 1) < half
    turned = pltpu.roll(outer_rows, half, 1)
    left_twice[...] = jnp.where(first, outer_rows, turned)
    packed = jnp.where(first[: rows // 2], turned[: rows // 2], outer_rows[rows // 2 :])
    right_copies[...] = jnp.broadcast_to(packed.astype(BF16)[None], right_copies.shape)


def pair_body(
    rights,
    pick,
    left_twice,
    pair,
    outer_out,
    gates_in,
    values_in,
    last_in,
    live,
    tiles,
    mid,
    out_gate,
):
    rows, cols, channels = pair.shape
    half = channels // 2
    taken = mm(pick[...], rights[...].reshape(-1, channels), 1, 0)
    taken = taken.reshape(cols // rows, rows // 2, channels)
    first = lax.broadcasted_iota(jnp.int32, (rows // 2, channels), 1) < half
    pieces = []
    for k in range(cols // rows):
        turned = pltpu.roll(taken[k], half, 1)
        pieces.append(jnp.where(first, taken[k], turned))
        pieces.append(jnp.where(first, turned, taken[k]))
    right_twice = jnp.concatenate(pieces, axis=0)
    left = left_twice[...][:, None, :]
    right = right_twice[None, :, :]
    lane = lax.broadcasted_iota(jnp.int32, (rows, cols, channels), 2)
    feat = jnp.where(lane < half, left * right, left - right).astype(BF16)
    feat = feat.reshape(rows * cols, channels)
    pair_mid = pair[...].astype(F32).reshape(rows * cols, channels) + mm(feat, outer_out[...], 1, 0)
    mid[...] = pair_mid
    normed = layer_norm(pair_mid).astype(BF16)
    flat = (-1, channels)
    opened = jax.nn.sigmoid(mm(gates_in[...].reshape(flat), normed, 1, 1))
    operands = opened * mm(values_in[...].reshape(flat), normed, 1, 1) * live[...]
    tiles[...] = operands.astype(BF16).reshape(tiles.shape)
    out_gate[...] = jax.nn.sigmoid(mm(normed, last_in[...], 1, 0))


def tail_body(
    sequence_near,
    product,
    mid,
    out_gate,
    triangle_out,
    transition_up,
    transition_down,
    sequence_out,
    out,
    held,
    left,
):
    copies = [pltpu.make_async_copy(sequence_near, sequence_out, left.at[TAIL_PARTS])]
    copies[0].start()
    normed_product = layer_norm(product[...].astype(F32), axis=0)
    normed_product = jnp.transpose(normed_product).astype(BF16)
    late = mid[...] + out_gate[...] * mm(normed_product, triangle_out[...], 1, 0)
    normed_late = layer_norm(late).astype(BF16)
    hidden = jnp.maximum(mm(normed_late, transition_up[...], 1, 0), 0.0).astype(BF16)
    part = mid.shape[0] // TAIL_PARTS
    for k in range(TAIL_PARTS):
        here = slice(k * part, (k + 1) * part)
        held[here] = (late[here] + mm(hidden[here], transition_down[...], 1, 0)).astype(BF16)
        copies.append(pltpu.make_async_copy(held.at[here], out.at[here], left.at[k]))
        copies[-1].start()
    for copy in copies:
        copy.wait()


def per_device(
    sequence,
    pair_state,
    residue_mask,
    chain_index,
    attention_in,
    attention_out,
    bias_weight,
    chain_bias,
    outer_in,
    outer_out,
    triangle_in,
    triangle_out,
    transition_up,
    transition_down,
):
    rows_here, cols_here, channels = pair_state.shape
    length_all = residue_mask.shape[0]
    pairs_here = rows_here * cols_here
    row_index = lax.axis_index(ROW)
    col_index = lax.axis_index("col")
    row_count = lax.axis_size(ROW)
    col_count = lax.axis_size("col")
    row_start = row_index * rows_here

    group = channels // col_count
    heads_here = bias_weight.shape[1] // col_count

    weights = jnp.transpose(attention_in, (1, 2, 0)).reshape(-1, sequence.shape[1])
    key_values, query, gate, sequence_near = local_kernel(
        project_body,
        (
            pltpu.VMEM((row_count, rows_here, LANES), BF16),
            pltpu.VMEM((rows_here, LANES), F32),
            pltpu.VMEM((rows_here, LANES), F32),
            pltpu.VMEM(sequence.shape, BF16),
        ),
        "project",
        sequence,
        weights,
        scratch=(pltpu.VMEM(weights.shape, BF16), pltpu.SemaphoreType.DMA((3,))),
        far=True,
    )
    key_values_all = exchange(key_values, ROW)

    bias_in = jnp.transpose(bias_weight)
    triangle = jnp.transpose(triangle_in, (1, 0, 2))
    kept = dict(
        pair=pair_state,
        attention_out=attention_out,
        outer_in=outer_in,
        outer_out=outer_out,
        triangle_out=triangle_out,
        transition_up=transition_up,
        transition_down=transition_down,
    )
    few = rows_here // I_PARTS
    near = local_kernel(
        prepare_body,
        (
            *[pltpu.VMEM(kept[k].shape, kept[k].dtype) for k in KEPT],
            pltpu.VMEM((col_count, heads_here * GROUPS, LANES), F32),
            pltpu.VMEM((col_count, 2 * group, channels), BF16),
            pltpu.VMEM((col_count, 2 * group, channels), BF16),
            pltpu.VMEM((channels, channels), BF16),
            pltpu.VMEM((1, pairs_here), F32),
            pltpu.VMEM((2 * group * rows_here,) * 2, BF16),
            pltpu.VMEM((group * rows_here, K_PARTS * group * rows_here), BF16),
            pltpu.VMEM((heads_here * rows_here, length_all), F32),
            pltpu.VMEM((cols_here // 2, length_all // 2), BF16),
        ),
        "prepare",
        row_start.reshape(1),
        col_index.reshape(1),
        chain_bias,
        *[kept[k] for k in KEPT],
        residue_mask.reshape(1, -1),
        chain_index.reshape(1, -1),
        bias_in,
        triangle,
        scalars=3,
        scratch=(
            pltpu.VMEM((1, length_all), jnp.int32),
            pltpu.VMEM((1, length_all), jnp.int32),
            pltpu.VMEM(bias_in.shape, BF16),
            pltpu.VMEM(triangle.shape, BF16),
            pltpu.VMEM((GROUPS, bias_in.shape[0], LANES), F32),
            pltpu.SemaphoreType.DMA((len(KEPT) + 4,)),
        ),
        far=True,
    )
    near, made = dict(zip(KEPT, near)), near[len(KEPT) :]
    bias_blocks, gates_in, values_in, last_in, pair_live, spread_order, gather_order, extra, pick = made

    key_values_all, bias_blocks = lax.optimization_barrier((key_values_all, bias_blocks))
    bias_blocks = exchange(bias_blocks, "col")
    terms = local_kernel(
        attention_body,
        pltpu.VMEM((col_count, *sequence.shape), BF16),
        "attention",
        bias_blocks,
        extra,
        key_values_all,
        query,
        gate,
        near["attention_out"],
        scratch=(
            pltpu.VMEM((heads_here * rows_here, LANES), F32),
            pltpu.VMEM((rows_here, LANES), F32),
        ),
    )
    terms = exchange(terms, "col")
    width = outer_in.shape[1]
    sequence_summed, left_twice, right_copies = local_kernel(
        settle_body,
        (
            pltpu.VMEM(sequence.shape, BF16),
            pltpu.VMEM((rows_here, width), F32),
            pltpu.VMEM((row_count, rows_here // 2, width), BF16),
        ),
        "settle",
        terms,
        sequence_near,
        near["outer_in"],
    )
    rights = exchange(right_copies, ROW)
    tiles, pair_mid, out_gate = local_kernel(
        pair_body,
        (
            pltpu.VMEM((col_count, 2 * group, pairs_here), BF16),
            pltpu.VMEM((pairs_here, channels), F32),
            pltpu.VMEM((pairs_here, channels), F32),
        ),
        "pair",
        rights,
        pick,
        left_twice,
        near["pair"],
        near["outer_out"],
        gates_in,
        values_in,
        last_in,
        pair_live,
    )

    tiles = exchange(tiles, "col")
    panels = local_kernel(
        spread_body,
        pltpu.VMEM((row_count, few + rows_here, length_all // K_PARTS), BF16),
        "spread",
        tiles,
        spread_order,
    )
    panels = exchange(panels, ROW)
    product = lax.dot_general(
        panels[:, :few].reshape(-1, length_all // K_PARTS),
        panels[:, few:].reshape(-1, length_all // K_PARTS),
        (((1,), (1,)), ((), ())),
        preferred_element_type=F32,
    ).astype(BF16)
    product = exchange(product.reshape(row_count, few, length_all), ROW)
    product = local_kernel(
        gather_body,
        pltpu.VMEM((col_count, group, pairs_here), BF16),
        "gather",
        product,
        gather_order,
    )
    product = exchange(product, "col").reshape(channels, pairs_here)

    sequence_out, pair_out = local_kernel(
        tail_body,
        (
            jax.ShapeDtypeStruct(sequence.shape, BF16),
            jax.ShapeDtypeStruct((pairs_here, channels), BF16),
        ),
        "tail",
        sequence_summed,
        product,
        pair_mid,
        out_gate,
        near["triangle_out"],
        near["transition_up"],
        near["transition_down"],
        scratch=(
            pltpu.VMEM((pairs_here, channels), BF16),
            pltpu.SemaphoreType.DMA((TAIL_PARTS + 1,)),
        ),
    )
    pair_out = pair_out.reshape(rows_here, cols_here, channels)
    return (sequence_out, pair_out)


def solution(mesh):
    finer = Mesh(mesh.devices.reshape(4, 8, mesh.shape["col"]), ("row_0", "row_1", "col"))
    placed = (
        P(ROW, None),
        P(ROW, "col", None),
        P(),
        P(),
        P(None, None, "col"),
        P("col", None),
        P(),
        P(),
        P(),
        P(),
        P(),
        P(),
        P(),
        P(),
    )
    return jax.shard_map(
        per_device,
        mesh=finer,
        in_specs=placed,
        out_specs=(P(ROW, None), P(ROW, "col", None)),
        check_vma=False,
    )
```
